256 devices in a mesh: seq: 32 (over z, x), tp: 8 (over y, core).
Axes of the slice: x: 4, y: 4, z: 8, core: 2. Of those that a mesh axis runs over, the one named last changes fastest.
Arguments:
- queries: bfloat16 [6144, 6144], P('seq', 'tp'), may hold values from -400 to 400
- key_vectors: bfloat16 [6144, 1024], P('seq', 'tp'), may hold values from -8 to 8
- value_vectors: bfloat16 [6144, 1024], P('seq', 'tp'), may hold values from -6 to 6
- positions: int32 [6144], P('seq'), may hold values from 0 to 6143, as said below
- residual: bfloat16 [6144, 6144], P('seq', 'tp'), may hold values from -200 to 200
- norm_gain: float32 [1, 6144], P(None, 'tp'), may hold values from 0.5 to 1.5
- out_weight: bfloat16 [6144, 6144], P('tp'), may hold values from -0.3125 to 0.3125
Outputs:
- quantized: bfloat16 [6144, 6144], P('seq')
- token_scale: float32 [6144], P('seq')
- new_residual: bfloat16 [6144, 6144], P('seq', 'tp')
The draws below stay inside these ranges and needn't reach their ends.
Inputs may be any that keep to these rules, and one draw needn't show every extreme that they name: The positions are a permutation of 0 to 6143. Cut into 64 runs of 96 consecutive positions, the rows of one index of seq hold run r in their first 96 rows and run 2 * 32 - 1 - r in their last ones, both in increasing order, with r differing between the indices of seq.
All inputs are finite; a program needn't handle non-finite values. Where the reference program divides by a largest or mean magnitude, that divisor is 1e-20 or more.
Results may differ from the reference program's by a relative error of at most 0.012.
Values may be sent and summed in bfloat16 or wider, within the bound.
A program may use at most 64 MiB of HBM per device.

```python
import math
import jax
import jax.numpy as jnp
from jax import lax

D = 6144
Q_HEADS = 48
KV_HEADS = 8
HEAD = 128
TOK_DEV = 192
TOKENS = 6144
N_SEQ = 32
N_TP = 8


def shared_keys(key):
    inner_key = jax.random.fold_in(key, 21)
    shape = (TOKENS, KV_HEADS * HEAD)
    base_draw = jax.random.truncated_normal(inner_key, -5.0, 5.0, shape, jnp.float32)
    return base_draw


def draw_key_vectors(key, part):
    base_draw = shared_keys(key)
    return base_draw.astype(jnp.bfloat16)


def draw_queries(key, part):
    shape = (TOKENS, Q_HEADS * HEAD)
    noise_key = jax.random.fold_in(key, 23)
    base_draw = 2.0 * jax.random.truncated_normal(noise_key, -5.0, 5.0, shape, jnp.float32)
    return base_draw.astype(jnp.bfloat16)


def draw_positions(key, part):
    run_order = jax.random.permutation(jax.random.fold_in(key, 11), N_SEQ).astype(jnp.int32)
    half_rows = TOK_DEV // 2
    lane_index = jnp.arange(half_rows, dtype=jnp.int32)
    first_run = run_order[:, None] * half_rows + lane_index[None, :]
    second = (2 * N_SEQ - 1 - run_order)[:, None] * half_rows + lane_index[None, :]
    return jnp.concatenate([first_run, second], axis=1).reshape(TOKENS).astype(jnp.int32)


def draw_residual(key, part):
    noise_key = jax.random.fold_in(key, 31)
    column_key = jax.random.fold_in(key, 32)
    row_key = jax.random.fold_in(key, 33)
    column_index = jnp.arange(D, dtype=jnp.float32)
    column_scale = 3.0 ** (column_index / D) * jnp.exp(jax.random.uniform(column_key, (D,), jnp.float32, 0.0, 1.2))
    noise = jax.random.truncated_normal(noise_key, -5.0, 5.0, (TOKENS, D), jnp.float32)
    row_scale = jnp.exp(jax.random.uniform(row_key, (TOKENS, 1), jnp.float32, 0.0, math.log(10.0)))
    return (0.2 * noise * row_scale * column_scale[None, :]).astype(jnp.bfloat16)


def steps_of(stream_key, extent, shards, low, largest):
    gain, own = 1.0, jax.random.fold_in(stream_key, 6)
    for position, shards_of in shards:
        draws = jnp.exp(jax.random.uniform(jax.random.fold_in(own, position), (shards_of,), jnp.float32, low / len(shards), largest / len(shards)))
        gain = gain * jnp.repeat(draws, extent[position] // shards_of).reshape([-1 if axis == position else 1 for axis in range(len(extent))])
    return gain


def centred(stream_key, extent, scale, reach, shards=(), kind=jnp.bfloat16):
    loudness = steps_of(stream_key, extent, shards, -0.22, 0.18) if shards else 1.0
    values = jax.random.normal(stream_key, extent, jnp.float32) * scale * loudness
    return jnp.minimum(jnp.maximum(values, -reach), reach).astype(kind)


def setup_inputs(seed: int = 0) -> dict:
    splits = jax.random.split(jax.random.key(seed), 8)
    return {
        "queries": draw_queries(jax.random.fold_in(splits[7], 71), 0),
        "key_vectors": draw_key_vectors(jax.random.fold_in(splits[7], 71), 0),
        "value_vectors": centred(splits[2], (TOKENS, KV_HEADS * HEAD), 1.0, 6.0, ((0, 32), (1, 8))),
        "positions": draw_positions(jax.random.fold_in(splits[7], 71), 0),
        "residual": draw_residual(jax.random.fold_in(splits[7], 71), 0),
        "norm_gain": jnp.clip(1.0 + 0.1 * jax.random.normal(splits[5], (1, D), jnp.float32), 0.5, 1.5),
        "out_weight": centred(splits[6], (Q_HEADS * HEAD, D), (Q_HEADS * HEAD // 16) ** -0.5, 0.3125, ((0, 8),)),
    }


def reference(queries, key_vectors, value_vectors, positions, residual, norm_gain, out_weight):
    token_count = queries.shape[0]
    group_size = Q_HEADS // KV_HEADS
    score_scale = 1.0 / math.sqrt(HEAD)
    query_heads = queries.reshape(token_count, Q_HEADS, HEAD).transpose(1, 0, 2)
    key_heads = key_vectors.reshape(token_count, KV_HEADS, HEAD).transpose(1, 0, 2)
    value_heads = value_vectors.reshape(token_count, KV_HEADS, HEAD).transpose(1, 0, 2)
    block_rows = TOK_DEV
    block_count = token_count // block_rows
    query_blocks = query_heads.reshape(Q_HEADS, block_count, block_rows, HEAD)
    pos_blocks = positions.reshape(block_count, block_rows)

    def one_head(head_index):
        key_rows = key_heads[head_index // group_size]
        value_rows = value_heads[head_index // group_size]

        def one_block(block_pair):
            query_block, block_pos = block_pair
            scores = jnp.dot(query_block, key_rows.T, preferred_element_type=jnp.float32) * score_scale
            visible = positions[None, :] <= block_pos[:, None]
            scores = jnp.where(visible, scores, -1e+30)
            row_max = lax.optimization_barrier(jnp.max(scores, axis=1, keepdims=True))
            raw_weights = jnp.where(visible, jnp.exp(scores - row_max), 0.0)
            weight_sum = lax.optimization_barrier(jnp.sum(raw_weights, axis=1, keepdims=True))
            mixed = jnp.dot(raw_weights.astype(jnp.bfloat16), value_rows, preferred_element_type=jnp.float32)
            return (mixed / weight_sum).astype(jnp.bfloat16)
        return lax.map(one_block, (query_blocks[head_index], pos_blocks))
    attended = lax.map(one_head, jnp.arange(Q_HEADS, dtype=jnp.int32))
    attended = attended.reshape(Q_HEADS, token_count, HEAD).transpose(1, 0, 2).reshape(token_count, Q_HEADS * HEAD)
    group_width = Q_HEADS * HEAD // N_TP
    summed = residual.astype(jnp.float32)
    for group_index in range(N_TP):
        lower = group_index * group_width
        partial_value = jnp.dot(attended[:, lower:lower + group_width], out_weight[lower:lower + group_width], preferred_element_type=jnp.float32)
        partial_value = lax.optimization_barrier(partial_value.astype(jnp.bfloat16))
        summed = summed + partial_value.astype(jnp.float32)
    new_residual = summed.astype(jnp.bfloat16)
    mean_square = lax.optimization_barrier(jnp.mean(summed * summed, axis=1, keepdims=True))
    normed = summed * lax.rsqrt(mean_square + 1e-05) * norm_gain
    token_scale = lax.optimization_barrier(jnp.max(jnp.abs(normed), axis=1)) + 1e-06
    quantized = (normed / token_scale[:, None]).astype(jnp.bfloat16)
    return (quantized, token_scale, new_residual)
```

```python
import functools
import heapq
import math

import jax
import jax.numpy as jnp
from jax import lax
from jax.experimental import pallas as pl
from jax.experimental.pallas import tpu as pltpu
from jax.sharding import PartitionSpec as P

D = 6144
HEADS = 6
HEAD = 128
TOK = 192
RUN = TOK // 2
NX = 4
NZ = 8
ROWS = HEADS * RUN
GROUP = NX * RUN
NEG = -1e30
EXP_SCALE = math.log2(math.e) / math.sqrt(HEAD)
MESH = pl.DeviceIdType.MESH

K_LO, V_LO, K_HI, V_HI, RUN_ID = range(5)
X_FIRST = {K_LO: True, V_LO: False, K_HI: True, V_HI: False, RUN_ID: True}
REACH = {
    K_LO: (2, 1, 4, 3),
    V_LO: (2, 1, 4, 3),
    K_HI: (1, 2, 3, 4),
    V_HI: (1, 2, 3, 4),
    RUN_ID: (2, 1, 4, 3),
}
GROUP_ORDER = (0, 1, -1, 2, -2, 3, -3, 4)


def children(kind, mx, mz):
    xp, xn, zp, zn = REACH[kind]
    along_x, along_z = [], []
    if 0 <= mx < xp:
        along_x.append((kind, mx + 1, mz, 0))
    if -xn < mx <= 0:
        along_x.append((kind, mx - 1, mz, 1))
    if 0 <= mz < zp:
        along_z.append((kind, mx, mz + 1, 2))
    if -zn < mz <= 0:
        along_z.append((kind, mx, mz - 1, 3))
    if X_FIRST[kind]:
        return along_z + along_x if mz == 0 else along_z
    return along_x + along_z if mx == 0 else along_x


def plan():
    latency, piece, tiny = 2.2, 0.55, 0.05
    free = [0.0] * 4
    arrivals = []
    order = []

    def send_all(now, kind, mx, mz):
        for child in children(kind, mx, mz):
            direction = child[3]
            took = tiny if kind == RUN_ID else piece
            free[direction] = max(free[direction], now) + took
            heapq.heappush(arrivals, (free[direction] + latency, child[:3]))

    for kind in (K_LO, V_LO, RUN_ID, K_HI, V_HI):
        send_all(0.0, kind, 0, 0)
    units = []
    for dz in GROUP_ORDER:
        units.append((dz, (K_LO, V_LO, RUN_ID), 0.6))
        units.append((dz, (K_HI, V_HI), 0.4))
    have = set()
    now = 0.5
    steps = []
    for dz, kinds, cost in units:
        needed = set()
        for kind in kinds:
            xp, xn, zp, zn = REACH[kind]
            for mx in range(-xn, xp + 1):
                for mz in range(-zn, zp + 1):
                    if (mz - dz) % NZ == 0 and (mx, mz) != (0, 0):
                        needed.add((kind, mx, mz))
        waits = []
        while arrivals and (not needed <= have or arrivals[0][0] <= now):
            when, key = heapq.heappop(arrivals)
            now = max(now, when)
            have.add(key)
            waits.append(key)
            send_all(now, *key)
        now += cost
        steps.append(waits)
    assert not arrivals
    return steps, now


STEPS, PLANNED_US = plan()
EVENT_ID = {key: i for i, key in enumerate(key for waits in STEPS for key in waits)}
N_EVENTS = len(EVENT_ID)


def update(rows, queries, m_ref, l_ref, acc_ref, keys, values, bias, chunk):
    for start in range(rows[0], rows[1], chunk):
        at = pl.ds(start, chunk)
        scores = lax.dot_general(
            queries[at, :], keys, (((1,), (1,)), ((), ())), preferred_element_type=jnp.float32
        )
        scores = scores * EXP_SCALE
        if bias is not None:
            scores = scores + bias
        width = scores.shape[1]
        old = m_ref[at, :]
        new = jnp.maximum(old, jnp.max(scores, axis=1, keepdims=True))
        factor = jnp.exp2(old - new)
        weights = [
            jnp.exp2(scores[:, i : i + HEAD] - new) for i in range(0, width, HEAD)
        ]
        m_ref[at, :] = new
        l_ref[at, :] = l_ref[at, :] * factor + functools.reduce(jnp.add, weights)
        probs = jnp.concatenate([w.astype(jnp.bfloat16) for w in weights], axis=1)
        acc_ref[at, :] = acc_ref[at, :] * factor + jnp.dot(
            probs, values, preferred_element_type=jnp.float32
        )


def first_block(first, queries, m_ref, l_ref, acc_ref, keys, values):
    at = pl.ds(first, ROWS)
    scores = lax.dot_general(
        queries[at, :], keys, (((1,), (1,)), ((), ())), preferred_element_type=jnp.float32
    )
    scores = (scores * EXP_SCALE).reshape(HEADS, RUN, RUN)
    row = lax.broadcasted_iota(jnp.int32, (HEADS, RUN, RUN), 1)
    column = lax.broadcasted_iota(jnp.int32, (HEADS, RUN, RUN), 2)
    scores = jnp.where(column <= row, scores, NEG).reshape(ROWS, RUN)
    high = jnp.max(scores, axis=1, keepdims=True)
    weights = jnp.exp2(scores - high)
    m_ref[at, :] = jnp.broadcast_to(high, (ROWS, HEAD))
    total = jnp.sum(weights, axis=1, keepdims=True)
    lane = lax.broadcasted_iota(jnp.int32, (ROWS, HEAD), 1)
    l_ref[at, :] = jnp.where(lane == 0, total, 0.0)
    acc_ref[at, :] = jnp.dot(
        weights.astype(jnp.bfloat16), values, preferred_element_type=jnp.float32
    )


def lane_bias(ids, mine, low):
    one = [
        jnp.where(ids[j] < mine if low else ids[j] > mine, 0.0, NEG) for j in range(NX)
    ]
    lane = lax.broadcasted_iota(jnp.int32, (1, HEAD), 1)
    tiles = [
        jnp.where(lane < 96, one[0], one[1]),
        jnp.where(lane < 64, one[1], one[2]),
        jnp.where(lane < 32, one[2], one[3]),
    ]
    return jnp.concatenate(tiles, axis=1)


def attention_kernel(
    q_ref, own_ref, run_ref, swap_ref, out_ref, kv, ids, queries, m_ref, l_ref, acc_ref, send, recv
):
    seq = lax.axis_index("seq")
    tp = lax.axis_index("tp")
    x = lax.rem(seq, NX)
    z = seq // NX
    neighbours = (
        z * NX + lax.rem(x + 1, NX),
        z * NX + lax.rem(x + NX - 1, NX),
        lax.rem(z + 1, NZ) * NX + x,
        lax.rem(z + NZ - 1, NZ) * NX + x,
    )

    def source_of(mx, mz):
        return lax.rem(z + 2 * NZ - mz, NZ) * NX + lax.rem(x + 2 * NX - mx, NX)

    def place(kind, index):
        if kind == RUN_ID:
            return ids.at[index]
        return kv.at[kind, index]

    def copy_to(kind, mx, mz, child):
        own = (mx, mz) == (0, 0)
        index = source_of(mx, mz)
        target = place(kind, index)
        if own:
            source = run_ref.at[0] if kind == RUN_ID else own_ref.at[kind]
        else:
            source = target
        event = EVENT_ID[child[:3]]
        return pltpu.make_async_remote_copy(
            src_ref=source,
            dst_ref=target,
            send_sem=send.at[event],
            recv_sem=recv.at[event],
            device_id=(neighbours[child[3]], tp),
            device_id_type=MESH,
        )

    def send_all(kind, mx, mz):
        for child in children(kind, mx, mz):
            copy_to(kind, mx, mz, child).start()

    def run_events(waits):
        for kind, mx, mz in waits:
            target = place(kind, source_of(mx, mz))
            pltpu.make_async_remote_copy(
                src_ref=target,
                dst_ref=target,
                send_sem=send.at[EVENT_ID[(kind, mx, mz)]],
                recv_sem=recv.at[EVENT_ID[(kind, mx, mz)]],
                device_id=(neighbours[0], tp),
                device_id_type=MESH,
            ).wait_recv()
            send_all(kind, mx, mz)

    barrier = pltpu.get_barrier_semaphore()
    for peer in neighbours:
        pl.semaphore_signal(barrier, inc=1, device_id=(peer, tp), device_id_type=MESH)
    pl.semaphore_wait(barrier, 4)

    for kind in (K_LO, V_LO, RUN_ID, K_HI, V_HI):
        send_all(kind, 0, 0)

    swapped = jnp.broadcast_to(swap_ref[...], (RUN, HEAD)) > 0.5
    for head in range(HEADS):
        columns = pl.ds(head * HEAD, HEAD)
        first = q_ref[pl.ds(0, RUN), columns].astype(jnp.float32)
        last = q_ref[pl.ds(RUN, RUN), columns].astype(jnp.float32)
        queries[pl.ds(head * RUN, RUN), :] = jnp.where(swapped, last, first).astype(jnp.bfloat16)
        queries[pl.ds(ROWS + head * RUN, RUN), :] = jnp.where(swapped, first, last).astype(
            jnp.bfloat16
        )
    for kind in (K_LO, V_LO, K_HI, V_HI):
        kv[kind, seq] = own_ref[kind]
    ids[seq] = run_ref[0]
    mine = run_ref[0]

    first_block(0, queries, m_ref, l_ref, acc_ref, own_ref[K_LO], own_ref[V_LO])
    first_block(ROWS, queries, m_ref, l_ref, acc_ref, own_ref[K_HI], own_ref[V_HI])

    @pl.loop(0, NZ)
    def _(step):
        half = (step + 1) // 2
        dz = jnp.where(lax.rem(step, 2) == 1, half, -half)
        group = lax.rem(z + 2 * NZ - dz, NZ) * NX
        for j in range(NZ):

            @pl.when(step == j)
            def _(j=j):
                run_events(STEPS[2 * j])

        at = pl.ds(group, NX)
        found = ids[at]
        keys = kv[K_LO, at].reshape(GROUP, HEAD)
        values = kv[V_LO, at].reshape(GROUP, HEAD)
        state = (queries, m_ref, l_ref, acc_ref)
        update((0, ROWS), *state, keys, values, lane_bias(found, mine, True), RUN)
        update((ROWS, 2 * ROWS), *state, keys, values, None, RUN)
        for j in range(NZ):

            @pl.when(step == j)
            def _(j=j):
                run_events(STEPS[2 * j + 1])

        keys = kv[K_HI, at].reshape(GROUP, HEAD)
        values = kv[V_HI, at].reshape(GROUP, HEAD)
        update((ROWS, 2 * ROWS), *state, keys, values, lane_bias(found, mine, False), RUN)

    for head in range(HEADS):
        columns = pl.ds(head * HEAD, HEAD)
        parts = []
        for base in (0, ROWS):
            at = pl.ds(base + head * RUN, RUN)
            total = jnp.sum(l_ref[at, :], axis=1, keepdims=True)
            parts.append(acc_ref[at, :] / total)
        low, high = parts
        out_ref[pl.ds(0, RUN), columns] = jnp.where(swapped, high, low).astype(jnp.bfloat16)
        out_ref[pl.ds(RUN, RUN), columns] = jnp.where(swapped, low, high).astype(jnp.bfloat16)

    for kind in (K_LO, V_LO, RUN_ID, K_HI, V_HI):
        xp, xn, zp, zn = REACH[kind]
        for mx in range(-xn, xp + 1):
            for mz in range(-zn, zp + 1):
                for child in children(kind, mx, mz):
                    copy_to(kind, mx, mz, child).wait_send()


def attend(queries, key_vectors, value_vectors, positions):
    swap = positions[0] > positions[RUN]
    low_run = jnp.minimum(positions[0], positions[RUN]) // RUN
    run_row = jnp.full((1, 1, HEAD), low_run, jnp.int32).astype(jnp.float32)
    swap_row = jnp.full((1, HEAD), swap, jnp.int32).astype(jnp.float32)
    lo_k, hi_k = key_vectors[:RUN], key_vectors[RUN:]
    lo_v, hi_v = value_vectors[:RUN], value_vectors[RUN:]
    own = jnp.stack(
        (
            jnp.where(swap, hi_k, lo_k),
            jnp.where(swap, hi_v, lo_v),
            jnp.where(swap, lo_k, hi_k),
            jnp.where(swap, lo_v, hi_v),
        )
    )
    vmem = pl.BlockSpec(memory_space=pltpu.VMEM)
    return pl.pallas_call(
        attention_kernel,
        out_shape=jax.ShapeDtypeStruct((TOK, HEADS * HEAD), jnp.bfloat16),
        in_specs=[vmem] * 4,
        out_specs=vmem,
        scratch_shapes=[
            pltpu.VMEM((4, NX * NZ, RUN, HEAD), jnp.bfloat16),
            pltpu.VMEM((NX * NZ, 1, HEAD), jnp.float32),
            pltpu.VMEM((2 * ROWS, HEAD), jnp.bfloat16),
            pltpu.VMEM((2 * ROWS, HEAD), jnp.float32),
            pltpu.VMEM((2 * ROWS, HEAD), jnp.float32),
            pltpu.VMEM((2 * ROWS, HEAD), jnp.float32),
            pltpu.SemaphoreType.DMA((N_EVENTS,)),
            pltpu.SemaphoreType.DMA((N_EVENTS,)),
        ],
        compiler_params=pltpu.CompilerParams(collective_id=0, has_side_effects=True),
        name="gather_attend",
    )(queries, own, run_row, swap_row)


def in_order(tiles, dim):
    dims = list(tiles.shape[1:])
    dims[dim] *= tiles.shape[0]
    return jnp.moveaxis(tiles, 0, dim).reshape(dims)


def sent_to_all(x, axis):
    peers = lax.axis_size(axis)
    return lax.all_to_all(jnp.broadcast_to(x[None], (peers, *x.shape)), axis, 0, 0, tiled=True)


def cut_along(x, dim, peers):
    dims = x.shape
    tiles = x.reshape(*dims[:dim], peers, dims[dim] // peers, *dims[dim + 1 :])
    return jnp.moveaxis(tiles, dim, 0)


def on_device(queries, key_vectors, value_vectors, positions, residual, norm_gain, out_weight):
    attended = attend(queries, key_vectors, value_vectors, positions)
    partial_value = jnp.dot(attended, out_weight, preferred_element_type=jnp.float32)
    tiles = lax.all_to_all(
        cut_along(partial_value.astype(jnp.bfloat16), 1, 8), "tp", 0, 0, tiled=True
    )
    summed = jnp.sum(tiles.astype(jnp.float32), axis=0) + residual.astype(jnp.float32)
    square_sum = sent_to_all(jnp.sum(summed * summed, axis=1), "tp").sum(axis=0)
    normed = summed * lax.rsqrt(square_sum / D + 1e-05)[:, None] * norm_gain
    peak_value = sent_to_all(jnp.max(jnp.abs(normed), axis=1), "tp").max(axis=0) + 1e-06
    local_scaled = (normed / peak_value[:, None]).astype(jnp.bfloat16)
    quantized = in_order(sent_to_all(local_scaled, "tp"), 1)
    return (quantized, peak_value, summed.astype(jnp.bfloat16))


def solution(mesh):
    in_specs = (
        P("seq", "tp"),
        P("seq", "tp"),
        P("seq", "tp"),
        P("seq"),
        P("seq", "tp"),
        P(None, "tp"),
        P("tp", None),
    )
    out_specs = (P("seq", None), P("seq"), P("seq", "tp"))
    return jax.shard_map(
        on_device, mesh=mesh, in_specs=in_specs, out_specs=out_specs, check_vma=False
    )
```

```python
import functools
import heapq
import math

import jax
import jax.numpy as jnp
from jax import lax
from jax.experimental import pallas as pl
from jax.experimental.pallas import tpu as pltpu
from jax.sharding import PartitionSpec as P

D = 6144
HEADS = 6
HEAD = 128
TOK = 192
RUN = TOK // 2
NX = 4
NZ = 8
ROWS = HEADS * RUN
GROUP = NX * RUN
CHUNK = 2 * RUN
COLS = HEADS * HEAD
HALF = COLS // 2
N_TP = 8
NY = 4
PARTS = 4
PART = TOK // PARTS
NEG = -1e30
EXP_SCALE = math.log2(math.e) / math.sqrt(HEAD)
MESH = pl.DeviceIdType.MESH

K_LO, V_LO, K_HI, V_HI, RUN_ID = range(5)
X_FIRST = {K_LO: True, V_LO: False, K_HI: True, V_HI: False, RUN_ID: True}
REACH = {
    K_LO: (2, 1, 4, 3),
    V_LO: (2, 1, 4, 3),
    K_HI: (1, 2, 3, 4),
    V_HI: (1, 2, 3, 4),
    RUN_ID: (2, 1, 4, 3),
}
GROUP_ORDER = (0, 1, -1, 2, -2, 3, -3, 4)


def children(kind, mx, mz):
    xp, xn, zp, zn = REACH[kind]
    along_x, along_z = [], []
    if 0 <= mx < xp:
        along_x.append((kind, mx + 1, mz, 0))
    if -xn < mx <= 0:
        along_x.append((kind, mx - 1, mz, 1))
    if 0 <= mz < zp:
        along_z.append((kind, mx, mz + 1, 2))
    if -zn < mz <= 0:
        along_z.append((kind, mx, mz - 1, 3))
    if X_FIRST[kind]:
        return along_z + along_x if mz == 0 else along_z
    return along_x + along_z if mx == 0 else along_x


def plan():
    latency, piece, tiny = 2.2, 0.55, 0.05
    free = [0.0] * 4
    arrivals = []
    order = []

    def send_all(now, kind, mx, mz):
        for child in children(kind, mx, mz):
            direction = child[3]
            took = tiny if kind == RUN_ID else piece
            free[direction] = max(free[direction], now) + took
            heapq.heappush(arrivals, (free[direction] + latency, child[:3]))

    for kind in (K_LO, V_LO, RUN_ID, K_HI, V_HI):
        send_all(0.0, kind, 0, 0)
    units = []
    for dz in GROUP_ORDER:
        units.append((dz, (K_LO, V_LO, RUN_ID), 0.6))
        units.append((dz, (K_HI, V_HI), 0.4))
    have = set()
    now = 0.5
    steps = []
    for dz, kinds, cost in units:
        needed = set()
        for kind in kinds:
            xp, xn, zp, zn = REACH[kind]
            for mx in range(-xn, xp + 1):
                for mz in range(-zn, zp + 1):
                    if (mz - dz) % NZ == 0 and (mx, mz) != (0, 0):
                        needed.add((kind, mx, mz))
        waits = []
        while arrivals and (not needed <= have or arrivals[0][0] <= now):
            when, key = heapq.heappop(arrivals)
            now = max(now, when)
            have.add(key)
            waits.append(key)
            send_all(now, *key)
        now += cost
        steps.append(waits)
    assert not arrivals
    return steps, now


STEPS, PLANNED_US = plan()
EVENT_ID = {key: i for i, key in enumerate(key for waits in STEPS for key in waits)}
N_EVENTS = len(EVENT_ID)


def update(rows, queries, m_ref, l_ref, acc_ref, keys, values, bias, chunk):
    starts = range(rows[0], rows[1], chunk)
    all_scores, all_new, all_factors = [], [], []
    for start in starts:
        scores = lax.dot_general(
            queries[pl.ds(start, chunk), :],
            keys,
            (((1,), (1,)), ((), ())),
            preferred_element_type=jnp.float32,
        )
        scores = scores * EXP_SCALE
        all_scores.append(scores if bias is None else scores + bias)
    for start, scores in zip(starts, all_scores):
        at = pl.ds(start, chunk)
        old = m_ref[at, :]
        new = jnp.maximum(old, jnp.max(scores, axis=1, keepdims=True))
        m_ref[at, :] = new
        all_new.append(new)
        all_factors.append(jnp.exp2(old - new))
    for start, scores, new, factor in zip(starts, all_scores, all_new, all_factors):
        at = pl.ds(start, chunk)
        weights = [
            jnp.exp2(scores[:, i : i + HEAD] - new) for i in range(0, scores.shape[1], HEAD)
        ]
        l_ref[at, :] = l_ref[at, :] * factor + functools.reduce(jnp.add, weights)
        probs = jnp.concatenate([w.astype(jnp.bfloat16) for w in weights], axis=1)
        acc_ref[at, :] = acc_ref[at, :] * factor + jnp.dot(
            probs, values, preferred_element_type=jnp.float32
        )


def first_block(first, queries, m_ref, l_ref, acc_ref, keys, values):
    at = pl.ds(first, ROWS)
    scores = lax.dot_general(
        queries[at, :], keys, (((1,), (1,)), ((), ())), preferred_element_type=jnp.float32
    )
    scores = (scores * EXP_SCALE).reshape(HEADS, RUN, RUN)
    row = lax.broadcasted_iota(jnp.int32, (HEADS, RUN, RUN), 1)
    column = lax.broadcasted_iota(jnp.int32, (HEADS, RUN, RUN), 2)
    scores = jnp.where(column <= row, scores, NEG).reshape(ROWS, RUN)
    high = jnp.max(scores, axis=1, keepdims=True)
    weights = jnp.exp2(scores - high)
    m_ref[at, :] = jnp.broadcast_to(high, (ROWS, HEAD))
    total = jnp.sum(weights, axis=1, keepdims=True)
    lane = lax.broadcasted_iota(jnp.int32, (ROWS, HEAD), 1)
    l_ref[at, :] = jnp.where(lane == 0, total, 0.0)
    acc_ref[at, :] = jnp.dot(
        weights.astype(jnp.bfloat16), values, preferred_element_type=jnp.float32
    )


def lane_bias(ids, mine, low):
    one = [
        jnp.where(ids[j] < mine if low else ids[j] > mine, 0.0, NEG) for j in range(NX)
    ]
    lane = lax.broadcasted_iota(jnp.int32, (1, HEAD), 1)
    tiles = [
        jnp.where(lane < 96, one[0], one[1]),
        jnp.where(lane < 64, one[1], one[2]),
        jnp.where(lane < 32, one[2], one[3]),
    ]
    return jnp.concatenate(tiles, axis=1)


def attention_kernel(
    q_ref, own_ref, run_ref, swap_ref, out_ref, kv, ids, queries, m_ref, l_ref, acc_ref, send, recv
):
    seq = lax.axis_index("seq")
    tp = lax.axis_index("tp")
    x = lax.rem(seq, NX)
    z = seq // NX
    neighbours = (
        z * NX + lax.rem(x + 1, NX),
        z * NX + lax.rem(x + NX - 1, NX),
        lax.rem(z + 1, NZ) * NX + x,
        lax.rem(z + NZ - 1, NZ) * NX + x,
    )

    def source_of(mx, mz):
        return lax.rem(z + 2 * NZ - mz, NZ) * NX + lax.rem(x + 2 * NX - mx, NX)

    def place(kind, index):
        if kind == RUN_ID:
            return ids.at[index]
        return kv.at[kind, index]

    def copy_to(kind, mx, mz, child):
        own = (mx, mz) == (0, 0)
        index = source_of(mx, mz)
        target = place(kind, index)
        if own:
            source = run_ref.at[0] if kind == RUN_ID else own_ref.at[kind]
        else:
            source = target
        event = EVENT_ID[child[:3]]
        return pltpu.make_async_remote_copy(
            src_ref=source,
            dst_ref=target,
            send_sem=send.at[event],
            recv_sem=recv.at[event],
            device_id=(neighbours[child[3]], tp),
            device_id_type=MESH,
        )

    def send_all(kind, mx, mz):
        for child in children(kind, mx, mz):
            copy_to(kind, mx, mz, child).start()

    def run_events(waits):
        for kind, mx, mz in waits:
            target = place(kind, source_of(mx, mz))
            pltpu.make_async_remote_copy(
                src_ref=target,
                dst_ref=target,
                send_sem=send.at[EVENT_ID[(kind, mx, mz)]],
                recv_sem=recv.at[EVENT_ID[(kind, mx, mz)]],
                device_id=(neighbours[0], tp),
                device_id_type=MESH,
            ).wait_recv()
            send_all(kind, mx, mz)

    barrier = pltpu.get_barrier_semaphore()
    for peer in neighbours:
        pl.semaphore_signal(barrier, inc=1, device_id=(peer, tp), device_id_type=MESH)
    pl.semaphore_wait(barrier, 4)

    for kind in (K_LO, V_LO, RUN_ID, K_HI, V_HI):
        send_all(kind, 0, 0)

    swapped = jnp.broadcast_to(swap_ref[...], (RUN, HEAD)) > 0.5
    for head in range(HEADS):
        columns = pl.ds(head * HEAD, HEAD)
        first = q_ref[pl.ds(0, RUN), columns].astype(jnp.float32)
        last = q_ref[pl.ds(RUN, RUN), columns].astype(jnp.float32)
        queries[pl.ds(head * RUN, RUN), :] = jnp.where(swapped, last, first).astype(jnp.bfloat16)
        queries[pl.ds(ROWS + head * RUN, RUN), :] = jnp.where(swapped, first, last).astype(
            jnp.bfloat16
        )
    for kind in (K_LO, V_LO, K_HI, V_HI):
        kv[kind, seq] = own_ref[kind]
    ids[seq] = run_ref[0]
    mine = run_ref[0]

    first_block(0, queries, m_ref, l_ref, acc_ref, own_ref[K_LO], own_ref[V_LO])
    first_block(ROWS, queries, m_ref, l_ref, acc_ref, own_ref[K_HI], own_ref[V_HI])

    @pl.loop(0, NZ)
    def _(step):
        half = (step + 1) // 2
        dz = jnp.where(lax.rem(step, 2) == 1, half, -half)
        group = lax.rem(z + 2 * NZ - dz, NZ) * NX
        for j in range(NZ):

            @pl.when(step == j)
            def _(j=j):
                run_events(STEPS[2 * j])

        at = pl.ds(group, NX)
        found = ids[at]
        keys = kv[K_LO, at].reshape(GROUP, HEAD)
        values = kv[V_LO, at].reshape(GROUP, HEAD)
        state = (queries, m_ref, l_ref, acc_ref)
        update((0, ROWS), *state, keys, values, lane_bias(found, mine, True), CHUNK)
        update((ROWS, 2 * ROWS), *state, keys, values, None, CHUNK)
        for j in range(NZ):

            @pl.when(step == j)
            def _(j=j):
                run_events(STEPS[2 * j + 1])

        keys = kv[K_HI, at].reshape(GROUP, HEAD)
        values = kv[V_HI, at].reshape(GROUP, HEAD)
        update((ROWS, 2 * ROWS), *state, keys, values, lane_bias(found, mine, False), CHUNK)

    for head in range(HEADS):
        columns = pl.ds(head * HEAD, HEAD)
        parts = []
        for base in (0, ROWS):
            at = pl.ds(base + head * RUN, RUN)
            total = jnp.sum(l_ref[at, :], axis=1, keepdims=True)
            parts.append(acc_ref[at, :] / total)
        low, high = parts
        out_ref[pl.ds(0, RUN), columns] = jnp.where(swapped, high, low).astype(jnp.bfloat16)
        out_ref[pl.ds(RUN, RUN), columns] = jnp.where(swapped, low, high).astype(jnp.bfloat16)

    for kind in (K_LO, V_LO, RUN_ID, K_HI, V_HI):
        xp, xn, zp, zn = REACH[kind]
        for mx in range(-xn, xp + 1):
            for mz in range(-zn, zp + 1):
                for child in children(kind, mx, mz):
                    copy_to(kind, mx, mz, child).wait_send()


def attend(queries, key_vectors, value_vectors, positions):
    swap = positions[0] > positions[RUN]
    low_run = jnp.minimum(positions[0], positions[RUN]) // RUN
    run_row = jnp.full((1, 1, HEAD), low_run, jnp.int32).astype(jnp.float32)
    swap_row = jnp.full((1, HEAD), swap, jnp.int32).astype(jnp.float32)
    lo_k, hi_k = key_vectors[:RUN], key_vectors[RUN:]
    lo_v, hi_v = value_vectors[:RUN], value_vectors[RUN:]
    own = jnp.stack(
        (
            jnp.where(swap, hi_k, lo_k),
            jnp.where(swap, hi_v, lo_v),
            jnp.where(swap, lo_k, hi_k),
            jnp.where(swap, lo_v, hi_v),
        )
    )
    vmem = pl.BlockSpec(memory_space=pltpu.VMEM)
    return pl.pallas_call(
        attention_kernel,
        out_shape=jax.ShapeDtypeStruct((TOK, HEADS * HEAD), jnp.bfloat16),
        in_specs=[vmem] * 4,
        out_specs=vmem,
        scratch_shapes=[
            pltpu.VMEM((4, NX * NZ, RUN, HEAD), jnp.bfloat16),
            pltpu.VMEM((NX * NZ, 1, HEAD), jnp.float32),
            pltpu.VMEM((2 * ROWS, HEAD), jnp.bfloat16),
            pltpu.VMEM((2 * ROWS, HEAD), jnp.float32),
            pltpu.VMEM((2 * ROWS, HEAD), jnp.float32),
            pltpu.VMEM((2 * ROWS, HEAD), jnp.float32),
            pltpu.SemaphoreType.DMA((N_EVENTS,)),
            pltpu.SemaphoreType.DMA((N_EVENTS,)),
        ],
        compiler_params=pltpu.CompilerParams(collective_id=0, has_side_effects=True),
        name="gather_attend",
    )(queries, own, run_row, swap_row)


FAR = (2, 1, -1, 0)
ONTO_PARTNER, STEP_UP, STEP_DOWN = range(3)
(
    PAIR_0, PAIR_1, PAIR_2, PAIR_3,
    UP_RELAY, UP_DIRECT, UP_LAST, DOWN_RELAY, DOWN_DIRECT, DOWN_LAST,
    X_UP, X_DOWN, X_UP_FAR, X_DOWN_FAR,
    X_PAIR, X_PAIR_UP, X_PAIR_DOWN, X_PAIR_UP_FAR, X_PAIR_DOWN_FAR,
) = range(19)
N_ARRIVALS = 19


def tail_kernel(
    att_ref, w_ref, residual_ref, gain_ref,
    x_ref, new_ref, factor_ref, scale_ref,
    weights, to_pair, from_pair, mine, outgoing, relayed, got, stats,
    w_sem, send, recv, stat_send, stat_recv,
):
    seq = lax.axis_index("seq")
    tp = lax.axis_index("tp")
    core = lax.rem(tp, 2)
    y = tp // 2
    peers = (
        y * 2 + 1 - core,
        lax.rem(tp + 2, N_TP),
        lax.rem(tp + 6, N_TP),
    )

    def block_of(step, parity):
        return lax.rem(y + step + NY, NY) * 2 + parity

    def columns(step, parity, first=0, width=COLS):
        return pl.ds(pl.multiple_of(block_of(step, parity) * COLS + first, HEAD), width)

    loads = []
    for slot in range(8):
        parity = 1 - core if slot < 4 else core
        load = pltpu.make_async_copy(
            w_ref.at[:, columns(FAR[slot % 4], parity)], weights.at[slot], w_sem.at[slot]
        )
        load.start()
        loads.append(load)

    barrier = pltpu.get_barrier_semaphore()
    for step in range(1, N_TP):
        pl.semaphore_signal(
            barrier, inc=1, device_id=(seq, lax.rem(tp + step, N_TP)), device_id_type=MESH
        )
    pl.semaphore_wait(barrier, N_TP - 1)

    sent = []

    def ship(part, event, source, target, peer):
        copy = pltpu.make_async_remote_copy(
            src_ref=source,
            dst_ref=target,
            send_sem=send.at[part, event],
            recv_sem=recv.at[part, event],
            device_id=(seq, peers[peer]),
            device_id_type=MESH,
        )
        copy.start()
        sent.append(copy)

    def await_arrival(part, event, target):
        pltpu.make_async_remote_copy(
            src_ref=target,
            dst_ref=target,
            send_sem=send.at[part, event],
            recv_sem=recv.at[part, event],
            device_id=(seq, peers[0]),
            device_id_type=MESH,
        ).wait_recv()

    def rows(part):
        return pl.ds(part * PART, PART)

    for slot in range(8):
        loads[slot].wait()
        product = jnp.dot(att_ref[...], weights[slot], preferred_element_type=jnp.float32)
        if slot < 4:
            to_pair[slot] = product.astype(jnp.bfloat16)
            for part in range(PARTS):
                ship(
                    part,
                    PAIR_0 + slot,
                    to_pair.at[slot, rows(part)],
                    from_pair.at[slot, rows(part)],
                    ONTO_PARTNER,
                )
        else:
            mine[slot - 4] = product

    left = pl.ds(0, HALF)
    right = pl.ds(HALF, HALF)

    def slab(event, part):
        return got.at[event - UP_RELAY, rows(part)]

    def pair_sum(part):
        at = rows(part)
        for slot, step in enumerate(FAR):
            await_arrival(part, PAIR_0 + slot, from_pair.at[slot, at])
            total = mine[slot, at, :] + from_pair[slot, at, :].astype(jnp.float32)
            if step == 0:
                mine[slot, at, :] = total
                continue
            outgoing[slot, at, :] = total.astype(jnp.bfloat16)
            here = outgoing.at[slot, at]
            if step == 2:
                ship(part, UP_RELAY, here.at[:, left], slab(UP_RELAY, part), STEP_UP)
                ship(part, DOWN_RELAY, here.at[:, right], slab(DOWN_RELAY, part), STEP_DOWN)
            elif step == 1:
                ship(part, UP_DIRECT, here.at[:, right], slab(UP_DIRECT, part), STEP_UP)
            else:
                ship(part, DOWN_DIRECT, here.at[:, left], slab(DOWN_DIRECT, part), STEP_DOWN)

    def relay_sum(part):
        at = rows(part)
        for way, (arrival, onward, slot, half, peer) in enumerate(
            (
                (UP_RELAY, UP_LAST, 1, left, STEP_UP),
                (DOWN_RELAY, DOWN_LAST, 2, right, STEP_DOWN),
            )
        ):
            await_arrival(part, arrival, slab(arrival, part))
            total = outgoing[slot, at, half].astype(jnp.float32) + slab(arrival, part)[
                ...
            ].astype(jnp.float32)
            relayed[way, at, :] = total.astype(jnp.bfloat16)
            ship(part, onward, relayed.at[way, at], slab(onward, part), peer)

    def finish_sum(part):
        at = rows(part)
        squares = jnp.zeros((PART, HEAD), jnp.float32)
        peak = jnp.zeros((PART, HEAD), jnp.float32)
        for first, direct, last in ((0, DOWN_DIRECT, UP_LAST), (HALF, UP_DIRECT, DOWN_LAST)):
            half = pl.ds(first, HALF)
            await_arrival(part, direct, slab(direct, part))
            await_arrival(part, last, slab(last, part))
            summed = (
                mine[3, at, half]
                + slab(direct, part)[...].astype(jnp.float32)
                + slab(last, part)[...].astype(jnp.float32)
                + residual_ref[at, half].astype(jnp.float32)
            )
            new_ref[at, half] = summed.astype(jnp.bfloat16)
            gained = summed * gain_ref[:, half]
            x_ref[at, columns(0, core, first, HALF)] = gained.astype(jnp.bfloat16)
            for lane in range(0, HALF, HEAD):
                piece = summed[:, lane : lane + HEAD]
                squares = squares + piece * piece
                peak = jnp.maximum(peak, jnp.abs(gained[:, lane : lane + HEAD]))
        block = x_ref.at[at, columns(0, core)]
        ship(part, X_UP, block, block, STEP_UP)
        ship(part, X_DOWN, block, block, STEP_DOWN)
        ship(part, X_PAIR, block, block, ONTO_PARTNER)
        lane = lax.broadcasted_iota(jnp.int32, (PART, HEAD), 1)
        both = jnp.where(
            lane == 0,
            jnp.sum(squares, axis=1, keepdims=True),
            jnp.max(peak, axis=1, keepdims=True),
        )
        both = jnp.concatenate([both, jnp.zeros((HEAD - PART, HEAD), jnp.float32)], axis=0)
        stats[part, tp] = jnp.transpose(both)[0:8, :]
        for step in range(1, N_TP):
            copy = pltpu.make_async_remote_copy(
                src_ref=stats.at[part, tp],
                dst_ref=stats.at[part, tp],
                send_sem=stat_send.at[part, step],
                recv_sem=stat_recv.at[part, step],
                device_id=(seq, lax.rem(tp + step, N_TP)),
                device_id_type=MESH,
            )
            copy.start()
            sent.append(copy)

    def share(part):
        at = rows(part)
        for arrival, far, pair, step, first, peer in (
            (X_UP, X_UP_FAR, X_PAIR_UP, -1, 0, STEP_UP),
            (X_DOWN, X_DOWN_FAR, X_PAIR_DOWN, 1, HALF, STEP_DOWN),
        ):
            block = x_ref.at[at, columns(step, core)]
            await_arrival(part, arrival, block)
            half = x_ref.at[at, columns(step, core, first, HALF)]
            ship(part, far, half, half, peer)
            ship(part, pair, block, block, ONTO_PARTNER)

    def share_far(part):
        at = rows(part)
        for arrival, pair, first in (
            (X_UP_FAR, X_PAIR_UP_FAR, 0),
            (X_DOWN_FAR, X_PAIR_DOWN_FAR, HALF),
        ):
            half = x_ref.at[at, columns(2, core, first, HALF)]
            await_arrival(part, arrival, half)
            ship(part, pair, half, half, ONTO_PARTNER)

    def scales(part):
        at = rows(part)
        for step in range(1, N_TP):
            source = lax.rem(tp + N_TP - step, N_TP)
            pltpu.make_async_remote_copy(
                src_ref=stats.at[part, source],
                dst_ref=stats.at[part, source],
                send_sem=stat_send.at[part, step],
                recv_sem=stat_recv.at[part, step],
                device_id=(seq, peers[0]),
                device_id_type=MESH,
            ).wait_recv()
        total = stats[part, 0, 0:1, :]
        high = stats[part, 0, 1:2, :]
        for source in range(1, N_TP):
            total = total + stats[part, source, 0:1, :]
            high = jnp.maximum(high, stats[part, source, 1:2, :])
        root = lax.rsqrt(total / D + 1e-05)
        scale = high * root + 1e-06
        scale_ref[part] = scale
        factor = jnp.transpose(jnp.broadcast_to(root / scale, (HEAD, HEAD)))
        factor_ref[at, :] = factor[0:PART, :]

    def from_partner(part):
        at = rows(part)
        other = 1 - core
        for event, step, first, width in (
            (X_PAIR, 0, 0, COLS),
            (X_PAIR_UP, -1, 0, COLS),
            (X_PAIR_DOWN, 1, 0, COLS),
            (X_PAIR_UP_FAR, 2, 0, HALF),
            (X_PAIR_DOWN_FAR, 2, HALF, HALF),
        ):
            await_arrival(part, event, x_ref.at[at, columns(step, other, first, width)])

    stages = (pair_sum, relay_sum, finish_sum, share, share_far, scales, from_partner)
    for tick in range(PARTS + len(stages) - 1):
        for depth, stage in enumerate(stages):
            if 0 <= tick - depth < PARTS:
                stage(tick - depth)
    for copy in sent:
        copy.wait_send()


def project_and_share(attended, out_weight, residual, norm_gain):
    vmem = pl.BlockSpec(memory_space=pltpu.VMEM)
    bf16, f32 = jnp.bfloat16, jnp.float32
    return pl.pallas_call(
        tail_kernel,
        out_shape=(
            jax.ShapeDtypeStruct((TOK, D), bf16),
            jax.ShapeDtypeStruct((TOK, COLS), bf16),
            jax.ShapeDtypeStruct((TOK, HEAD), f32),
            jax.ShapeDtypeStruct((PARTS, 1, HEAD), f32),
        ),
        in_specs=[vmem, pl.BlockSpec(memory_space=pl.ANY), vmem, vmem],
        out_specs=[vmem] * 4,
        scratch_shapes=[
            pltpu.VMEM((8, COLS, COLS), bf16),
            pltpu.VMEM((4, TOK, COLS), bf16),
            pltpu.VMEM((4, TOK, COLS), bf16),
            pltpu.VMEM((4, TOK, COLS), f32),
            pltpu.VMEM((3, TOK, COLS), bf16),
            pltpu.VMEM((2, TOK, HALF), bf16),
            pltpu.VMEM((6, TOK, HALF), bf16),
            pltpu.VMEM((PARTS, N_TP, 8, HEAD), f32),
            pltpu.SemaphoreType.DMA((8,)),
            pltpu.SemaphoreType.DMA((PARTS, N_ARRIVALS)),
            pltpu.SemaphoreType.DMA((PARTS, N_ARRIVALS)),
            pltpu.SemaphoreType.DMA((PARTS, N_TP)),
            pltpu.SemaphoreType.DMA((PARTS, N_TP)),
        ],
        compiler_params=pltpu.CompilerParams(
            collective_id=1, has_side_effects=True, vmem_limit_bytes=60 * 2**20
        ),
        name="project_share",
    )(attended, out_weight, residual, norm_gain)


def on_device(queries, key_vectors, value_vectors, positions, residual, norm_gain, out_weight):
    attended = attend(queries, key_vectors, value_vectors, positions)
    shared, new_residual, factor, scale = project_and_share(
        attended, out_weight, residual, norm_gain
    )
    quantized = (shared.astype(jnp.float32) * factor[:, :1]).astype(jnp.bfloat16)
    return (quantized, scale[:, 0, :PART].reshape(TOK), new_residual)


def solution(mesh):
    in_specs = (
        P("seq", "tp"),
        P("seq", "tp"),
        P("seq", "tp"),
        P("seq"),
        P("seq", "tp"),
        P(None, "tp"),
        P("tp", None),
    )
    out_specs = (P("seq", None), P("seq"), P("seq", "tp"))
    return jax.shard_map(
        on_device, mesh=mesh, in_specs=in_specs, out_specs=out_specs, check_vma=False
    )
```

```python
import functools
import heapq
import math

import jax
import jax.numpy as jnp
from jax import lax
from jax.experimental import pallas as pl
from jax.experimental.pallas import tpu as pltpu
from jax.sharding import PartitionSpec as P

D = 6144
HEADS = 6
HEAD = 128
TOK = 192
RUN = TOK // 2
NX = 4
NY = 4
NZ = 8
N_TP = 8
ROWS = HEADS * RUN
GROUP = NX * RUN
CHUNK = 2 * RUN
COLS = HEADS * HEAD
HALF = COLS // 2
PER_HALF = 2
PARTS = 2 * PER_HALF
PART = TOK // PARTS
NEG = -1e30
EXP_SCALE = math.log2(math.e) / math.sqrt(HEAD)
MESH = pl.DeviceIdType.MESH

K_LO, V_LO, K_HI, V_HI, RUN_ID = range(5)
KINDS = (K_LO, V_LO, RUN_ID, K_HI, V_HI)
X_FIRST = {K_LO: True, V_LO: False, K_HI: True, V_HI: False, RUN_ID: True}
REACH = {
    K_LO: (2, 1, 4, 3),
    V_LO: (2, 1, 4, 3),
    K_HI: (1, 2, 3, 4),
    V_HI: (1, 2, 3, 4),
    RUN_ID: (2, 1, 4, 3),
}
LO, HI = 0, 1
FAR = (2, 1, -1, 0)
X_PLUS, X_MINUS, Z_PLUS, Z_MINUS, Y_PLUS, Y_MINUS, PAIR = range(7)
(
    UP_RELAY, UP_DIRECT, UP_LAST, DOWN_RELAY, DOWN_DIRECT, DOWN_LAST,
    X_UP, X_DOWN, X_UP_FAR, X_DOWN_FAR,
    X_PAIR, X_PAIR_UP, X_PAIR_DOWN, X_PAIR_UP_FAR, X_PAIR_DOWN_FAR,
) = range(15)
N_ARRIVALS = 15


def children(kind, mx, mz):
    xp, xn, zp, zn = REACH[kind]
    along_x, along_z = [], []
    if 0 <= mx < xp:
        along_x.append((kind, mx + 1, mz, X_PLUS))
    if -xn < mx <= 0:
        along_x.append((kind, mx - 1, mz, X_MINUS))
    if 0 <= mz < zp:
        along_z.append((kind, mx, mz + 1, Z_PLUS))
    if -zn < mz <= 0:
        along_z.append((kind, mx, mz - 1, Z_MINUS))
    if X_FIRST[kind]:
        return along_z + along_x if mz == 0 else along_z
    return along_x + along_z if mx == 0 else along_x


def moves(kind):
    xp, xn, zp, zn = REACH[kind]
    return [
        (kind, mx, mz)
        for mx in range(-xn, xp + 1)
        for mz in range(-zn, zp + 1)
        if (mx, mz) != (0, 0)
    ]


EVENT_ID = {key: i for i, key in enumerate(key for kind in KINDS for key in moves(kind))}
N_EVENTS = len(EVENT_ID)
UNIT_US = 0.6
PROJECT_US = 0.5
HOP_US = 2.3
PAIR_US = 1.1
PIECE_US = 0.55
PART_US = 1.6 * PART / RUN


def plan():
    tasks = {}
    for kind in KINDS:
        took = 0.04 if kind == RUN_ID else PIECE_US
        for key in [(kind, 0, 0)] + moves(kind):
            sends = [(child[:3], child[3], took) for child in children(*key)]
            own = key[1:] == (0, 0)
            rank = (0 if kind in (K_LO, V_LO, RUN_ID) else 1) + (-2 if own else 0)
            tasks[("relay",) + key] = (rank, [] if own else [key], [], 0.03, sends)
    start = [("relay", kind, 0, 0) for kind in KINDS]
    tasks[("diagonal",)] = (2, [], start, 0.8, [])

    def group_keys(kinds, dz):
        return [k for kind in kinds for k in moves(kind) if (k[2] - dz) % NZ == 0]

    lo_kinds, hi_kinds = (K_LO, V_LO, RUN_ID), (K_HI, V_HI)
    fins = {LO: [("diagonal",)], HI: [("diagonal",)]}
    for i, dz in enumerate((0, 1, -1, 2, -2, 3, -3, 4)):
        for name, kinds, half, base in (
            ("lo_lo", lo_kinds, LO, 20),
            ("hi_lo", lo_kinds, HI, 40),
            ("hi_hi", hi_kinds, HI, 41),
        ):
            keys = group_keys(kinds, dz) + (group_keys((RUN_ID,), dz) if name == "hi_hi" else [])
            task = (name, dz)
            relays = [("relay",) + k for k in keys]
            tasks[task] = (base + 0.1 * i, [], relays + [("diagonal",)], UNIT_US, [])
            fins[half].append(task)
    for half in (LO, HI):
        late = 0.5 * half
        parts = range(half * PER_HALF, (half + 1) * PER_HALF)
        tasks[("attended", half)] = (10, [], fins[half], 0.4, [(("att", half), PAIR, 0.3)])
        for slot, step in enumerate(FAR):
            sends = []
            for part in parts:
                if step == 2:
                    sends += [((part, UP_RELAY), Y_PLUS, PART_US), ((part, DOWN_RELAY), Y_MINUS, PART_US)]
                elif step == 1:
                    sends += [((part, UP_DIRECT), Y_PLUS, PART_US)]
                elif step == -1:
                    sends += [((part, DOWN_DIRECT), Y_MINUS, PART_US)]
            needs = [("attended", half)] if slot == 0 else [("project", half, slot - 1)]
            tasks[("project", half, slot)] = (9 + late, [("att", half)], needs, PROJECT_US, sends)
        for part in parts:
            tasks[("pass_up", part)] = (
                4 + late, [(part, UP_RELAY)], [("project", half, 1)], 0.1,
                [((part, UP_LAST), Y_PLUS, PART_US)],
            )
            tasks[("pass_down", part)] = (
                4 + late, [(part, DOWN_RELAY)], [("project", half, 2)], 0.1,
                [((part, DOWN_LAST), Y_MINUS, PART_US)],
            )
            tasks[("finish", part)] = (
                6 + late,
                [(part, e) for e in (UP_DIRECT, DOWN_DIRECT, UP_LAST, DOWN_LAST)],
                [("project", half, 3)],
                0.4,
                [
                    ((part, X_UP), Y_PLUS, 2 * PART_US),
                    ((part, X_DOWN), Y_MINUS, 2 * PART_US),
                    ((part, X_PAIR), PAIR, 0.15),
                    ((part, "stats"), PAIR, 0.1),
                ],
            )
            tasks[("share_up", part)] = (
                5 + late, [(part, X_UP)], [], 0.03,
                [((part, X_UP_FAR), Y_PLUS, PART_US), ((part, X_PAIR_UP), PAIR, 0.15)],
            )
            tasks[("share_down", part)] = (
                5 + late, [(part, X_DOWN)], [], 0.03,
                [((part, X_DOWN_FAR), Y_MINUS, PART_US), ((part, X_PAIR_DOWN), PAIR, 0.15)],
            )
            tasks[("far_up", part)] = (
                5 + late, [(part, X_UP_FAR)], [], 0.03, [((part, X_PAIR_UP_FAR), PAIR, 0.1)]
            )
            tasks[("far_down", part)] = (
                5 + late, [(part, X_DOWN_FAR)], [], 0.03, [((part, X_PAIR_DOWN_FAR), PAIR, 0.1)]
            )
            tasks[("scales", part)] = (50, [(part, "stats")], [("finish", part)], 0.3, [])
            pairs = (X_PAIR, X_PAIR_UP, X_PAIR_DOWN, X_PAIR_UP_FAR, X_PAIR_DOWN_FAR)
            tasks[("collect", part)] = (60, [(part, e) for e in pairs], [], 0.02, [])

    free = [0.0] * 7
    when = {}
    order, done = [], set()
    left = dict(tasks)
    now = 0.0
    while left:
        best = None
        soonest = None
        for task, (rank, arrivals, needs, cost, sends) in left.items():
            if not all(n in done for n in needs) or not all(a in when for a in arrivals):
                continue
            ready = max([when[a] for a in arrivals], default=0.0)
            if ready <= now:
                if best is None or rank < best[0]:
                    best = (rank, task)
            elif soonest is None or ready < soonest:
                soonest = ready
        if best is None:
            now = soonest
            continue
        task = best[1]
        rank, arrivals, needs, cost, sends = left.pop(task)
        now += cost
        done.add(task)
        order.append((task, now))
        for arrival, link, took in sends:
            free[link] = max(free[link], now) + took
            hop = 3.0 if arrival[-1] == "stats" else PAIR_US if link == PAIR else HOP_US
            when[arrival] = free[link] + hop
    return order, now


ORDER, PLANNED_US = plan()


def update(rows, queries, m_ref, l_ref, acc_ref, keys, values, bias, chunk):
    starts = range(rows[0], rows[1], chunk)
    all_scores, all_new, all_factors = [], [], []
    for start in starts:
        scores = lax.dot_general(
            queries[pl.ds(start, chunk), :],
            keys,
            (((1,), (1,)), ((), ())),
            preferred_element_type=jnp.float32,
        )
        scores = scores * EXP_SCALE
        all_scores.append(scores if bias is None else scores + bias)
    for start, scores in zip(starts, all_scores):
        at = pl.ds(start, chunk)
        old = m_ref[at, :]
        new = jnp.maximum(old, jnp.max(scores, axis=1, keepdims=True))
        m_ref[at, :] = new
        all_new.append(new)
        all_factors.append(jnp.exp2(old - new))
    for start, scores, new, factor in zip(starts, all_scores, all_new, all_factors):
        at = pl.ds(start, chunk)
        weights = [
            jnp.exp2(scores[:, i : i + HEAD] - new) for i in range(0, scores.shape[1], HEAD)
        ]
        l_ref[at, :] = l_ref[at, :] * factor + functools.reduce(jnp.add, weights)
        probs = jnp.concatenate([w.astype(jnp.bfloat16) for w in weights], axis=1)
        acc_ref[at, :] = acc_ref[at, :] * factor + jnp.dot(
            probs, values, preferred_element_type=jnp.float32
        )


def first_block(first, queries, m_ref, l_ref, acc_ref, keys, values):
    at = pl.ds(first, ROWS)
    scores = lax.dot_general(
        queries[at, :], keys, (((1,), (1,)), ((), ())), preferred_element_type=jnp.float32
    )
    scores = (scores * EXP_SCALE).reshape(HEADS, RUN, RUN)
    row = lax.broadcasted_iota(jnp.int32, (HEADS, RUN, RUN), 1)
    column = lax.broadcasted_iota(jnp.int32, (HEADS, RUN, RUN), 2)
    scores = jnp.where(column <= row, scores, NEG).reshape(ROWS, RUN)
    high = jnp.max(scores, axis=1, keepdims=True)
    weights = jnp.exp2(scores - high)
    m_ref[at, :] = jnp.broadcast_to(high, (ROWS, HEAD))
    total = jnp.sum(weights, axis=1, keepdims=True)
    lane = lax.broadcasted_iota(jnp.int32, (ROWS, HEAD), 1)
    l_ref[at, :] = jnp.where(lane == 0, total, 0.0)
    acc_ref[at, :] = jnp.dot(
        weights.astype(jnp.bfloat16), values, preferred_element_type=jnp.float32
    )


def lane_bias(ids, mine, low):
    one = [
        jnp.where(ids[j] < mine if low else ids[j] > mine, 0.0, NEG) for j in range(NX)
    ]
    lane = lax.broadcasted_iota(jnp.int32, (1, HEAD), 1)
    tiles = [
        jnp.where(lane < 96, one[0], one[1]),
        jnp.where(lane < 64, one[1], one[2]),
        jnp.where(lane < 32, one[2], one[3]),
    ]
    return jnp.concatenate(tiles, axis=1)


def fused_kernel(
    pos_ref, q_hbm, k_ref, v_ref, w_ref, residual_hbm, gain_ref,
    x_ref, new_ref, factor_ref, scale_ref,
    q_ref, residual_ref, own, own_id, kv, ids, queries, m_ref, l_ref, acc_ref,
    weights, attended, mine, outgoing, relayed, got, stats,
    load_sem, send, recv, w_send, w_recv, att_send, att_recv,
    part_send, part_recv, stat_send, stat_recv,
):
    seq = lax.axis_index("seq")
    tp = lax.axis_index("tp")
    x = lax.rem(seq, NX)
    z = seq // NX
    core = lax.rem(tp, 2)
    y = tp // 2
    peers = (
        (z * NX + lax.rem(x + 1, NX), tp),
        (z * NX + lax.rem(x + NX - 1, NX), tp),
        (lax.rem(z + 1, NZ) * NX + x, tp),
        (lax.rem(z + NZ - 1, NZ) * NX + x, tp),
        (seq, lax.rem(tp + 2, N_TP)),
        (seq, lax.rem(tp + 6, N_TP)),
        (seq, y * 2 + 1 - core),
    )

    def columns(step, parity, first=0, width=COLS):
        block = lax.rem(y + step + NY, NY) * 2 + parity
        return pl.ds(pl.multiple_of(block * COLS + first, HEAD), width)

    sent = []

    def remote(source, target, send_sem, recv_sem, peer):
        return pltpu.make_async_remote_copy(
            src_ref=source,
            dst_ref=target,
            send_sem=send_sem,
            recv_sem=recv_sem,
            device_id=peer,
            device_id_type=MESH,
        )

    def ship(*args):
        copy = remote(*args)
        copy.start()
        sent.append(copy)

    def arrive(target, send_sem, recv_sem):
        remote(target, target, send_sem, recv_sem, peers[PAIR]).wait_recv()

    loads = [
        pltpu.make_async_copy(q_hbm, q_ref, load_sem.at[0]),
        pltpu.make_async_copy(residual_hbm, residual_ref, load_sem.at[1]),
    ]
    for slot, step in enumerate(FAR):
        loads.append(
            pltpu.make_async_copy(
                w_ref.at[:, columns(step, core)],
                weights.at[slot, pl.ds(0, COLS)],
                load_sem.at[2 + slot],
            )
        )
    for load in loads[:2]:
        load.start()

    first, last = pos_ref[0], pos_ref[RUN]
    low_run = jnp.minimum(first, last) // RUN
    mine_id = jnp.full((1, HEAD), low_run, jnp.int32).astype(jnp.float32)
    swapped = jnp.full((RUN, HEAD), jnp.where(first > last, 1, 0), jnp.int32) > 0

    def pick(ref, columns, half):
        one = ref[pl.ds(0, RUN), columns].astype(jnp.float32)
        two = ref[pl.ds(RUN, RUN), columns].astype(jnp.float32)
        return jnp.where(swapped, two, one) if half == LO else jnp.where(swapped, one, two)

    every = pl.ds(0, HEAD)
    for kind, ref, half in ((K_LO, k_ref, LO), (V_LO, v_ref, LO), (K_HI, k_ref, HI), (V_HI, v_ref, HI)):
        piece = pick(ref, every, half).astype(jnp.bfloat16)
        own[kind] = piece
        kv[kind, seq] = piece
    own_id[0] = mine_id
    ids[seq] = mine_id

    barrier = pltpu.get_barrier_semaphore()
    greeted = list(peers[:4]) + [(seq, lax.rem(tp + step, N_TP)) for step in range(1, N_TP)]
    for peer in greeted:
        pl.semaphore_signal(barrier, inc=1, device_id=peer, device_id_type=MESH)
    pl.semaphore_wait(barrier, len(greeted))

    def source_of(mx, mz):
        return lax.rem(z + 2 * NZ - mz, NZ) * NX + lax.rem(x + 2 * NX - mx, NX)

    def place(kind, index):
        return ids.at[index] if kind == RUN_ID else kv.at[kind, index]

    def relay(kind, mx, mz):
        index = source_of(mx, mz)
        here = place(kind, index)
        source = here
        if (mx, mz) == (0, 0):
            source = own_id.at[0] if kind == RUN_ID else own.at[kind]
        else:
            event = EVENT_ID[(kind, mx, mz)]
            arrive(here, send.at[event], recv.at[event])
        for child in children(kind, mx, mz):
            event = EVENT_ID[child[:3]]
            ship(source, here, send.at[event], recv.at[event], peers[child[3]])

    def diagonal():
        for slot in range(4):
            loads[2 + slot].start()
        for slot, step in enumerate(FAR):
            ship(
                w_ref.at[:, columns(step, 1 - core)],
                weights.at[slot, pl.ds(COLS, COLS)],
                w_send.at[slot],
                w_recv.at[slot],
                peers[PAIR],
            )
        loads[0].wait()
        for head in range(HEADS):
            for half in (LO, HI):
                queries[pl.ds(half * ROWS + head * RUN, RUN), :] = pick(
                    q_ref, pl.ds(head * HEAD, HEAD), half
                ).astype(jnp.bfloat16)
        first_block(0, queries, m_ref, l_ref, acc_ref, own[K_LO], own[V_LO])
        first_block(ROWS, queries, m_ref, l_ref, acc_ref, own[K_HI], own[V_HI])

    def unit(dz, half, low_keys):
        at = pl.ds(lax.rem(z + 2 * NZ - dz, NZ) * NX, NX)
        keys = kv[K_LO if low_keys else K_HI, at].reshape(GROUP, HEAD)
        values = kv[V_LO if low_keys else V_HI, at].reshape(GROUP, HEAD)
        bias = None
        if low_keys == (half == LO):
            bias = lane_bias(ids[at], mine_id, low_keys)
        bounds = (half * ROWS, (half + 1) * ROWS)
        update(bounds, queries, m_ref, l_ref, acc_ref, keys, values, bias, CHUNK)

    def attend_half(half):
        for head in range(HEADS):
            at = pl.ds(half * ROWS + head * RUN, RUN)
            total = jnp.sum(l_ref[at, :], axis=1, keepdims=True)
            attended[half, 0, :, pl.ds(head * HEAD, HEAD)] = (acc_ref[at, :] / total).astype(
                jnp.bfloat16
            )
        ship(
            attended.at[half, 0],
            attended.at[half, 1],
            att_send.at[half],
            att_recv.at[half],
            peers[PAIR],
        )

    def rows(part):
        return pl.ds(part * PART, PART)

    left = pl.ds(0, HALF)
    right = pl.ds(HALF, HALF)

    def slab(event, part):
        return got.at[event, rows(part)]

    def send_part(part, event, source, target, peer):
        ship(source, target, part_send.at[part, event], part_recv.at[part, event], peers[peer])

    def await_part(part, event, target):
        arrive(target, part_send.at[part, event], part_recv.at[part, event])

    def project(half, slot):
        if slot == 0:
            arrive(attended.at[half, 1], att_send.at[half], att_recv.at[half])
        if half == LO:
            loads[2 + slot].wait()
            arrive(weights.at[slot, pl.ds(COLS, COLS)], w_send.at[slot], w_recv.at[slot])
        product = jnp.dot(
            attended[half, 0], weights[slot, pl.ds(0, COLS), :], preferred_element_type=jnp.float32
        ) + jnp.dot(
            attended[half, 1],
            weights[slot, pl.ds(COLS, COLS), :],
            preferred_element_type=jnp.float32,
        )
        step = FAR[slot]
        if step == 0:
            mine[pl.ds(half * RUN, RUN), :] = product
            return
        outgoing[slot, pl.ds(half * RUN, RUN), :] = product.astype(jnp.bfloat16)
        for part in range(half * PER_HALF, (half + 1) * PER_HALF):
            here = outgoing.at[slot, rows(part)]
            if step == 2:
                send_part(part, UP_RELAY, here.at[:, left], slab(UP_RELAY, part), Y_PLUS)
                send_part(part, DOWN_RELAY, here.at[:, right], slab(DOWN_RELAY, part), Y_MINUS)
            elif step == 1:
                send_part(part, UP_DIRECT, here.at[:, right], slab(UP_DIRECT, part), Y_PLUS)
            else:
                send_part(part, DOWN_DIRECT, here.at[:, left], slab(DOWN_DIRECT, part), Y_MINUS)

    def pass_on(part, way):
        arrival, onward, slot, half, peer = (
            (UP_RELAY, UP_LAST, 1, left, Y_PLUS),
            (DOWN_RELAY, DOWN_LAST, 2, right, Y_MINUS),
        )[way]
        at = rows(part)
        await_part(part, arrival, slab(arrival, part))
        total = outgoing[slot, at, half].astype(jnp.float32) + slab(arrival, part)[...].astype(
            jnp.float32
        )
        relayed[way, at, :] = total.astype(jnp.bfloat16)
        send_part(part, onward, relayed.at[way, at], slab(onward, part), peer)

    def finish(part):
        at = rows(part)
        half_of = part // PER_HALF
        if part == 0:
            loads[1].wait()
        squares = jnp.zeros((PART, HEAD), jnp.float32)
        peak = jnp.zeros((PART, HEAD), jnp.float32)
        inside = (part % PER_HALF) * PART
        one, two = pl.ds(inside, PART), pl.ds(RUN + inside, PART)
        turned = swapped[0:PART]
        for first, direct, last in ((0, DOWN_DIRECT, UP_LAST), (HALF, UP_DIRECT, DOWN_LAST)):
            await_part(part, direct, slab(direct, part))
            await_part(part, last, slab(last, part))
            for lane in range(0, HALF, HEAD):
                here = pl.ds(first + lane, HEAD)
                there = pl.ds(lane, HEAD)
                low = residual_ref[one, here].astype(jnp.float32)
                high = residual_ref[two, here].astype(jnp.float32)
                old = jnp.where(turned, high, low) if half_of == LO else jnp.where(turned, low, high)
                summed = (
                    mine[at, here]
                    + slab(direct, part)[:, there].astype(jnp.float32)
                    + slab(last, part)[:, there].astype(jnp.float32)
                    + old
                )
                new_ref[at, here] = summed.astype(jnp.bfloat16)
                gained = summed * gain_ref[:, here]
                x_ref[at, columns(0, core, first + lane, HEAD)] = gained.astype(jnp.bfloat16)
                squares = squares + summed * summed
                peak = jnp.maximum(peak, jnp.abs(gained))
        block = x_ref.at[at, columns(0, core)]
        lane = lax.broadcasted_iota(jnp.int32, (PART, HEAD), 1)
        both = jnp.where(
            lane == 0,
            jnp.sum(squares, axis=1, keepdims=True),
            jnp.max(peak, axis=1, keepdims=True),
        )
        if PART < HEAD:
            both = jnp.concatenate([both, jnp.zeros((HEAD - PART, HEAD), jnp.float32)], axis=0)
        stats[part, tp] = jnp.transpose(both)[0:8, :]
        send_part(part, X_UP, block, block, Y_PLUS)
        send_part(part, X_DOWN, block, block, Y_MINUS)
        send_part(part, X_PAIR, block, block, PAIR)
        for step in range(1, N_TP):
            ship(
                stats.at[part, tp],
                stats.at[part, tp],
                stat_send.at[part, step],
                stat_recv.at[part, step],
                (seq, lax.rem(tp + step, N_TP)),
            )

    def share(part, way):
        arrival, far, pair, step, first, peer = (
            (X_UP, X_UP_FAR, X_PAIR_UP, -1, 0, Y_PLUS),
            (X_DOWN, X_DOWN_FAR, X_PAIR_DOWN, 1, HALF, Y_MINUS),
        )[way]
        at = rows(part)
        block = x_ref.at[at, columns(step, core)]
        await_part(part, arrival, block)
        half = x_ref.at[at, columns(step, core, first, HALF)]
        send_part(part, far, half, half, peer)
        send_part(part, pair, block, block, PAIR)

    def share_far(part, way):
        arrival, pair, first = (
            (X_UP_FAR, X_PAIR_UP_FAR, 0),
            (X_DOWN_FAR, X_PAIR_DOWN_FAR, HALF),
        )[way]
        half = x_ref.at[rows(part), columns(2, core, first, HALF)]
        await_part(part, arrival, half)
        send_part(part, pair, half, half, PAIR)

    def scales(part):
        for step in range(1, N_TP):
            source = lax.rem(tp + N_TP - step, N_TP)
            arrive(stats.at[part, source], stat_send.at[part, step], stat_recv.at[part, step])
        total = stats[part, 0, 0:1, :]
        high = stats[part, 0, 1:2, :]
        for source in range(1, N_TP):
            total = total + stats[part, source, 0:1, :]
            high = jnp.maximum(high, stats[part, source, 1:2, :])
        root = lax.rsqrt(total / D + 1e-05)
        scale = high * root + 1e-06
        scale_ref[part] = scale
        factor = jnp.transpose(jnp.broadcast_to(root / scale, (HEAD, HEAD)))
        factor_ref[rows(part), :] = factor[0:PART, :]

    def collect(part):
        at = rows(part)
        other = 1 - core
        for event, step, first, width in (
            (X_PAIR, 0, 0, COLS),
            (X_PAIR_UP, -1, 0, COLS),
            (X_PAIR_DOWN, 1, 0, COLS),
            (X_PAIR_UP_FAR, 2, 0, HALF),
            (X_PAIR_DOWN_FAR, 2, HALF, HALF),
        ):
            await_part(part, event, x_ref.at[at, columns(step, other, first, width)])

    emit = {
        "relay": relay,
        "diagonal": diagonal,
        "lo_lo": lambda dz: unit(dz, LO, True),
        "hi_lo": lambda dz: unit(dz, HI, True),
        "hi_hi": lambda dz: unit(dz, HI, False),
        "attended": attend_half,
        "project": project,
        "pass_up": lambda part: pass_on(part, 0),
        "pass_down": lambda part: pass_on(part, 1),
        "finish": finish,
        "share_up": lambda part: share(part, 0),
        "share_down": lambda part: share(part, 1),
        "far_up": lambda part: share_far(part, 0),
        "far_down": lambda part: share_far(part, 1),
        "scales": scales,
        "collect": collect,
    }
    for task, _ in ORDER:
        emit[task[0]](*task[1:])
    for copy in sent:
        copy.wait_send()


def fused(positions, queries, keys, values, out_weight, residual, gain):
    vmem = pl.BlockSpec(memory_space=pltpu.VMEM)
    hbm = pl.BlockSpec(memory_space=pl.ANY)
    smem = pl.BlockSpec(memory_space=pltpu.SMEM)
    bf16, f32 = jnp.bfloat16, jnp.float32
    dma = pltpu.SemaphoreType.DMA
    return pl.pallas_call(
        fused_kernel,
        out_shape=(
            jax.ShapeDtypeStruct((TOK, D), bf16),
            jax.ShapeDtypeStruct((TOK, COLS), bf16),
            jax.ShapeDtypeStruct((TOK, HEAD), f32),
            jax.ShapeDtypeStruct((PARTS, 1, HEAD), f32),
        ),
        in_specs=[smem, hbm, vmem, vmem, hbm, hbm, vmem],
        out_specs=[vmem] * 4,
        scratch_shapes=[
            pltpu.VMEM((TOK, COLS), bf16),
            pltpu.VMEM((TOK, COLS), bf16),
            pltpu.VMEM((4, RUN, HEAD), bf16),
            pltpu.VMEM((1, 1, HEAD), f32),
            pltpu.VMEM((4, NX * NZ, RUN, HEAD), bf16),
            pltpu.VMEM((NX * NZ, 1, HEAD), f32),
            pltpu.VMEM((2 * ROWS, HEAD), bf16),
            pltpu.VMEM((2 * ROWS, HEAD), f32),
            pltpu.VMEM((2 * ROWS, HEAD), f32),
            pltpu.VMEM((2 * ROWS, HEAD), f32),
            pltpu.VMEM((4, 2 * COLS, COLS), bf16),
            pltpu.VMEM((2, 2, RUN, COLS), bf16),
            pltpu.VMEM((TOK, COLS), f32),
            pltpu.VMEM((3, TOK, COLS), bf16),
            pltpu.VMEM((2, TOK, HALF), bf16),
            pltpu.VMEM((6, TOK, HALF), bf16),
            pltpu.VMEM((PARTS, N_TP, 8, HEAD), f32),
            dma((6,)),
            dma((N_EVENTS,)),
            dma((N_EVENTS,)),
            dma((4,)),
            dma((4,)),
            dma((2,)),
            dma((2,)),
            dma((PARTS, N_ARRIVALS)),
            dma((PARTS, N_ARRIVALS)),
            dma((PARTS, N_TP)),
            dma((PARTS, N_TP)),
        ],
        compiler_params=pltpu.CompilerParams(
            collective_id=0, has_side_effects=True, vmem_limit_bytes=VMEM_LIMIT
        ),
        name="fused",
    )(positions, queries, keys, values, out_weight, residual, gain)


VMEM_LIMIT = 40 * 2**20
WIDTH = 1536


def final_kernel(pos_ref, x_ref, new_ref, factor_ref, scale_ref, out_ref, row_ref, kept_ref):
    first = (pl.program_id(0) == 0) & (pl.program_id(1) == 0)

    @pl.when(first)
    def _():
        swapped = pos_ref[0] > pos_ref[RUN]
        low = jnp.concatenate([scale_ref[i][:, :PART] for i in range(PER_HALF)], axis=1)
        high = jnp.concatenate([scale_ref[i][:, :PART] for i in range(PER_HALF, PARTS)], axis=1)
        turned = jnp.full((1, RUN), jnp.where(swapped, 1, 0), jnp.int32) > 0
        row_ref[...] = jnp.concatenate(
            [jnp.where(turned, high, low), jnp.where(turned, low, high)], axis=1
        )

    kept_ref[...] = new_ref[...]
    factor = factor_ref[...]
    for lane in range(0, WIDTH, HEAD):
        at = pl.ds(lane, HEAD)
        out_ref[:, at] = (x_ref[:, at].astype(jnp.float32) * factor).astype(jnp.bfloat16)


def finalize(positions, x, new, factor, scale):
    def turned(i, pos):
        return jnp.where(pos[0] > pos[RUN], 1 - i, i)

    return pl.pallas_call(
        final_kernel,
        out_shape=(
            jax.ShapeDtypeStruct((TOK, D), jnp.bfloat16),
            jax.ShapeDtypeStruct((1, TOK), jnp.float32),
            jax.ShapeDtypeStruct((TOK, COLS), jnp.bfloat16),
        ),
        grid_spec=pltpu.PrefetchScalarGridSpec(
            num_scalar_prefetch=1,
            grid=(2, D // WIDTH),
            in_specs=[
                pl.BlockSpec((RUN, WIDTH), lambda i, j, pos: (turned(i, pos), j)),
                pl.BlockSpec((RUN, COLS), lambda i, j, pos: (turned(i, pos), 0)),
                pl.BlockSpec((RUN, HEAD), lambda i, j, pos: (turned(i, pos), 0)),
                pl.BlockSpec((PARTS, 1, HEAD), lambda i, j, pos: (0, 0, 0)),
            ],
            out_specs=[
                pl.BlockSpec((RUN, WIDTH), lambda i, j, pos: (i, j)),
                pl.BlockSpec((1, TOK), lambda i, j, pos: (0, 0)),
                pl.BlockSpec((RUN, COLS), lambda i, j, pos: (i, 0)),
            ],
        ),
        compiler_params=pltpu.CompilerParams(vmem_limit_bytes=16 * 2**20),
        name="final",
    )(positions, x, new, factor, scale)


def on_device(queries, key_vectors, value_vectors, positions, residual, norm_gain, out_weight):
    shared, new, factor, scale = fused(
        positions, queries, key_vectors, value_vectors, out_weight, residual, norm_gain
    )
    quantized, row, new_residual = finalize(positions, shared, new, factor, scale)
    return (quantized, row.reshape(TOK), new_residual)


def solution(mesh):
    in_specs = (
        P("seq", "tp"),
        P("seq", "tp"),
        P("seq", "tp"),
        P("seq"),
        P("seq", "tp"),
        P(None, "tp"),
        P("tp", None),
    )
    out_specs = (P("seq", None), P("seq"), P("seq", "tp"))
    return jax.shard_map(
        on_device, mesh=mesh, in_specs=in_specs, out_specs=out_specs, check_vma=False
    )
```

```python
import functools
import heapq
import math

import jax
import jax.numpy as jnp
from jax import lax
from jax.experimental import pallas as pl
from jax.experimental.pallas import tpu as pltpu
from jax.sharding import PartitionSpec as P

D = 6144
HEADS = 6
HEAD = 128
TOK = 192
RUN = TOK // 2
NX = 4
NY = 4
NZ = 8
N_TP = 8
ROWS = HEADS * RUN
GROUP = NX * RUN
CHUNK = 2 * RUN
COLS = HEADS * HEAD
HALF = COLS // 2
PER_HALF = 2
PARTS = 2 * PER_HALF
PART = TOK // PARTS
NEG = -1e30
EXP_SCALE = math.log2(math.e) / math.sqrt(HEAD)
MESH = pl.DeviceIdType.MESH

K_LO, V_LO, K_HI, V_HI, RUN_ID = range(5)
KINDS = (V_LO, K_LO, RUN_ID, V_HI, K_HI)
X_FIRST = {K_LO: True, V_LO: False, K_HI: True, V_HI: False, RUN_ID: True}
REACH = {
    K_LO: (2, 1, 4, 3),
    V_LO: (2, 1, 4, 3),
    K_HI: (1, 2, 3, 4),
    V_HI: (1, 2, 3, 4),
    RUN_ID: (2, 1, 4, 3),
}
LO, HI = 0, 1
DIRECT = (K_LO, K_HI, RUN_ID, V_LO, V_HI)
for _k in DIRECT:
    REACH[_k] = (2, 1) + REACH[_k][2:]
FAR = (2, 1, -1, 0)
X_PLUS, X_MINUS, Z_PLUS, Z_MINUS, Y_PLUS, Y_MINUS, PAIR, X_FAR = range(8)
(
    UP_RELAY, UP_DIRECT, UP_LAST, DOWN_RELAY, DOWN_DIRECT, DOWN_LAST,
    X_UP, X_DOWN, X_UP_FAR, X_DOWN_FAR,
    X_PAIR, X_PAIR_UP, X_PAIR_DOWN, X_PAIR_UP_FAR, X_PAIR_DOWN_FAR,
) = range(15)
N_ARRIVALS = 15


def children(kind, mx, mz):
    xp, xn, zp, zn = REACH[kind]
    along_x, along_z = [], []
    if kind in DIRECT and mx == 0:
        along_x = [(kind, 1, mz, X_PLUS), (kind, -1, mz, X_MINUS), (kind, 2, mz, X_FAR)]
    if kind in DIRECT:
        xp = xn = 0
    if 0 <= mx < xp:
        along_x.append((kind, mx + 1, mz, X_PLUS))
    if -xn < mx <= 0:
        along_x.append((kind, mx - 1, mz, X_MINUS))
    if 0 <= mz < zp:
        along_z.append((kind, mx, mz + 1, Z_PLUS))
    if -zn < mz <= 0:
        along_z.append((kind, mx, mz - 1, Z_MINUS))
    if X_FIRST[kind]:
        return along_z + along_x if mz == 0 else along_z
    return along_x + along_z if mx == 0 else along_x


def moves(kind):
    xp, xn, zp, zn = REACH[kind]
    return [
        (kind, mx, mz)
        for mx in range(-xn, xp + 1)
        for mz in range(-zn, zp + 1)
        if (mx, mz) != (0, 0)
    ]


EVENT_ID = {key: i for i, key in enumerate(key for kind in KINDS for key in moves(kind))}
N_EVENTS = len(EVENT_ID)
UNIT_US = 0.6
PROJECT_US = 0.5
HOP_US = 2.3
PAIR_US = 1.1
PIECE_US = 0.55
PART_US = 1.6 * PART / RUN


def plan():
    tasks = {}
    for kind in KINDS:
        took = 0.04 if kind == RUN_ID else PIECE_US
        for key in [(kind, 0, 0)] + moves(kind):
            sends = [(child[:3], child[3], took) for child in children(*key)]
            own = key[1:] == (0, 0)
            rank = (0 if kind in (K_LO, V_LO, RUN_ID) else 1) + (-2 if own else 0)
            tasks[("relay",) + key] = (rank, [] if own else [key], [], 0.03, sends)
    start = [("relay", kind, 0, 0) for kind in KINDS]
    tasks[("diagonal",)] = (2, [], start, 0.8, [])

    def group_keys(kinds, dz):
        return [k for kind in kinds for k in moves(kind) if (k[2] - dz) % NZ == 0]

    lo_kinds, hi_kinds = (K_LO, V_LO, RUN_ID), (K_HI, V_HI)
    fins = {LO: [("diagonal",)], HI: [("diagonal",)]}
    for i, dz in enumerate((0, 1, -1, 2, -2, 3, -3, 4)):
        for name, kinds, half, base in (
            ("lo_lo", lo_kinds, LO, 20),
            ("hi_lo", lo_kinds, HI, 40),
            ("hi_hi", hi_kinds, HI, 41),
        ):
            keys = group_keys(kinds, dz) + (group_keys((RUN_ID,), dz) if name == "hi_hi" else [])
            task = (name, dz)
            relays = [("relay",) + k for k in keys]
            tasks[task] = (base + 0.1 * i, [], relays + [("diagonal",)], UNIT_US, [])
            fins[half].append(task)
    for half in (LO, HI):
        late = 0.5 * half
        parts = range(half * PER_HALF, (half + 1) * PER_HALF)
        tasks[("attended", half)] = (10, [], fins[half], 0.4, [(("att", half), PAIR, 0.3)])
        for slot, step in enumerate(FAR):
            sends = []
            for part in parts:
                if step == 2:
                    sends += [((part, UP_RELAY), Y_PLUS, PART_US), ((part, DOWN_RELAY), Y_MINUS, PART_US)]
                elif step == 1:
                    sends += [((part, UP_DIRECT), Y_PLUS, PART_US)]
                elif step == -1:
                    sends += [((part, DOWN_DIRECT), Y_MINUS, PART_US)]
            needs = [("attended", half)] if slot == 0 else [("project", half, slot - 1)]
            tasks[("project", half, slot)] = (9 + late, [("att", half)], needs, PROJECT_US, sends)
        for part in parts:
            tasks[("pass_up", part)] = (
                4 + late, [(part, UP_RELAY)], [("project", half, 1)], 0.1,
                [((part, UP_LAST), Y_PLUS, PART_US)],
            )
            tasks[("pass_down", part)] = (
                4 + late, [(part, DOWN_RELAY)], [("project", half, 2)], 0.1,
                [((part, DOWN_LAST), Y_MINUS, PART_US)],
            )
            tasks[("finish", part)] = (
                6 + late,
                [(part, e) for e in (UP_DIRECT, DOWN_DIRECT, UP_LAST, DOWN_LAST)],
                [("project", half, 3)],
                0.4,
                [
                    ((part, X_UP), Y_PLUS, 2 * PART_US),
                    ((part, X_DOWN), Y_MINUS, 2 * PART_US),
                    ((part, X_PAIR), PAIR, 0.15),
                    ((part, "stats"), PAIR, 0.1),
                ],
            )
            tasks[("share_up", part)] = (
                5 + late, [(part, X_UP)], [], 0.03,
                [((part, X_UP_FAR), Y_PLUS, PART_US), ((part, X_PAIR_UP), PAIR, 0.15)],
            )
            tasks[("share_down", part)] = (
                5 + late, [(part, X_DOWN)], [], 0.03,
                [((part, X_DOWN_FAR), Y_MINUS, PART_US), ((part, X_PAIR_DOWN), PAIR, 0.15)],
            )
            tasks[("far_up", part)] = (
                5 + late, [(part, X_UP_FAR)], [], 0.03, [((part, X_PAIR_UP_FAR), PAIR, 0.1)]
            )
            tasks[("far_down", part)] = (
                5 + late, [(part, X_DOWN_FAR)], [], 0.03, [((part, X_PAIR_DOWN_FAR), PAIR, 0.1)]
            )
            tasks[("scales", part)] = (
                50,
                [(part, "stats")],
                [(far, every) for far in ("far_up", "far_down") for every in range(PARTS)],
                0.3,
                [],
            )
            pairs = (X_PAIR, X_PAIR_UP, X_PAIR_DOWN, X_PAIR_UP_FAR, X_PAIR_DOWN_FAR)
            tasks[("collect", part)] = (60, [(part, e) for e in pairs], [], 0.02, [])

    free = [0.0] * 8
    when = {}
    order, done = [], set()
    left = dict(tasks)
    now = 0.0
    while left:
        best = None
        soonest = None
        for task, (rank, arrivals, needs, cost, sends) in left.items():
            if not all(n in done for n in needs) or not all(a in when for a in arrivals):
                continue
            ready = max([when[a] for a in arrivals], default=0.0)
            if ready <= now:
                if best is None or rank < best[0]:
                    best = (rank, task)
            elif soonest is None or ready < soonest:
                soonest = ready
        if best is None:
            now = soonest
            continue
        task = best[1]
        rank, arrivals, needs, cost, sends = left.pop(task)
        now += cost
        done.add(task)
        order.append((task, now))
        for arrival, link, took in sends:
            if link == X_FAR:
                free[X_PLUS] = max(free[X_PLUS], now) + took
                free[X_MINUS] = max(free[X_MINUS], now) + took
                when[arrival] = max(free[X_PLUS], free[X_MINUS]) + HOP_US + 0.7
                continue
            free[link] = max(free[link], now) + took
            hop = 3.0 if arrival[-1] == "stats" else PAIR_US if link == PAIR else HOP_US
            when[arrival] = free[link] + hop
    return order, now


ORDER, PLANNED_US = plan()


def update(rows, queries, m_ref, l_ref, acc_ref, keys, values, bias, chunk):
    starts = range(rows[0], rows[1], chunk)
    all_scores, all_new, all_factors = [], [], []
    for start in starts:
        scores = lax.dot_general(
            queries[pl.ds(start, chunk), :],
            keys,
            (((1,), (1,)), ((), ())),
            preferred_element_type=jnp.float32,
        )
        scores = scores * EXP_SCALE
        all_scores.append(scores if bias is None else scores + bias)
    for start, scores in zip(starts, all_scores):
        at = pl.ds(start, chunk)
        old = m_ref[at, :]
        new = jnp.maximum(old, jnp.max(scores, axis=1, keepdims=True))
        m_ref[at, :] = new
        all_new.append(new)
        all_factors.append(jnp.exp2(old - new))
    for start, scores, new, factor in zip(starts, all_scores, all_new, all_factors):
        at = pl.ds(start, chunk)
        weights = [
            jnp.exp2(scores[:, i : i + HEAD] - new) for i in range(0, scores.shape[1], HEAD)
        ]
        l_ref[at, :] = l_ref[at, :] * factor + functools.reduce(jnp.add, weights)
        probs = jnp.concatenate([w.astype(jnp.bfloat16) for w in weights], axis=1)
        acc_ref[at, :] = acc_ref[at, :] * factor + jnp.dot(
            probs, values, preferred_element_type=jnp.float32
        )


def first_block(first, queries, m_ref, l_ref, acc_ref, keys, values):
    at = pl.ds(first, ROWS)
    scores = lax.dot_general(
        queries[at, :], keys, (((1,), (1,)), ((), ())), preferred_element_type=jnp.float32
    )
    scores = (scores * EXP_SCALE).reshape(HEADS, RUN, RUN)
    row = lax.broadcasted_iota(jnp.int32, (HEADS, RUN, RUN), 1)
    column = lax.broadcasted_iota(jnp.int32, (HEADS, RUN, RUN), 2)
    scores = jnp.where(column <= row, scores, NEG).reshape(ROWS, RUN)
    high = jnp.max(scores, axis=1, keepdims=True)
    weights = jnp.exp2(scores - high)
    m_ref[at, :] = jnp.broadcast_to(high, (ROWS, HEAD))
    total = jnp.sum(weights, axis=1, keepdims=True)
    lane = lax.broadcasted_iota(jnp.int32, (ROWS, HEAD), 1)
    l_ref[at, :] = jnp.where(lane == 0, total, 0.0)
    acc_ref[at, :] = jnp.dot(
        weights.astype(jnp.bfloat16), values, preferred_element_type=jnp.float32
    )


def lane_bias(ids, mine, low):
    one = [
        jnp.where(ids[j] < mine if low else ids[j] > mine, 0.0, NEG) for j in range(NX)
    ]
    lane = lax.broadcasted_iota(jnp.int32, (1, HEAD), 1)
    tiles = [
        jnp.where(lane < 96, one[0], one[1]),
        jnp.where(lane < 64, one[1], one[2]),
        jnp.where(lane < 32, one[2], one[3]),
    ]
    return jnp.concatenate(tiles, axis=1)


def fused_kernel(
    pos_hbm, q_hbm, k_hbm, v_hbm, w_ref, residual_hbm, gain_hbm,
    x_hbm, new_ref, factor_ref, scale_ref, turn_ref,
    x_ref, pos_ref, q_ref, k_ref, v_ref, residual_ref, gain_ref, own, own_id, kv, ids, queries, m_ref, l_ref, acc_ref,
    weights, attended, mine, outgoing, relayed, got, stats,
    store_sem, early_sem, load_sem, send, recv, w_send, w_recv, att_send, att_recv,
    part_send, part_recv, stat_send, stat_recv,
):
    seq = lax.axis_index("seq")
    tp = lax.axis_index("tp")
    x = lax.rem(seq, NX)
    z = seq // NX
    core = lax.rem(tp, 2)
    y = tp // 2
    peers = (
        (z * NX + lax.rem(x + 1, NX), tp),
        (z * NX + lax.rem(x + NX - 1, NX), tp),
        (lax.rem(z + 1, NZ) * NX + x, tp),
        (lax.rem(z + NZ - 1, NZ) * NX + x, tp),
        (seq, lax.rem(tp + 2, N_TP)),
        (seq, lax.rem(tp + 6, N_TP)),
        (seq, y * 2 + 1 - core),
        (z * NX + lax.rem(x + 2, NX), tp),
    )

    def columns(step, parity, first=0, width=COLS):
        block = lax.rem(y + step + NY, NY) * 2 + parity
        return pl.ds(pl.multiple_of(block * COLS + first, HEAD), width)

    sent = []
    stores = []

    def remote(source, target, send_sem, recv_sem, peer):
        return pltpu.make_async_remote_copy(
            src_ref=source,
            dst_ref=target,
            send_sem=send_sem,
            recv_sem=recv_sem,
            device_id=peer,
            device_id_type=MESH,
        )

    def ship(*args):
        copy = remote(*args)
        copy.start()
        sent.append(copy)

    def arrive(target, send_sem, recv_sem):
        remote(target, target, send_sem, recv_sem, peers[PAIR]).wait_recv()

    loads = [
        pltpu.make_async_copy(q_hbm, q_ref, load_sem.at[0]),
        pltpu.make_async_copy(residual_hbm, residual_ref, load_sem.at[1]),
    ]
    for slot, step in enumerate(FAR):
        loads.append(
            pltpu.make_async_copy(
                w_ref.at[:, columns(step, core)],
                weights.at[slot, pl.ds(0, COLS)],
                load_sem.at[2 + slot],
            )
        )
    early = [
        pltpu.make_async_copy(k_hbm, k_ref, early_sem.at[0]),
        pltpu.make_async_copy(v_hbm, v_ref, early_sem.at[1]),
        pltpu.make_async_copy(pos_hbm, pos_ref, early_sem.at[2]),
        pltpu.make_async_copy(gain_hbm, gain_ref, early_sem.at[3]),
    ]
    for load in early + loads[:2]:
        load.start()

    barrier = pltpu.get_barrier_semaphore()
    greeted = list(peers[:4]) + [peers[X_FAR]] + [(seq, lax.rem(tp + step, N_TP)) for step in range(1, N_TP)]
    for peer in greeted:
        pl.semaphore_signal(barrier, inc=1, device_id=peer, device_id_type=MESH)
    for load in early:
        load.wait()

    first, last = pos_ref[0], pos_ref[RUN]
    low_run = jnp.minimum(first, last) // RUN
    mine_id = jnp.full((1, HEAD), low_run, jnp.int32).astype(jnp.float32)
    swapped = jnp.full((RUN, HEAD), jnp.where(first > last, 1, 0), jnp.int32) > 0

    def pick(ref, columns, half):
        one = ref[pl.ds(0, RUN), columns].astype(jnp.float32)
        two = ref[pl.ds(RUN, RUN), columns].astype(jnp.float32)
        return jnp.where(swapped, two, one) if half == LO else jnp.where(swapped, one, two)

    every = pl.ds(0, HEAD)
    for kind, ref, half in ((K_LO, k_ref, LO), (V_LO, v_ref, LO), (K_HI, k_ref, HI), (V_HI, v_ref, HI)):
        piece = pick(ref, every, half).astype(jnp.bfloat16)
        own[kind] = piece
        kv[kind, seq] = piece
    turn_ref[...] = swapped[0:1].astype(jnp.float32)
    own_id[0] = mine_id
    ids[seq] = mine_id

    pl.semaphore_wait(barrier, len(greeted))

    def source_of(mx, mz):
        return lax.rem(z + 2 * NZ - mz, NZ) * NX + lax.rem(x + 2 * NX - mx, NX)

    def place(kind, index):
        return ids.at[index] if kind == RUN_ID else kv.at[kind, index]

    def relay(kind, mx, mz):
        index = source_of(mx, mz)
        here = place(kind, index)
        source = here
        if (mx, mz) == (0, 0):
            source = own_id.at[0] if kind == RUN_ID else own.at[kind]
        else:
            event = EVENT_ID[(kind, mx, mz)]
            arrive(here, send.at[event], recv.at[event])
        for child in children(kind, mx, mz):
            event = EVENT_ID[child[:3]]
            ship(source, here, send.at[event], recv.at[event], peers[child[3]])

    def diagonal():
        for slot in range(4):
            loads[2 + slot].start()
        for slot, step in enumerate(FAR):
            ship(
                w_ref.at[:, columns(step, 1 - core)],
                weights.at[slot, pl.ds(COLS, COLS)],
                w_send.at[slot],
                w_recv.at[slot],
                peers[PAIR],
            )
        loads[0].wait()
        for head in range(HEADS):
            for half in (LO, HI):
                queries[pl.ds(half * ROWS + head * RUN, RUN), :] = pick(
                    q_ref, pl.ds(head * HEAD, HEAD), half
                ).astype(jnp.bfloat16)
        first_block(0, queries, m_ref, l_ref, acc_ref, own[K_LO], own[V_LO])
        first_block(ROWS, queries, m_ref, l_ref, acc_ref, own[K_HI], own[V_HI])

    def unit(dz, half, low_keys):
        at = pl.ds(lax.rem(z + 2 * NZ - dz, NZ) * NX, NX)
        keys = kv[K_LO if low_keys else K_HI, at].reshape(GROUP, HEAD)
        values = kv[V_LO if low_keys else V_HI, at].reshape(GROUP, HEAD)
        bias = None
        if low_keys == (half == LO):
            bias = lane_bias(ids[at], mine_id, low_keys)
        bounds = (half * ROWS, (half + 1) * ROWS)
        update(bounds, queries, m_ref, l_ref, acc_ref, keys, values, bias, CHUNK)

    def attend_half(half):
        for head in range(HEADS):
            at = pl.ds(half * ROWS + head * RUN, RUN)
            total = jnp.sum(l_ref[at, :], axis=1, keepdims=True)
            attended[half, 0, :, pl.ds(head * HEAD, HEAD)] = (acc_ref[at, :] / total).astype(
                jnp.bfloat16
            )
        ship(
            attended.at[half, 0],
            attended.at[half, 1],
            att_send.at[half],
            att_recv.at[half],
            peers[PAIR],
        )

    def rows(part):
        return pl.ds(part * PART, PART)

    left = pl.ds(0, HALF)
    right = pl.ds(HALF, HALF)

    def slab(event, part):
        return got.at[event, rows(part)]

    def send_part(part, event, source, target, peer):
        ship(source, target, part_send.at[part, event], part_recv.at[part, event], peers[peer])

    def await_part(part, event, target):
        arrive(target, part_send.at[part, event], part_recv.at[part, event])

    def project(half, slot):
        if slot == 0:
            arrive(attended.at[half, 1], att_send.at[half], att_recv.at[half])
        if half == LO:
            loads[2 + slot].wait()
            arrive(weights.at[slot, pl.ds(COLS, COLS)], w_send.at[slot], w_recv.at[slot])
        product = jnp.dot(
            attended[half, 0], weights[slot, pl.ds(0, COLS), :], preferred_element_type=jnp.float32
        ) + jnp.dot(
            attended[half, 1],
            weights[slot, pl.ds(COLS, COLS), :],
            preferred_element_type=jnp.float32,
        )
        step = FAR[slot]
        if step == 0:
            mine[pl.ds(half * RUN, RUN), :] = product
            return
        outgoing[slot, pl.ds(half * RUN, RUN), :] = product.astype(jnp.bfloat16)
        for part in range(half * PER_HALF, (half + 1) * PER_HALF):
            here = outgoing.at[slot, rows(part)]
            if step == 2:
                send_part(part, UP_RELAY, here.at[:, left], slab(UP_RELAY, part), Y_PLUS)
                send_part(part, DOWN_RELAY, here.at[:, right], slab(DOWN_RELAY, part), Y_MINUS)
            elif step == 1:
                send_part(part, UP_DIRECT, here.at[:, right], slab(UP_DIRECT, part), Y_PLUS)
            else:
                send_part(part, DOWN_DIRECT, here.at[:, left], slab(DOWN_DIRECT, part), Y_MINUS)

    def pass_on(part, way):
        arrival, onward, slot, half, peer = (
            (UP_RELAY, UP_LAST, 1, left, Y_PLUS),
            (DOWN_RELAY, DOWN_LAST, 2, right, Y_MINUS),
        )[way]
        at = rows(part)
        await_part(part, arrival, slab(arrival, part))
        total = outgoing[slot, at, half].astype(jnp.float32) + slab(arrival, part)[...].astype(
            jnp.float32
        )
        relayed[way, at, :] = total.astype(jnp.bfloat16)
        send_part(part, onward, relayed.at[way, at], slab(onward, part), peer)

    def finish(part):
        at = rows(part)
        half_of = part // PER_HALF
        if part == 0:
            loads[1].wait()
        squares = jnp.zeros((PART, HEAD), jnp.float32)
        peak = jnp.zeros((PART, HEAD), jnp.float32)
        inside = (part % PER_HALF) * PART
        one, two = pl.ds(inside, PART), pl.ds(RUN + inside, PART)
        turned = swapped[0:PART]
        for first, direct, last in ((0, DOWN_DIRECT, UP_LAST), (HALF, UP_DIRECT, DOWN_LAST)):
            await_part(part, direct, slab(direct, part))
            await_part(part, last, slab(last, part))
            for lane in range(0, HALF, HEAD):
                here = pl.ds(first + lane, HEAD)
                there = pl.ds(lane, HEAD)
                low = residual_ref[one, here].astype(jnp.float32)
                high = residual_ref[two, here].astype(jnp.float32)
                old = jnp.where(turned, high, low) if half_of == LO else jnp.where(turned, low, high)
                summed = (
                    mine[at, here]
                    + slab(direct, part)[:, there].astype(jnp.float32)
                    + slab(last, part)[:, there].astype(jnp.float32)
                    + old
                )
                new_ref[at, here] = summed.astype(jnp.bfloat16)
                gained = summed * gain_ref[:, here]
                x_ref[at, columns(0, core, first + lane, HEAD)] = gained.astype(jnp.bfloat16)
                squares = squares + summed * summed
                peak = jnp.maximum(peak, jnp.abs(gained))
        block = x_ref.at[at, columns(0, core)]
        lane = lax.broadcasted_iota(jnp.int32, (PART, HEAD), 1)
        both = jnp.where(
            lane == 0,
            jnp.sum(squares, axis=1, keepdims=True),
            jnp.max(peak, axis=1, keepdims=True),
        )
        if PART < HEAD:
            both = jnp.concatenate([both, jnp.zeros((HEAD - PART, HEAD), jnp.float32)], axis=0)
        stats[part, tp] = jnp.transpose(both)[0:8, :]
        send_part(part, X_UP, block, block, Y_PLUS)
        send_part(part, X_DOWN, block, block, Y_MINUS)
        send_part(part, X_PAIR, block, block, PAIR)
        for step in range(1, N_TP):
            ship(
                stats.at[part, tp],
                stats.at[part, tp],
                stat_send.at[part, step],
                stat_recv.at[part, step],
                (seq, lax.rem(tp + step, N_TP)),
            )

    def share(part, way):
        arrival, far, pair, step, first, peer = (
            (X_UP, X_UP_FAR, X_PAIR_UP, -1, 0, Y_PLUS),
            (X_DOWN, X_DOWN_FAR, X_PAIR_DOWN, 1, HALF, Y_MINUS),
        )[way]
        at = rows(part)
        block = x_ref.at[at, columns(step, core)]
        await_part(part, arrival, block)
        half = x_ref.at[at, columns(step, core, first, HALF)]
        send_part(part, far, half, half, peer)
        send_part(part, pair, block, block, PAIR)

    def share_far(part, way):
        arrival, pair, first = (
            (X_UP_FAR, X_PAIR_UP_FAR, 0),
            (X_DOWN_FAR, X_PAIR_DOWN_FAR, HALF),
        )[way]
        half = x_ref.at[rows(part), columns(2, core, first, HALF)]
        await_part(part, arrival, half)
        send_part(part, pair, half, half, PAIR)

    def scales(part):
        for step in range(1, N_TP):
            source = lax.rem(tp + N_TP - step, N_TP)
            arrive(stats.at[part, source], stat_send.at[part, step], stat_recv.at[part, step])
        total = stats[part, 0, 0:1, :]
        high = stats[part, 0, 1:2, :]
        for source in range(1, N_TP):
            total = total + stats[part, source, 0:1, :]
            high = jnp.maximum(high, stats[part, source, 1:2, :])
        root = lax.rsqrt(total / D + 1e-05)
        scale = high * root + 1e-06
        scale_ref[part] = scale
        factor = jnp.transpose(jnp.broadcast_to(root / scale, (HEAD, HEAD)))
        factor_ref[rows(part), :] = factor[0:PART, :]

    def collect(part):
        at = rows(part)
        other = 1 - core
        for event, step, first, width in (
            (X_PAIR, 0, 0, COLS),
            (X_PAIR_UP, -1, 0, COLS),
            (X_PAIR_DOWN, 1, 0, COLS),
            (X_PAIR_UP_FAR, 2, 0, HALF),
            (X_PAIR_DOWN_FAR, 2, HALF, HALF),
        ):
            await_part(part, event, x_ref.at[at, columns(step, other, first, width)])
        store = pltpu.make_async_copy(x_ref.at[at], x_hbm.at[at], store_sem.at[part])
        store.start()
        stores.append(store)

    emit = {
        "relay": relay,
        "diagonal": diagonal,
        "lo_lo": lambda dz: unit(dz, LO, True),
        "hi_lo": lambda dz: unit(dz, HI, True),
        "hi_hi": lambda dz: unit(dz, HI, False),
        "attended": attend_half,
        "project": project,
        "pass_up": lambda part: pass_on(part, 0),
        "pass_down": lambda part: pass_on(part, 1),
        "finish": finish,
        "share_up": lambda part: share(part, 0),
        "share_down": lambda part: share(part, 1),
        "far_up": lambda part: share_far(part, 0),
        "far_down": lambda part: share_far(part, 1),
        "scales": scales,
        "collect": collect,
    }
    for task, _ in ORDER:
        emit[task[0]](*task[1:])
    for copy in sent:
        copy.wait_send()
    for store in stores:
        store.wait()


def fused(positions, queries, keys, values, out_weight, residual, gain):
    vmem = pl.BlockSpec(memory_space=pltpu.VMEM)
    hbm = pl.BlockSpec(memory_space=pltpu.HBM)
    bf16, f32 = jnp.bfloat16, jnp.float32
    dma = pltpu.SemaphoreType.DMA
    return pl.pallas_call(
        fused_kernel,
        out_shape=(
            jax.ShapeDtypeStruct((TOK, D), bf16),
            jax.ShapeDtypeStruct((TOK, COLS), bf16),
            jax.ShapeDtypeStruct((TOK, HEAD), f32),
            jax.ShapeDtypeStruct((PARTS, 1, HEAD), f32),
            jax.ShapeDtypeStruct((1, HEAD), f32),
        ),
        in_specs=[hbm] * 7,
        out_specs=[hbm] + [vmem] * 4,
        scratch_shapes=[
            pltpu.VMEM((TOK, D), bf16),
            pltpu.SMEM((TOK,), jnp.int32),
            pltpu.VMEM((TOK, COLS), bf16),
            pltpu.VMEM((TOK, HEAD), bf16),
            pltpu.VMEM((TOK, HEAD), bf16),
            pltpu.VMEM((TOK, COLS), bf16),
            pltpu.VMEM((1, COLS), f32),
            pltpu.VMEM((4, RUN, HEAD), bf16),
            pltpu.VMEM((1, 1, HEAD), f32),
            pltpu.VMEM((4, NX * NZ, RUN, HEAD), bf16),
            pltpu.VMEM((NX * NZ, 1, HEAD), f32),
            pltpu.VMEM((2 * ROWS, HEAD), bf16),
            pltpu.VMEM((2 * ROWS, HEAD), f32),
            pltpu.VMEM((2 * ROWS, HEAD), f32),
            pltpu.VMEM((2 * ROWS, HEAD), f32),
            pltpu.VMEM((4, 2 * COLS, COLS), bf16),
            pltpu.VMEM((2, 2, RUN, COLS), bf16),
            pltpu.VMEM((TOK, COLS), f32),
            pltpu.VMEM((3, TOK, COLS), bf16),
            pltpu.VMEM((2, TOK, HALF), bf16),
            pltpu.VMEM((6, TOK, HALF), bf16),
            pltpu.VMEM((PARTS, N_TP, 8, HEAD), f32),
            dma((PARTS,)),
            dma((4,)),
            dma((6,)),
            dma((N_EVENTS,)),
            dma((N_EVENTS,)),
            dma((4,)),
            dma((4,)),
            dma((2,)),
            dma((2,)),
            dma((PARTS, N_ARRIVALS)),
            dma((PARTS, N_ARRIVALS)),
            dma((PARTS, N_TP)),
            dma((PARTS, N_TP)),
        ],
        compiler_params=pltpu.CompilerParams(
            collective_id=0, has_side_effects=True, vmem_limit_bytes=VMEM_LIMIT
        ),
        name="fused",
    )(positions, queries, keys, values, out_weight, residual, gain)


VMEM_LIMIT = 67043328
STRIP = 32


def final_kernel(
    x_hbm, new_hbm, factor_hbm, scale_hbm, turn_hbm, out_hbm, row_ref, kept_ref,
    x_ref, new_ref, factor_ref, scale_ref, turn_ref, out_ref, load_sem, x_sem, sem,
):
    loads = [
        pltpu.make_async_copy(source, target, load_sem.at[i])
        for i, (source, target) in enumerate(
            (
                (turn_hbm, turn_ref),
                (factor_hbm, factor_ref),
                (scale_hbm, scale_ref),
                (new_hbm, new_ref),
            )
        )
    ]
    strips = []
    for i, start in enumerate(range(0, RUN, STRIP)):
        for j in range(2):
            at = pl.ds(j * RUN + start, STRIP)
            strips.append(
                pltpu.make_async_copy(x_hbm.at[at], x_ref.at[at], x_sem.at[2 * i + j])
            )
    for load in loads[:2] + strips + loads[2:]:
        load.start()
    for load in loads[:2]:
        load.wait()
    turned = jnp.broadcast_to(turn_ref[...], (STRIP, HEAD)) > 0.5
    copies = []
    for start in range(0, RUN, STRIP):
        one, two = pl.ds(start, STRIP), pl.ds(RUN + start, STRIP)
        low, high = factor_ref[one, :], factor_ref[two, :]
        strips[len(copies)].wait()
        strips[len(copies) + 1].wait()

        def lanes(at, low, high, source, target, one=one, two=two):
            a = source[one, at].astype(jnp.float32) * low
            b = source[two, at].astype(jnp.float32) * high
            target[one, at] = jnp.where(turned, b, a).astype(jnp.bfloat16)
            target[two, at] = jnp.where(turned, a, b).astype(jnp.bfloat16)

        for lane in range(0, D, HEAD):
            lanes(pl.ds(lane, HEAD), low, high, x_ref, out_ref)
        for at in (one, two):
            copy = pltpu.make_async_copy(out_ref.at[at], out_hbm.at[at], sem.at[len(copies)])
            copy.start()
            copies.append(copy)
        if start == 0:
            for load in loads[2:]:
                load.wait()
        for lane in range(0, COLS, HEAD):
            lanes(pl.ds(lane, HEAD), 1.0, 1.0, new_ref, kept_ref)
    low = jnp.concatenate([scale_ref[i][:, :PART] for i in range(PER_HALF)], axis=1)
    high = jnp.concatenate([scale_ref[i][:, :PART] for i in range(PER_HALF, PARTS)], axis=1)
    flip = turn_ref[:, :RUN] > 0.5
    row_ref[...] = jnp.concatenate(
        [jnp.where(flip, high, low), jnp.where(flip, low, high)], axis=1
    )
    for copy in copies:
        copy.wait()


def finalize(*operands):
    vmem = pl.BlockSpec(memory_space=pltpu.VMEM)
    hbm = pl.BlockSpec(memory_space=pltpu.HBM)
    return pl.pallas_call(
        final_kernel,
        out_shape=(
            jax.ShapeDtypeStruct((TOK, D), jnp.bfloat16),
            jax.ShapeDtypeStruct((1, TOK), jnp.float32),
            jax.ShapeDtypeStruct((TOK, COLS), jnp.bfloat16),
        ),
        in_specs=[hbm] * 5,
        out_specs=[hbm, vmem, vmem],
        scratch_shapes=[
            pltpu.VMEM((TOK, D), jnp.bfloat16),
            pltpu.VMEM((TOK, COLS), jnp.bfloat16),
            pltpu.VMEM((TOK, HEAD), jnp.float32),
            pltpu.VMEM((PARTS, 1, HEAD), jnp.float32),
            pltpu.VMEM((1, HEAD), jnp.float32),
            pltpu.VMEM((TOK, D), jnp.bfloat16),
            pltpu.SemaphoreType.DMA((4,)),
            pltpu.SemaphoreType.DMA((2 * RUN // STRIP,)),
            pltpu.SemaphoreType.DMA((2 * RUN // STRIP,)),
        ],
        compiler_params=pltpu.CompilerParams(vmem_limit_bytes=VMEM_LIMIT),
        name="final",
    )(*operands)


def on_device(queries, key_vectors, value_vectors, positions, residual, norm_gain, out_weight):
    results = fused(
        positions, queries, key_vectors, value_vectors, out_weight, residual, norm_gain
    )
    quantized, row, new_residual = finalize(*results)
    return (quantized, row.reshape(TOK), new_residual)


def solution(mesh):
    in_specs = (
        P("seq", "tp"),
        P("seq", "tp"),
        P("seq", "tp"),
        P("seq"),
        P("seq", "tp"),
        P(None, "tp"),
        P("tp", None),
    )
    out_specs = (P("seq", None), P("seq"), P("seq", "tp"))
    return jax.shard_map(
        on_device, mesh=mesh, in_specs=in_specs, out_specs=out_specs, check_vma=False
    )
```

```python
import functools
import heapq
import math

import jax
import jax.numpy as jnp
from jax import lax
from jax.experimental import pallas as pl
from jax.experimental.pallas import tpu as pltpu
from jax.sharding import PartitionSpec as P

D = 6144
HEADS = 6
HEAD = 128
TOK = 192
RUN = TOK // 2
NX = 4
NY = 4
NZ = 8
N_TP = 8
ROWS = HEADS * RUN
GROUP = NX * RUN
CHUNK = 2 * RUN
COLS = HEADS * HEAD
HALF = COLS // 2
PER_HALF = 2
PARTS = 2 * PER_HALF
PART = TOK // PARTS
NEG = -1e30
SUM_DIRECT = ()
SHARE_DIRECT = ()
BEFORE_LO = [("pass_up", PARTS - 1), ("pass_down", PARTS - 1)]
EXP_SCALE = math.log2(math.e) / math.sqrt(HEAD)
MESH = pl.DeviceIdType.MESH

K_LO, V_LO, K_HI, V_HI, RUN_ID = range(5)
KINDS = (V_LO, K_LO, RUN_ID, V_HI, K_HI)
X_FIRST = {K_LO: True, V_LO: False, K_HI: True, V_HI: False, RUN_ID: True}
REACH = {
    K_LO: (2, 1, 4, 3),
    V_LO: (2, 1, 4, 3),
    K_HI: (1, 2, 3, 4),
    V_HI: (1, 2, 3, 4),
    RUN_ID: (2, 1, 4, 3),
}
LO, HI = 0, 1
DIRECT = (K_LO, K_HI, RUN_ID, V_LO, V_HI)
for _k in DIRECT:
    REACH[_k] = (2, 1) + REACH[_k][2:]
FAR = (2, 1, -1, 0)
X_PLUS, X_MINUS, Z_PLUS, Z_MINUS, Y_PLUS, Y_MINUS, PAIR, X_FAR, Y_FAR = range(9)
(
    UP_RELAY, UP_DIRECT, UP_LAST, DOWN_RELAY, DOWN_DIRECT, DOWN_LAST,
    X_UP, X_DOWN, X_UP_FAR, X_DOWN_FAR,
    X_PAIR, X_PAIR_UP, X_PAIR_DOWN, X_PAIR_UP_FAR, X_PAIR_DOWN_FAR,
) = range(15)
N_ARRIVALS = 15


def children(kind, mx, mz):
    xp, xn, zp, zn = REACH[kind]
    along_x, along_z = [], []
    if kind in DIRECT and mx == 0:
        along_x = [(kind, 1, mz, X_PLUS), (kind, -1, mz, X_MINUS), (kind, 2, mz, X_FAR)]
    if kind in DIRECT:
        xp = xn = 0
    if 0 <= mx < xp:
        along_x.append((kind, mx + 1, mz, X_PLUS))
    if -xn < mx <= 0:
        along_x.append((kind, mx - 1, mz, X_MINUS))
    if 0 <= mz < zp:
        along_z.append((kind, mx, mz + 1, Z_PLUS))
    if -zn < mz <= 0:
        along_z.append((kind, mx, mz - 1, Z_MINUS))
    if X_FIRST[kind]:
        return along_z + along_x if mz == 0 else along_z
    return along_x + along_z if mx == 0 else along_x


def moves(kind):
    xp, xn, zp, zn = REACH[kind]
    return [
        (kind, mx, mz)
        for mx in range(-xn, xp + 1)
        for mz in range(-zn, zp + 1)
        if (mx, mz) != (0, 0)
    ]


EVENT_ID = {key: i for i, key in enumerate(key for kind in KINDS for key in moves(kind))}
N_EVENTS = len(EVENT_ID)
UNIT_US = 0.6
PROJECT_US = 0.5
HOP_US = 2.3
PAIR_US = 1.1
PIECE_US = 0.55
PART_US = 1.6 * PART / RUN


def plan():
    tasks = {}
    for kind in KINDS:
        took = 0.04 if kind == RUN_ID else PIECE_US
        for key in [(kind, 0, 0)] + moves(kind):
            sends = [(child[:3], child[3], took) for child in children(*key)]
            own = key[1:] == (0, 0)
            rank = (0 if kind in (K_LO, V_LO, RUN_ID) else 1) + (-2 if own else 0)
            tasks[("relay",) + key] = (rank, [] if own else [key], [], 0.03, sends)
    start = [("relay", kind, 0, 0) for kind in KINDS]
    tasks[("diagonal",)] = (2, [], start, 0.8, [])

    def group_keys(kinds, dz):
        return [k for kind in kinds for k in moves(kind) if (k[2] - dz) % NZ == 0]

    lo_kinds, hi_kinds = (K_LO, V_LO, RUN_ID), (K_HI, V_HI)
    fins = {LO: [("diagonal",)], HI: [("diagonal",)]}
    for i, dz in enumerate((0, 1, -1, 2, -2, 3, -3, 4)):
        for name, kinds, half, base in (
            ("lo_lo", lo_kinds, LO, 20),
            ("hi_lo", lo_kinds, HI, 40),
            ("hi_hi", hi_kinds, HI, 41),
        ):
            keys = group_keys(kinds, dz) + (group_keys((RUN_ID,), dz) if name == "hi_hi" else [])
            task = (name, dz)
            relays = [("relay",) + k for k in keys]
            tasks[task] = (base + 0.1 * i, [], relays + [("diagonal",)], UNIT_US, [])
            fins[half].append(task)
    for half in (LO, HI):
        late = 0.5 * half
        parts = range(half * PER_HALF, (half + 1) * PER_HALF)
        tasks[("attended", half)] = (10, [], fins[half], 0.4, [(("att", half), PAIR, 0.3)])
        for slot, step in enumerate(FAR):
            sends = []
            for part in parts:
                if part in SUM_DIRECT:
                    pairs, link = {
                        2: ((UP_RELAY, DOWN_RELAY), Y_FAR),
                        1: ((UP_LAST, UP_DIRECT), Y_PLUS),
                        -1: ((DOWN_DIRECT, DOWN_LAST), Y_MINUS),
                        0: ((), Y_PLUS),
                    }[step]
                    sends += [((part, event), link, PART_US) for event in pairs]
                elif step == 2:
                    sends += [((part, UP_RELAY), Y_PLUS, PART_US), ((part, DOWN_RELAY), Y_MINUS, PART_US)]
                elif step == 1:
                    sends += [((part, UP_DIRECT), Y_PLUS, PART_US)]
                elif step == -1:
                    sends += [((part, DOWN_DIRECT), Y_MINUS, PART_US)]
            needs = [("attended", half)] if slot == 0 else [("project", half, slot - 1)]
            tasks[("project", half, slot)] = (9 + late, [("att", half)], needs, PROJECT_US, sends)
        for part in parts:
            direct = part in SUM_DIRECT
            if not direct:
                tasks[("pass_up", part)] = (
                    4 + late, [(part, UP_RELAY)], [("project", half, 1)], 0.1,
                    [((part, UP_LAST), Y_PLUS, PART_US)],
                )
                tasks[("pass_down", part)] = (
                    4 + late, [(part, DOWN_RELAY)], [("project", half, 2)], 0.1,
                    [((part, DOWN_LAST), Y_MINUS, PART_US)],
                )
            tasks[("finish", part)] = (
                6 + late,
                [
                    (part, e)
                    for e in (UP_DIRECT, DOWN_DIRECT, UP_LAST, DOWN_LAST)
                    + ((UP_RELAY, DOWN_RELAY) if direct else ())
                ],
                [("project", half, 3)],
                0.4,
                [((part, "stats"), PAIR, 0.1)],
            )
            tasks[("publish", part)] = (
                6.1 + late,
                [],
                [("finish", part)] + (BEFORE_LO if half == LO else []),
                0.02,
                [
                    ((part, X_UP), Y_PLUS, 2 * PART_US),
                    ((part, X_DOWN), Y_MINUS, 2 * PART_US),
                    ((part, X_PAIR), PAIR, 0.15),
                ]
                + (
                    [((part, X_UP_FAR), Y_FAR, PART_US), ((part, X_DOWN_FAR), Y_FAR, PART_US)]
                    if part in SHARE_DIRECT
                    else []
                ),
            )
            tasks[("share_up", part)] = (
                5 + late, [(part, X_UP)], [], 0.03,
                [((part, X_PAIR_UP), PAIR, 0.15)]
                + ([] if part in SHARE_DIRECT else [((part, X_UP_FAR), Y_PLUS, PART_US)]),
            )
            tasks[("share_down", part)] = (
                5 + late, [(part, X_DOWN)], [], 0.03,
                [((part, X_PAIR_DOWN), PAIR, 0.15)]
                + ([] if part in SHARE_DIRECT else [((part, X_DOWN_FAR), Y_MINUS, PART_US)]),
            )
            tasks[("far_up", part)] = (
                5 + late, [(part, X_UP_FAR)], [], 0.03, [((part, X_PAIR_UP_FAR), PAIR, 0.1)]
            )
            tasks[("far_down", part)] = (
                5 + late, [(part, X_DOWN_FAR)], [], 0.03, [((part, X_PAIR_DOWN_FAR), PAIR, 0.1)]
            )
            tasks[("scales", part)] = (
                50,
                [(part, "stats")],
                [("publish", part)],
                0.3,
                [],
            )
            pairs = (X_PAIR, X_PAIR_UP, X_PAIR_DOWN, X_PAIR_UP_FAR, X_PAIR_DOWN_FAR)
            tasks[("collect", part)] = (60, [(part, e) for e in pairs], [], 0.02, [])

    free = [0.0] * 9
    when = {}
    order, done = [], set()
    left = dict(tasks)
    now = 0.0
    while left:
        best = None
        soonest = None
        for task, (rank, arrivals, needs, cost, sends) in left.items():
            if not all(n in done for n in needs) or not all(a in when for a in arrivals):
                continue
            ready = max([when[a] for a in arrivals], default=0.0)
            if ready <= now:
                if best is None or rank < best[0]:
                    best = (rank, task)
            elif soonest is None or ready < soonest:
                soonest = ready
        if best is None:
            now = soonest
            continue
        task = best[1]
        rank, arrivals, needs, cost, sends = left.pop(task)
        now += cost
        done.add(task)
        order.append((task, now))
        for arrival, link, took in sends:
            if link in (X_FAR, Y_FAR):
                ways = (X_PLUS, X_MINUS) if link == X_FAR else (Y_PLUS, Y_MINUS)
                for way in ways:
                    free[way] = max(free[way], now) + took
                when[arrival] = max(free[way] for way in ways) + HOP_US + 0.7
                continue
            free[link] = max(free[link], now) + took
            hop = 7.0 if arrival[-1] == "stats" else PAIR_US if link == PAIR else HOP_US
            when[arrival] = free[link] + hop
    return order, now


ORDER, PLANNED_US = plan()


def update(rows, queries, m_ref, l_ref, acc_ref, keys, values, bias, chunk):
    starts = range(rows[0], rows[1], chunk)
    all_scores, all_new, all_factors = [], [], []
    for start in starts:
        scores = lax.dot_general(
            queries[pl.ds(start, chunk), :],
            keys,
            (((1,), (1,)), ((), ())),
            preferred_element_type=jnp.float32,
        )
        scores = scores * EXP_SCALE
        all_scores.append(scores if bias is None else scores + bias)
    for start, scores in zip(starts, all_scores):
        at = pl.ds(start, chunk)
        old = m_ref[at, :]
        new = jnp.maximum(old, jnp.max(scores, axis=1, keepdims=True))
        m_ref[at, :] = new
        all_new.append(new)
        all_factors.append(jnp.exp2(old - new))
    for start, scores, new, factor in zip(starts, all_scores, all_new, all_factors):
        at = pl.ds(start, chunk)
        weights = [
            jnp.exp2(scores[:, i : i + HEAD] - new) for i in range(0, scores.shape[1], HEAD)
        ]
        l_ref[at, :] = l_ref[at, :] * factor + functools.reduce(jnp.add, weights)
        probs = jnp.concatenate([w.astype(jnp.bfloat16) for w in weights], axis=1)
        acc_ref[at, :] = acc_ref[at, :] * factor + jnp.dot(
            probs, values, preferred_element_type=jnp.float32
        )


def first_block(first, queries, m_ref, l_ref, acc_ref, keys, values):
    at = pl.ds(first, ROWS)
    scores = lax.dot_general(
        queries[at, :], keys, (((1,), (1,)), ((), ())), preferred_element_type=jnp.float32
    )
    scores = (scores * EXP_SCALE).reshape(HEADS, RUN, RUN)
    row = lax.broadcasted_iota(jnp.int32, (HEADS, RUN, RUN), 1)
    column = lax.broadcasted_iota(jnp.int32, (HEADS, RUN, RUN), 2)
    scores = jnp.where(column <= row, scores, NEG).reshape(ROWS, RUN)
    high = jnp.max(scores, axis=1, keepdims=True)
    weights = jnp.exp2(scores - high)
    m_ref[at, :] = jnp.broadcast_to(high, (ROWS, HEAD))
    total = jnp.sum(weights, axis=1, keepdims=True)
    lane = lax.broadcasted_iota(jnp.int32, (ROWS, HEAD), 1)
    l_ref[at, :] = jnp.where(lane == 0, total, 0.0)
    acc_ref[at, :] = jnp.dot(
        weights.astype(jnp.bfloat16), values, preferred_element_type=jnp.float32
    )


def lane_bias(ids, mine, low):
    one = [
        jnp.where(ids[j] < mine if low else ids[j] > mine, 0.0, NEG) for j in range(NX)
    ]
    lane = lax.broadcasted_iota(jnp.int32, (1, HEAD), 1)
    tiles = [
        jnp.where(lane < 96, one[0], one[1]),
        jnp.where(lane < 64, one[1], one[2]),
        jnp.where(lane < 32, one[2], one[3]),
    ]
    return jnp.concatenate(tiles, axis=1)


def fused_kernel(
    pos_hbm, q_hbm, k_hbm, v_hbm, w_ref, residual_hbm, gain_hbm,
    x_hbm, new_hbm, factor_hbm, scale_hbm, turn_hbm,
    x_ref, new_ref, factor_ref, scale_ref, turn_ref, pos_ref, q_ref, k_ref, v_ref, residual_ref, gain_ref, own, own_id, kv, ids, queries, m_ref, l_ref, acc_ref,
    weights, attended, mine, outgoing, relayed, got, stats,
    store_sem, small_sem, early_sem, load_sem, send, recv, w_send, w_recv, att_send, att_recv,
    part_send, part_recv, stat_send, stat_recv,
):
    seq = lax.axis_index("seq")
    tp = lax.axis_index("tp")
    x = lax.rem(seq, NX)
    z = seq // NX
    core = lax.rem(tp, 2)
    y = tp // 2
    peers = (
        (z * NX + lax.rem(x + 1, NX), tp),
        (z * NX + lax.rem(x + NX - 1, NX), tp),
        (lax.rem(z + 1, NZ) * NX + x, tp),
        (lax.rem(z + NZ - 1, NZ) * NX + x, tp),
        (seq, lax.rem(tp + 2, N_TP)),
        (seq, lax.rem(tp + 6, N_TP)),
        (seq, y * 2 + 1 - core),
        (z * NX + lax.rem(x + 2, NX), tp),
        (seq, lax.rem(tp + 4, N_TP)),
    )

    def columns(step, parity, first=0, width=COLS):
        block = lax.rem(y + step + NY, NY) * 2 + parity
        return pl.ds(pl.multiple_of(block * COLS + first, HEAD), width)

    sent = []
    stores = []

    def keep(source, target, sem):
        store = pltpu.make_async_copy(source, target, sem)
        store.start()
        stores.append(store)

    def remote(source, target, send_sem, recv_sem, peer):
        return pltpu.make_async_remote_copy(
            src_ref=source,
            dst_ref=target,
            send_sem=send_sem,
            recv_sem=recv_sem,
            device_id=peer,
            device_id_type=MESH,
        )

    def ship(*args):
        copy = remote(*args)
        copy.start()
        sent.append(copy)

    def arrive(target, send_sem, recv_sem):
        remote(target, target, send_sem, recv_sem, peers[PAIR]).wait_recv()

    loads = [
        pltpu.make_async_copy(q_hbm, q_ref, load_sem.at[0]),
        pltpu.make_async_copy(residual_hbm, residual_ref, load_sem.at[1]),
    ]
    for slot, step in enumerate(FAR):
        loads.append(
            pltpu.make_async_copy(
                w_ref.at[:, columns(step, core)],
                weights.at[slot, pl.ds(0, COLS)],
                load_sem.at[2 + slot],
            )
        )
    early = [
        pltpu.make_async_copy(k_hbm, k_ref, early_sem.at[0]),
        pltpu.make_async_copy(v_hbm, v_ref, early_sem.at[1]),
        pltpu.make_async_copy(pos_hbm, pos_ref, early_sem.at[2]),
        pltpu.make_async_copy(gain_hbm, gain_ref, early_sem.at[3]),
    ]
    for load in early + loads[:2]:
        load.start()

    barrier = pltpu.get_barrier_semaphore()
    greeted = list(peers[:4]) + [peers[X_FAR]] + [(seq, lax.rem(tp + step, N_TP)) for step in range(1, N_TP)]
    for peer in greeted:
        pl.semaphore_signal(barrier, inc=1, device_id=peer, device_id_type=MESH)
    for load in early:
        load.wait()

    first, last = pos_ref[0], pos_ref[RUN]
    low_run = jnp.minimum(first, last) // RUN
    mine_id = jnp.full((1, HEAD), low_run, jnp.int32).astype(jnp.float32)
    swapped = jnp.full((RUN, HEAD), jnp.where(first > last, 1, 0), jnp.int32) > 0

    def pick(ref, columns, half):
        one = ref[pl.ds(0, RUN), columns].astype(jnp.float32)
        two = ref[pl.ds(RUN, RUN), columns].astype(jnp.float32)
        return jnp.where(swapped, two, one) if half == LO else jnp.where(swapped, one, two)

    every = pl.ds(0, HEAD)
    for kind, ref, half in ((K_LO, k_ref, LO), (V_LO, v_ref, LO), (K_HI, k_ref, HI), (V_HI, v_ref, HI)):
        piece = pick(ref, every, half).astype(jnp.bfloat16)
        own[kind] = piece
        kv[kind, seq] = piece
    turn_ref[...] = swapped[0:1].astype(jnp.float32)
    own_id[0] = mine_id
    ids[seq] = mine_id

    pl.semaphore_wait(barrier, len(greeted))

    def source_of(mx, mz):
        return lax.rem(z + 2 * NZ - mz, NZ) * NX + lax.rem(x + 2 * NX - mx, NX)

    def place(kind, index):
        return ids.at[index] if kind == RUN_ID else kv.at[kind, index]

    def relay(kind, mx, mz):
        index = source_of(mx, mz)
        here = place(kind, index)
        source = here
        if (mx, mz) == (0, 0):
            source = own_id.at[0] if kind == RUN_ID else own.at[kind]
        else:
            event = EVENT_ID[(kind, mx, mz)]
            arrive(here, send.at[event], recv.at[event])
        for child in children(kind, mx, mz):
            event = EVENT_ID[child[:3]]
            ship(source, here, send.at[event], recv.at[event], peers[child[3]])

    def diagonal():
        for slot in range(4):
            loads[2 + slot].start()
        for slot, step in enumerate(FAR):
            ship(
                w_ref.at[:, columns(step, 1 - core)],
                weights.at[slot, pl.ds(COLS, COLS)],
                w_send.at[slot],
                w_recv.at[slot],
                peers[PAIR],
            )
        loads[0].wait()
        for head in range(HEADS):
            for half in (LO, HI):
                queries[pl.ds(half * ROWS + head * RUN, RUN), :] = pick(
                    q_ref, pl.ds(head * HEAD, HEAD), half
                ).astype(jnp.bfloat16)
        first_block(0, queries, m_ref, l_ref, acc_ref, own[K_LO], own[V_LO])
        first_block(ROWS, queries, m_ref, l_ref, acc_ref, own[K_HI], own[V_HI])

    def unit(dz, half, low_keys):
        at = pl.ds(lax.rem(z + 2 * NZ - dz, NZ) * NX, NX)
        keys = kv[K_LO if low_keys else K_HI, at].reshape(GROUP, HEAD)
        values = kv[V_LO if low_keys else V_HI, at].reshape(GROUP, HEAD)
        bias = None
        if low_keys == (half == LO):
            bias = lane_bias(ids[at], mine_id, low_keys)
        bounds = (half * ROWS, (half + 1) * ROWS)
        update(bounds, queries, m_ref, l_ref, acc_ref, keys, values, bias, CHUNK)

    def attend_half(half):
        for head in range(HEADS):
            at = pl.ds(half * ROWS + head * RUN, RUN)
            total = jnp.sum(l_ref[at, :], axis=1, keepdims=True)
            attended[half, 0, :, pl.ds(head * HEAD, HEAD)] = (acc_ref[at, :] / total).astype(
                jnp.bfloat16
            )
        ship(
            attended.at[half, 0],
            attended.at[half, 1],
            att_send.at[half],
            att_recv.at[half],
            peers[PAIR],
        )

    def rows(part):
        return pl.ds(part * PART, PART)

    left = pl.ds(0, HALF)
    right = pl.ds(HALF, HALF)

    def slab(event, part):
        return got.at[event, rows(part)]

    def send_part(part, event, source, target, peer):
        ship(source, target, part_send.at[part, event], part_recv.at[part, event], peers[peer])

    def await_part(part, event, target):
        arrive(target, part_send.at[part, event], part_recv.at[part, event])

    def project(half, slot):
        if slot == 0:
            arrive(attended.at[half, 1], att_send.at[half], att_recv.at[half])
        if half == LO:
            loads[2 + slot].wait()
            arrive(weights.at[slot, pl.ds(COLS, COLS)], w_send.at[slot], w_recv.at[slot])
        product = jnp.dot(
            attended[half, 0], weights[slot, pl.ds(0, COLS), :], preferred_element_type=jnp.float32
        ) + jnp.dot(
            attended[half, 1],
            weights[slot, pl.ds(COLS, COLS), :],
            preferred_element_type=jnp.float32,
        )
        step = FAR[slot]
        if step == 0:
            mine[pl.ds(half * RUN, RUN), :] = product
            return
        outgoing[slot, pl.ds(half * RUN, RUN), :] = product.astype(jnp.bfloat16)
        for part in range(half * PER_HALF, (half + 1) * PER_HALF):
            here = outgoing.at[slot, rows(part)]
            if part in SUM_DIRECT:
                (first, second), peer = {
                    2: ((UP_RELAY, DOWN_RELAY), Y_FAR),
                    1: ((UP_LAST, UP_DIRECT), Y_PLUS),
                    -1: ((DOWN_DIRECT, DOWN_LAST), Y_MINUS),
                }[step]
                send_part(part, first, here.at[:, left], slab(first, part), peer)
                send_part(part, second, here.at[:, right], slab(second, part), peer)
            elif step == 2:
                send_part(part, UP_RELAY, here.at[:, left], slab(UP_RELAY, part), Y_PLUS)
                send_part(part, DOWN_RELAY, here.at[:, right], slab(DOWN_RELAY, part), Y_MINUS)
            elif step == 1:
                send_part(part, UP_DIRECT, here.at[:, right], slab(UP_DIRECT, part), Y_PLUS)
            else:
                send_part(part, DOWN_DIRECT, here.at[:, left], slab(DOWN_DIRECT, part), Y_MINUS)

    def pass_on(part, way):
        arrival, onward, slot, half, peer = (
            (UP_RELAY, UP_LAST, 1, left, Y_PLUS),
            (DOWN_RELAY, DOWN_LAST, 2, right, Y_MINUS),
        )[way]
        at = rows(part)
        await_part(part, arrival, slab(arrival, part))
        total = outgoing[slot, at, half].astype(jnp.float32) + slab(arrival, part)[...].astype(
            jnp.float32
        )
        relayed[way, at, :] = total.astype(jnp.bfloat16)
        send_part(part, onward, relayed.at[way, at], slab(onward, part), peer)

    def finish(part):
        at = rows(part)
        half_of = part // PER_HALF
        if part == 0:
            loads[1].wait()
        squares = jnp.zeros((PART, HEAD), jnp.float32)
        peak = jnp.zeros((PART, HEAD), jnp.float32)
        inside = (part % PER_HALF) * PART
        one, two = pl.ds(inside, PART), pl.ds(RUN + inside, PART)
        turned = swapped[0:PART]
        for first, *events in (
            (0, DOWN_DIRECT, UP_LAST, UP_RELAY),
            (HALF, UP_DIRECT, DOWN_LAST, DOWN_RELAY),
        ):
            events = events if part in SUM_DIRECT else events[:2]
            for event in events:
                await_part(part, event, slab(event, part))
            for lane in range(0, HALF, HEAD):
                here = pl.ds(first + lane, HEAD)
                there = pl.ds(lane, HEAD)
                low = residual_ref[one, here].astype(jnp.float32)
                high = residual_ref[two, here].astype(jnp.float32)
                old = jnp.where(turned, high, low) if half_of == LO else jnp.where(turned, low, high)
                summed = mine[at, here] + old
                for event in events:
                    summed = summed + slab(event, part)[:, there].astype(jnp.float32)
                new_ref[at, here] = summed.astype(jnp.bfloat16)
                gained = summed * gain_ref[:, here]
                x_ref[at, columns(0, core, first + lane, HEAD)] = gained.astype(jnp.bfloat16)
                squares = squares + summed * summed
                peak = jnp.maximum(peak, jnp.abs(gained))
        lane = lax.broadcasted_iota(jnp.int32, (PART, HEAD), 1)
        both = jnp.where(
            lane == 0,
            jnp.sum(squares, axis=1, keepdims=True),
            jnp.max(peak, axis=1, keepdims=True),
        )
        if PART < HEAD:
            both = jnp.concatenate([both, jnp.zeros((HEAD - PART, HEAD), jnp.float32)], axis=0)
        stats[part, tp] = jnp.transpose(both)[0:8, :]
        for step in range(1, N_TP):
            ship(
                stats.at[part, tp],
                stats.at[part, tp],
                stat_send.at[part, step],
                stat_recv.at[part, step],
                (seq, lax.rem(tp + step, N_TP)),
            )

    def publish(part):
        at = rows(part)
        keep(new_ref.at[at], new_hbm.at[at], small_sem.at[2, part])
        if part == 0:
            keep(turn_ref, turn_hbm, early_sem.at[4])
        block = x_ref.at[at, columns(0, core)]
        send_part(part, X_UP, block, block, Y_PLUS)
        send_part(part, X_DOWN, block, block, Y_MINUS)
        if part in SHARE_DIRECT:
            for event, first in ((X_UP_FAR, 0), (X_DOWN_FAR, HALF)):
                half = x_ref.at[at, columns(0, core, first, HALF)]
                send_part(part, event, half, half, Y_FAR)
        send_part(part, X_PAIR, block, block, PAIR)

    def share(part, way):
        arrival, far, pair, step, first, peer = (
            (X_UP, X_UP_FAR, X_PAIR_UP, -1, 0, Y_PLUS),
            (X_DOWN, X_DOWN_FAR, X_PAIR_DOWN, 1, HALF, Y_MINUS),
        )[way]
        at = rows(part)
        block = x_ref.at[at, columns(step, core)]
        await_part(part, arrival, block)
        if part not in SHARE_DIRECT:
            half = x_ref.at[at, columns(step, core, first, HALF)]
            send_part(part, far, half, half, peer)
        send_part(part, pair, block, block, PAIR)

    def share_far(part, way):
        arrival, pair, first = (
            (X_UP_FAR, X_PAIR_UP_FAR, 0),
            (X_DOWN_FAR, X_PAIR_DOWN_FAR, HALF),
        )[way]
        half = x_ref.at[rows(part), columns(2, core, first, HALF)]
        await_part(part, arrival, half)
        send_part(part, pair, half, half, PAIR)

    def scales(part):
        for step in range(1, N_TP):
            source = lax.rem(tp + N_TP - step, N_TP)
            arrive(stats.at[part, source], stat_send.at[part, step], stat_recv.at[part, step])
        total = stats[part, 0, 0:1, :]
        high = stats[part, 0, 1:2, :]
        for source in range(1, N_TP):
            total = total + stats[part, source, 0:1, :]
            high = jnp.maximum(high, stats[part, source, 1:2, :])
        root = lax.rsqrt(total / D + 1e-05)
        scale = high * root + 1e-06
        scale_ref[part] = scale
        factor = jnp.transpose(jnp.broadcast_to(root / scale, (HEAD, HEAD)))
        factor_ref[rows(part), :] = factor[0:PART, :]
        keep(scale_ref.at[part], scale_hbm.at[part], small_sem.at[0, part])
        keep(factor_ref.at[rows(part)], factor_hbm.at[rows(part)], small_sem.at[1, part])

    def collect(part):
        at = rows(part)
        other = 1 - core
        for event, step, first, width in (
            (X_PAIR, 0, 0, COLS),
            (X_PAIR_UP, -1, 0, COLS),
            (X_PAIR_DOWN, 1, 0, COLS),
            (X_PAIR_UP_FAR, 2, 0, HALF),
            (X_PAIR_DOWN_FAR, 2, HALF, HALF),
        ):
            await_part(part, event, x_ref.at[at, columns(step, other, first, width)])
        keep(x_ref.at[at], x_hbm.at[at], store_sem.at[part])

    emit = {
        "relay": relay,
        "diagonal": diagonal,
        "lo_lo": lambda dz: unit(dz, LO, True),
        "hi_lo": lambda dz: unit(dz, HI, True),
        "hi_hi": lambda dz: unit(dz, HI, False),
        "attended": attend_half,
        "project": project,
        "pass_up": lambda part: pass_on(part, 0),
        "pass_down": lambda part: pass_on(part, 1),
        "finish": finish,
        "publish": publish,
        "share_up": lambda part: share(part, 0),
        "share_down": lambda part: share(part, 1),
        "far_up": lambda part: share_far(part, 0),
        "far_down": lambda part: share_far(part, 1),
        "scales": scales,
        "collect": collect,
    }
    for task, _ in ORDER:
        emit[task[0]](*task[1:])
    for copy in sent:
        copy.wait_send()
    for store in stores:
        store.wait()


def fused(positions, queries, keys, values, out_weight, residual, gain):
    hbm = pl.BlockSpec(memory_space=pltpu.HBM)
    bf16, f32 = jnp.bfloat16, jnp.float32
    dma = pltpu.SemaphoreType.DMA
    return pl.pallas_call(
        fused_kernel,
        out_shape=(
            jax.ShapeDtypeStruct((TOK, D), bf16),
            jax.ShapeDtypeStruct((TOK, COLS), bf16),
            jax.ShapeDtypeStruct((TOK, HEAD), f32),
            jax.ShapeDtypeStruct((PARTS, 1, HEAD), f32),
            jax.ShapeDtypeStruct((1, HEAD), f32),
        ),
        in_specs=[hbm] * 7,
        out_specs=[hbm] * 5,
        scratch_shapes=[
            pltpu.VMEM((TOK, D), bf16),
            pltpu.VMEM((TOK, COLS), bf16),
            pltpu.VMEM((TOK, HEAD), f32),
            pltpu.VMEM((PARTS, 1, HEAD), f32),
            pltpu.VMEM((1, HEAD), f32),
            pltpu.SMEM((TOK,), jnp.int32),
            pltpu.VMEM((TOK, COLS), bf16),
            pltpu.VMEM((TOK, HEAD), bf16),
            pltpu.VMEM((TOK, HEAD), bf16),
            pltpu.VMEM((TOK, COLS), bf16),
            pltpu.VMEM((1, COLS), f32),
            pltpu.VMEM((4, RUN, HEAD), bf16),
            pltpu.VMEM((1, 1, HEAD), f32),
            pltpu.VMEM((4, NX * NZ, RUN, HEAD), bf16),
            pltpu.VMEM((NX * NZ, 1, HEAD), f32),
            pltpu.VMEM((2 * ROWS, HEAD), bf16),
            pltpu.VMEM((2 * ROWS, HEAD), f32),
            pltpu.VMEM((2 * ROWS, HEAD), f32),
            pltpu.VMEM((2 * ROWS, HEAD), f32),
            pltpu.VMEM((4, 2 * COLS, COLS), bf16),
            pltpu.VMEM((2, 2, RUN, COLS), bf16),
            pltpu.VMEM((TOK, COLS), f32),
            pltpu.VMEM((3, TOK, COLS), bf16),
            pltpu.VMEM((2, TOK, HALF), bf16),
            pltpu.VMEM((6, TOK, HALF), bf16),
            pltpu.VMEM((PARTS, N_TP, 8, HEAD), f32),
            dma((PARTS,)),
            dma((3, PARTS)),
            dma((5,)),
            dma((6,)),
            dma((N_EVENTS,)),
            dma((N_EVENTS,)),
            dma((4,)),
            dma((4,)),
            dma((2,)),
            dma((2,)),
            dma((PARTS, N_ARRIVALS)),
            dma((PARTS, N_ARRIVALS)),
            dma((PARTS, N_TP)),
            dma((PARTS, N_TP)),
        ],
        compiler_params=pltpu.CompilerParams(
            collective_id=0, has_side_effects=True, vmem_limit_bytes=VMEM_LIMIT
        ),
        name="fused",
    )(positions, queries, keys, values, out_weight, residual, gain)


VMEM_LIMIT = 67043328
STRIP = 32


def final_kernel(
    x_hbm, new_hbm, factor_hbm, scale_hbm, turn_hbm, out_hbm, row_ref, kept_ref,
    x_ref, new_ref, factor_ref, scale_ref, turn_ref, out_ref, load_sem, x_sem, sem,
):
    loads = [
        pltpu.make_async_copy(source, target, load_sem.at[i])
        for i, (source, target) in enumerate(
            (
                (turn_hbm, turn_ref),
                (factor_hbm, factor_ref),
                (scale_hbm, scale_ref),
                (new_hbm, new_ref),
            )
        )
    ]
    strips = []
    for i, start in enumerate(range(0, RUN, STRIP)):
        for j in range(2):
            at = pl.ds(j * RUN + start, STRIP)
            strips.append(
                pltpu.make_async_copy(x_hbm.at[at], x_ref.at[at], x_sem.at[2 * i + j])
            )
    for load in loads[:2] + strips + loads[2:]:
        load.start()
    for load in loads[:2]:
        load.wait()
    turned = jnp.broadcast_to(turn_ref[...], (STRIP, HEAD)) > 0.5
    copies = []
    for start in range(0, RUN, STRIP):
        one, two = pl.ds(start, STRIP), pl.ds(RUN + start, STRIP)
        low, high = factor_ref[one, :], factor_ref[two, :]
        strips[len(copies)].wait()
        strips[len(copies) + 1].wait()

        def lanes(at, low, high, source, target, one=one, two=two):
            a = source[one, at].astype(jnp.float32) * low
            b = source[two, at].astype(jnp.float32) * high
            target[one, at] = jnp.where(turned, b, a).astype(jnp.bfloat16)
            target[two, at] = jnp.where(turned, a, b).astype(jnp.bfloat16)

        for lane in range(0, D, HEAD):
            lanes(pl.ds(lane, HEAD), low, high, x_ref, out_ref)
        for at in (one, two):
            copy = pltpu.make_async_copy(out_ref.at[at], out_hbm.at[at], sem.at[len(copies)])
            copy.start()
            copies.append(copy)
        if start == 0:
            for load in loads[2:]:
                load.wait()
        for lane in range(0, COLS, HEAD):
            lanes(pl.ds(lane, HEAD), 1.0, 1.0, new_ref, kept_ref)
    low = jnp.concatenate([scale_ref[i][:, :PART] for i in range(PER_HALF)], axis=1)
    high = jnp.concatenate([scale_ref[i][:, :PART] for i in range(PER_HALF, PARTS)], axis=1)
    flip = turn_ref[:, :RUN] > 0.5
    row_ref[...] = jnp.concatenate(
        [jnp.where(flip, high, low), jnp.where(flip, low, high)], axis=1
    )
    for copy in copies:
        copy.wait()


def finalize(*operands):
    vmem = pl.BlockSpec(memory_space=pltpu.VMEM)
    hbm = pl.BlockSpec(memory_space=pltpu.HBM)
    return pl.pallas_call(
        final_kernel,
        out_shape=(
            jax.ShapeDtypeStruct((TOK, D), jnp.bfloat16),
            jax.ShapeDtypeStruct((1, TOK), jnp.float32),
            jax.ShapeDtypeStruct((TOK, COLS), jnp.bfloat16),
        ),
        in_specs=[hbm] * 5,
        out_specs=[hbm, vmem, vmem],
        scratch_shapes=[
            pltpu.VMEM((TOK, D), jnp.bfloat16),
            pltpu.VMEM((TOK, COLS), jnp.bfloat16),
            pltpu.VMEM((TOK, HEAD), jnp.float32),
            pltpu.VMEM((PARTS, 1, HEAD), jnp.float32),
            pltpu.VMEM((1, HEAD), jnp.float32),
            pltpu.VMEM((TOK, D), jnp.bfloat16),
            pltpu.SemaphoreType.DMA((4,)),
            pltpu.SemaphoreType.DMA((2 * RUN // STRIP,)),
            pltpu.SemaphoreType.DMA((2 * RUN // STRIP,)),
        ],
        compiler_params=pltpu.CompilerParams(vmem_limit_bytes=VMEM_LIMIT),
        name="final",
    )(*operands)


def on_device(queries, key_vectors, value_vectors, positions, residual, norm_gain, out_weight):
    results = fused(
        positions, queries, key_vectors, value_vectors, out_weight, residual, norm_gain
    )
    quantized, row, new_residual = finalize(*results)
    return (quantized, row.reshape(TOK), new_residual)


def solution(mesh):
    in_specs = (
        P("seq", "tp"),
        P("seq", "tp"),
        P("seq", "tp"),
        P("seq"),
        P("seq", "tp"),
        P(None, "tp"),
        P("tp", None),
    )
    out_specs = (P("seq", None), P("seq"), P("seq", "tp"))
    return jax.shard_map(
        on_device, mesh=mesh, in_specs=in_specs, out_specs=out_specs, check_vma=False
    )
```

```python
import functools
import heapq
import math

import jax
import jax.numpy as jnp
from jax import lax
from jax.experimental import pallas as pl
from jax.experimental.pallas import tpu as pltpu
from jax.sharding import PartitionSpec as P

D = 6144
HEADS = 6
HEAD = 128
TOK = 192
RUN = TOK // 2
NX = 4
NY = 4
NZ = 8
N_TP = 8
ROWS = HEADS * RUN
GROUP = NX * RUN
CHUNK = 2 * RUN
COLS = HEADS * HEAD
HALF = COLS // 2
PER_HALF = 1
PARTS = 2 * PER_HALF
PART = TOK // PARTS
NEG = -1e30
SUM_DIRECT = ()
SHARE_DIRECT = ()
BEFORE_LO = [("pass_up", PARTS - 1), ("pass_down", PARTS - 1)]
EXP_SCALE = math.log2(math.e) / math.sqrt(HEAD)
MESH = pl.DeviceIdType.MESH

K_LO, V_LO, K_HI, V_HI, RUN_ID = range(5)
KINDS = (V_LO, K_LO, RUN_ID, V_HI, K_HI)
X_FIRST = {K_LO: True, V_LO: False, K_HI: True, V_HI: False, RUN_ID: True}
REACH = {
    K_LO: (2, 1, 4, 3),
    V_LO: (2, 1, 4, 3),
    K_HI: (1, 2, 3, 4),
    V_HI: (1, 2, 3, 4),
    RUN_ID: (2, 1, 4, 3),
}
LO, HI = 0, 1
DIRECT = (K_LO, K_HI, RUN_ID, V_LO, V_HI)
for _k in DIRECT:
    REACH[_k] = (2, 1) + REACH[_k][2:]
REACH[RUN_ID] = (2, 1, 0, 0)
FAR = (2, 1, -1, 0)
X_PLUS, X_MINUS, Z_PLUS, Z_MINUS, Y_PLUS, Y_MINUS, PAIR, X_FAR, Y_FAR = range(9)
(
    UP_RELAY, UP_DIRECT, UP_LAST, DOWN_RELAY, DOWN_DIRECT, DOWN_LAST,
    X_UP, X_DOWN, X_UP_FAR, X_DOWN_FAR,
    X_PAIR, X_PAIR_UP, X_PAIR_DOWN, X_PAIR_UP_FAR, X_PAIR_DOWN_FAR,
) = range(15)
N_ARRIVALS = 15


def children(kind, mx, mz):
    xp, xn, zp, zn = REACH[kind]
    along_x, along_z = [], []
    if kind in DIRECT and mx == 0:
        along_x = [(kind, 1, mz, X_PLUS), (kind, -1, mz, X_MINUS), (kind, 2, mz, X_FAR)]
    if kind in DIRECT:
        xp = xn = 0
    if 0 <= mx < xp:
        along_x.append((kind, mx + 1, mz, X_PLUS))
    if -xn < mx <= 0:
        along_x.append((kind, mx - 1, mz, X_MINUS))
    if 0 <= mz < zp:
        along_z.append((kind, mx, mz + 1, Z_PLUS))
    if -zn < mz <= 0:
        along_z.append((kind, mx, mz - 1, Z_MINUS))
    if X_FIRST[kind]:
        return along_z + along_x if mz == 0 else along_z
    return along_x + along_z if mx == 0 else along_x


def moves(kind):
    xp, xn, zp, zn = REACH[kind]
    return [
        (kind, mx, mz)
        for mx in range(-xn, xp + 1)
        for mz in range(-zn, zp + 1)
        if (mx, mz) != (0, 0)
    ]


def onward(mz):
    steps = []
    if 0 <= mz < 4:
        steps.append((mz + 1, Z_PLUS))
    if -3 < mz <= 0:
        steps.append((mz - 1, Z_MINUS))
    return steps


EVENT_ID = {
    key: i
    for i, key in enumerate(
        [key for kind in KINDS for key in moves(kind)]
        + [("ids", mz) for mz in range(-3, 5) if mz]
    )
}
N_EVENTS = len(EVENT_ID)
UNIT_US = 0.6
PROJECT_US = 0.5
HOP_US = 2.9
PAIR_US = 1.5
PIECE_US = 0.55
PART_US = 1.6 * PART / RUN


def plan():
    tasks = {}
    for kind in KINDS:
        took = 0.04 if kind == RUN_ID else PIECE_US
        for key in [(kind, 0, 0)] + moves(kind):
            sends = [(child[:3], child[3], took) for child in children(*key)]
            own = key[1:] == (0, 0)
            rank = (0 if kind in (K_LO, V_LO, RUN_ID) else 1) + (-2 if own else 0)
            tasks[("relay",) + key] = (rank, [] if own else [key], [], 0.03, sends)
    start = [("relay", kind, 0, 0) for kind in KINDS]
    tasks[("diagonal",)] = (2, [], start, 0.8, [])

    for mz in range(-3, 5):
        needs = [("relay",) + key for key in moves(RUN_ID)] if mz == 0 else []
        tasks[("ids", mz)] = (
            0, [("ids", mz)] if mz else [], needs, 0.03,
            [(("ids", step), link, 0.05) for step, link in onward(mz)],
        )

    def group_keys(kinds, dz):
        return [k for kind in kinds for k in moves(kind) if (k[2] - dz) % NZ == 0]

    lo_kinds, hi_kinds = (K_LO, V_LO), (K_HI, V_HI)
    fins = {LO: [("diagonal",)], HI: [("diagonal",)]}
    for i, dz in enumerate((0, 1, -1, 2, -2, 3, -3, 4)):
        for name, kinds, half, base in (
            ("lo_lo", lo_kinds, LO, 20),
            ("hi_lo", lo_kinds, HI, 40),
            ("hi_hi", hi_kinds, HI, 41),
        ):
            keys = group_keys(kinds, dz)
            task = (name, dz)
            relays = [("relay",) + k for k in keys] + [("ids", dz)]
            tasks[task] = (base + 0.1 * i, [], relays + [("diagonal",)], UNIT_US, [])
            fins[half].append(task)
    for half in (LO, HI):
        late = 0.5 * half
        parts = range(half * PER_HALF, (half + 1) * PER_HALF)
        tasks[("attended", half)] = (10, [], fins[half], 0.4, [(("att", half), PAIR, 0.3)])
        for slot, step in enumerate(FAR):
            sends = []
            for part in parts:
                if part in SUM_DIRECT:
                    pairs, link = {
                        2: ((UP_RELAY, DOWN_RELAY), Y_FAR),
                        1: ((UP_LAST, UP_DIRECT), Y_PLUS),
                        -1: ((DOWN_DIRECT, DOWN_LAST), Y_MINUS),
                        0: ((), Y_PLUS),
                    }[step]
                    sends += [((part, event), link, PART_US) for event in pairs]
                elif step == 2:
                    sends += [((part, UP_RELAY), Y_PLUS, PART_US), ((part, DOWN_RELAY), Y_MINUS, PART_US)]
                elif step == 1:
                    sends += [((part, UP_DIRECT), Y_PLUS, PART_US)]
                elif step == -1:
                    sends += [((part, DOWN_DIRECT), Y_MINUS, PART_US)]
            needs = [("attended", half)] if slot == 0 else [("project", half, slot - 1)]
            tasks[("project", half, slot)] = (9 + late, [("att", half)], needs, PROJECT_US, sends)
        for part in parts:
            direct = part in SUM_DIRECT
            if not direct:
                tasks[("pass_up", part)] = (
                    4 + late, [(part, UP_RELAY)], [("project", half, 1)], 0.1,
                    [((part, UP_LAST), Y_PLUS, PART_US)],
                )
                tasks[("pass_down", part)] = (
                    4 + late, [(part, DOWN_RELAY)], [("project", half, 2)], 0.1,
                    [((part, DOWN_LAST), Y_MINUS, PART_US)],
                )
            tasks[("finish", part)] = (
                6 + late,
                [
                    (part, e)
                    for e in (UP_DIRECT, DOWN_DIRECT, UP_LAST, DOWN_LAST)
                    + ((UP_RELAY, DOWN_RELAY) if direct else ())
                ],
                [("project", half, 3)],
                0.4,
                [((part, "stats"), PAIR, 0.1)],
            )
            tasks[("publish", part)] = (
                6.1 + late,
                [],
                [("finish", part)] + (BEFORE_LO if half == LO else []),
                0.02,
                [
                    ((part, X_UP), Y_PLUS, 2 * PART_US),
                    ((part, X_DOWN), Y_MINUS, 2 * PART_US),
                    ((part, X_PAIR), PAIR, 0.15),
                ]
                + (
                    [((part, X_UP_FAR), Y_FAR, PART_US), ((part, X_DOWN_FAR), Y_FAR, PART_US)]
                    if part in SHARE_DIRECT
                    else []
                ),
            )
            tasks[("share_up", part)] = (
                5 + late, [(part, X_UP)], [], 0.03,
                [((part, X_PAIR_UP), PAIR, 0.15)]
                + ([] if part in SHARE_DIRECT else [((part, X_UP_FAR), Y_PLUS, PART_US)]),
            )
            tasks[("share_down", part)] = (
                5 + late, [(part, X_DOWN)], [], 0.03,
                [((part, X_PAIR_DOWN), PAIR, 0.15)]
                + ([] if part in SHARE_DIRECT else [((part, X_DOWN_FAR), Y_MINUS, PART_US)]),
            )
            tasks[("far_up", part)] = (
                5 + late, [(part, X_UP_FAR)], [], 0.03, [((part, X_PAIR_UP_FAR), PAIR, 0.1)]
            )
            tasks[("far_down", part)] = (
                5 + late, [(part, X_DOWN_FAR)], [], 0.03, [((part, X_PAIR_DOWN_FAR), PAIR, 0.1)]
            )
            tasks[("scales", part)] = (
                50,
                [(part, "stats")],
                [("publish", part)],
                0.3,
                [],
            )
            pairs = (X_PAIR, X_PAIR_UP, X_PAIR_DOWN, X_PAIR_UP_FAR, X_PAIR_DOWN_FAR)
            tasks[("collect", part)] = (60, [(part, e) for e in pairs], [], 0.02, [])

    free = [0.0] * 9
    when = {}
    order, done = [], set()
    left = dict(tasks)
    now = 0.0
    while left:
        best = None
        soonest = None
        for task, (rank, arrivals, needs, cost, sends) in left.items():
            if not all(n in done for n in needs) or not all(a in when for a in arrivals):
                continue
            ready = max([when[a] for a in arrivals], default=0.0)
            if ready <= now:
                if best is None or rank < best[0]:
                    best = (rank, task)
            elif soonest is None or ready < soonest:
                soonest = ready
        if best is None:
            now = soonest
            continue
        task = best[1]
        rank, arrivals, needs, cost, sends = left.pop(task)
        now += cost
        done.add(task)
        order.append((task, now))
        for arrival, link, took in sends:
            if link in (X_FAR, Y_FAR):
                ways = (X_PLUS, X_MINUS) if link == X_FAR else (Y_PLUS, Y_MINUS)
                for way in ways:
                    free[way] = max(free[way], now) + took
                when[arrival] = max(free[way] for way in ways) + HOP_US + 0.7
                continue
            free[link] = max(free[link], now) + took
            hop = 7.0 if arrival[-1] == "stats" else PAIR_US if link == PAIR else HOP_US
            when[arrival] = free[link] + hop
    return order, now


ORDER, PLANNED_US = plan()


def update(rows, queries, m_ref, l_ref, acc_ref, keys, values, bias, chunk):
    starts = range(rows[0], rows[1], chunk)
    all_scores, all_new, all_factors = [], [], []
    for start in starts:
        scores = lax.dot_general(
            queries[pl.ds(start, chunk), :],
            keys,
            (((1,), (1,)), ((), ())),
            preferred_element_type=jnp.float32,
        )
        scores = scores * EXP_SCALE
        all_scores.append(scores if bias is None else scores + bias)
    for start, scores in zip(starts, all_scores):
        at = pl.ds(start, chunk)
        old = m_ref[at, :]
        new = jnp.maximum(old, jnp.max(scores, axis=1, keepdims=True))
        m_ref[at, :] = new
        all_new.append(new)
        all_factors.append(jnp.exp2(old - new))
    for start, scores, new, factor in zip(starts, all_scores, all_new, all_factors):
        at = pl.ds(start, chunk)
        weights = [
            jnp.exp2(scores[:, i : i + HEAD] - new) for i in range(0, scores.shape[1], HEAD)
        ]
        l_ref[at, :] = l_ref[at, :] * factor + functools.reduce(jnp.add, weights)
        probs = jnp.concatenate([w.astype(jnp.bfloat16) for w in weights], axis=1)
        acc_ref[at, :] = acc_ref[at, :] * factor + jnp.dot(
            probs, values, preferred_element_type=jnp.float32
        )


def first_block(first, queries, m_ref, l_ref, acc_ref, keys, values):
    at = pl.ds(first, ROWS)
    scores = lax.dot_general(
        queries[at, :], keys, (((1,), (1,)), ((), ())), preferred_element_type=jnp.float32
    )
    scores = (scores * EXP_SCALE).reshape(HEADS, RUN, RUN)
    row = lax.broadcasted_iota(jnp.int32, (HEADS, RUN, RUN), 1)
    column = lax.broadcasted_iota(jnp.int32, (HEADS, RUN, RUN), 2)
    scores = jnp.where(column <= row, scores, NEG).reshape(ROWS, RUN)
    high = jnp.max(scores, axis=1, keepdims=True)
    weights = jnp.exp2(scores - high)
    m_ref[at, :] = jnp.broadcast_to(high, (ROWS, HEAD))
    total = jnp.sum(weights, axis=1, keepdims=True)
    lane = lax.broadcasted_iota(jnp.int32, (ROWS, HEAD), 1)
    l_ref[at, :] = jnp.where(lane == 0, total, 0.0)
    acc_ref[at, :] = jnp.dot(
        weights.astype(jnp.bfloat16), values, preferred_element_type=jnp.float32
    )


def lane_bias(ids, mine, low):
    one = [
        jnp.where(ids[j] < mine if low else ids[j] > mine, 0.0, NEG) for j in range(NX)
    ]
    lane = lax.broadcasted_iota(jnp.int32, (1, HEAD), 1)
    tiles = [
        jnp.where(lane < 96, one[0], one[1]),
        jnp.where(lane < 64, one[1], one[2]),
        jnp.where(lane < 32, one[2], one[3]),
    ]
    return jnp.concatenate(tiles, axis=1)


def fused_kernel(
    pos_hbm, q_hbm, k_hbm, v_hbm, w_ref, residual_hbm, gain_hbm,
    x_hbm, new_hbm, factor_hbm, scale_hbm, turn_hbm,
    x_ref, new_ref, factor_ref, scale_ref, turn_ref, pos_ref, q_ref, k_ref, v_ref, residual_ref, gain_ref, own, own_id, kv, ids, queries, m_ref, l_ref, acc_ref,
    weights, attended, mine, outgoing, relayed, got, stats,
    store_sem, small_sem, early_sem, load_sem, send, recv, w_send, w_recv, att_send, att_recv,
    part_send, part_recv, stat_send, stat_recv,
):
    seq = lax.axis_index("seq")
    tp = lax.axis_index("tp")
    x = lax.rem(seq, NX)
    z = seq // NX
    core = lax.rem(tp, 2)
    y = tp // 2
    peers = (
        (z * NX + lax.rem(x + 1, NX), tp),
        (z * NX + lax.rem(x + NX - 1, NX), tp),
        (lax.rem(z + 1, NZ) * NX + x, tp),
        (lax.rem(z + NZ - 1, NZ) * NX + x, tp),
        (seq, lax.rem(tp + 2, N_TP)),
        (seq, lax.rem(tp + 6, N_TP)),
        (seq, y * 2 + 1 - core),
        (z * NX + lax.rem(x + 2, NX), tp),
        (seq, lax.rem(tp + 4, N_TP)),
    )

    def columns(step, parity, first=0, width=COLS):
        block = lax.rem(y + step + NY, NY) * 2 + parity
        return pl.ds(pl.multiple_of(block * COLS + first, HEAD), width)

    sent = []
    stores = []

    def keep(source, target, sem):
        store = pltpu.make_async_copy(source, target, sem)
        store.start()
        stores.append(store)

    def remote(source, target, send_sem, recv_sem, peer):
        return pltpu.make_async_remote_copy(
            src_ref=source,
            dst_ref=target,
            send_sem=send_sem,
            recv_sem=recv_sem,
            device_id=peer,
            device_id_type=MESH,
        )

    def ship(*args):
        copy = remote(*args)
        copy.start()
        sent.append(copy)

    def arrive(target, send_sem, recv_sem):
        remote(target, target, send_sem, recv_sem, peers[PAIR]).wait_recv()

    loads = [
        pltpu.make_async_copy(q_hbm, q_ref, load_sem.at[0]),
        pltpu.make_async_copy(residual_hbm, residual_ref, load_sem.at[1]),
    ]
    for slot, step in enumerate(FAR):
        loads.append(
            pltpu.make_async_copy(
                w_ref.at[:, columns(step, core)],
                weights.at[slot, pl.ds(0, COLS)],
                load_sem.at[2 + slot],
            )
        )
    early = [
        pltpu.make_async_copy(k_hbm, k_ref, early_sem.at[0]),
        pltpu.make_async_copy(v_hbm, v_ref, early_sem.at[1]),
        pltpu.make_async_copy(pos_hbm, pos_ref, early_sem.at[2]),
        pltpu.make_async_copy(gain_hbm, gain_ref, early_sem.at[3]),
    ]
    for load in early + loads[:2]:
        load.start()

    barrier = pltpu.get_barrier_semaphore()
    greeted = list(peers[:4]) + [peers[X_FAR]] + [(seq, lax.rem(tp + step, N_TP)) for step in range(1, N_TP)]
    for peer in greeted:
        pl.semaphore_signal(barrier, inc=1, device_id=peer, device_id_type=MESH)
    for load in early:
        load.wait()

    first, last = pos_ref[0], pos_ref[RUN]
    low_run = jnp.minimum(first, last) // RUN
    mine_id = jnp.full((1, HEAD), low_run, jnp.int32).astype(jnp.float32)
    swapped = jnp.full((RUN, HEAD), jnp.where(first > last, 1, 0), jnp.int32) > 0

    def pick(ref, columns, half):
        one = ref[pl.ds(0, RUN), columns].astype(jnp.float32)
        two = ref[pl.ds(RUN, RUN), columns].astype(jnp.float32)
        return jnp.where(swapped, two, one) if half == LO else jnp.where(swapped, one, two)

    every = pl.ds(0, HEAD)
    for kind, ref, half in ((K_LO, k_ref, LO), (V_LO, v_ref, LO), (K_HI, k_ref, HI), (V_HI, v_ref, HI)):
        piece = pick(ref, every, half).astype(jnp.bfloat16)
        own[kind] = piece
        kv[kind, seq] = piece
    turn_ref[...] = swapped[0:1].astype(jnp.float32)
    own_id[0] = mine_id
    ids[seq] = mine_id

    pl.semaphore_wait(barrier, len(greeted))

    def source_of(mx, mz):
        return lax.rem(z + 2 * NZ - mz, NZ) * NX + lax.rem(x + 2 * NX - mx, NX)

    def place(kind, index):
        return ids.at[index] if kind == RUN_ID else kv.at[kind, index]

    def relay(kind, mx, mz):
        index = source_of(mx, mz)
        here = place(kind, index)
        source = here
        if (mx, mz) == (0, 0):
            source = own_id.at[0] if kind == RUN_ID else own.at[kind]
        else:
            event = EVENT_ID[(kind, mx, mz)]
            arrive(here, send.at[event], recv.at[event])
        for child in children(kind, mx, mz):
            event = EVENT_ID[child[:3]]
            ship(source, here, send.at[event], recv.at[event], peers[child[3]])

    def pass_ids(mz):
        here = ids.at[pl.ds(lax.rem(z + 2 * NZ - mz, NZ) * NX, NX)]
        if mz:
            event = EVENT_ID[("ids", mz)]
            arrive(here, send.at[event], recv.at[event])
        for step, link in onward(mz):
            event = EVENT_ID[("ids", step)]
            ship(here, here, send.at[event], recv.at[event], peers[link])

    def diagonal():
        for slot in range(4):
            loads[2 + slot].start()
        for slot, step in enumerate(FAR):
            ship(
                w_ref.at[:, columns(step, 1 - core)],
                weights.at[slot, pl.ds(COLS, COLS)],
                w_send.at[slot],
                w_recv.at[slot],
                peers[PAIR],
            )
        loads[0].wait()
        for head in range(HEADS):
            for half in (LO, HI):
                queries[pl.ds(half * ROWS + head * RUN, RUN), :] = pick(
                    q_ref, pl.ds(head * HEAD, HEAD), half
                ).astype(jnp.bfloat16)
        first_block(0, queries, m_ref, l_ref, acc_ref, own[K_LO], own[V_LO])
        first_block(ROWS, queries, m_ref, l_ref, acc_ref, own[K_HI], own[V_HI])

    def unit(dz, half, low_keys):
        at = pl.ds(lax.rem(z + 2 * NZ - dz, NZ) * NX, NX)
        keys = kv[K_LO if low_keys else K_HI, at].reshape(GROUP, HEAD)
        values = kv[V_LO if low_keys else V_HI, at].reshape(GROUP, HEAD)
        bias = None
        if low_keys == (half == LO):
            bias = lane_bias(ids[at], mine_id, low_keys)
        bounds = (half * ROWS, (half + 1) * ROWS)
        update(bounds, queries, m_ref, l_ref, acc_ref, keys, values, bias, CHUNK)

    def attend_half(half):
        for head in range(HEADS):
            at = pl.ds(half * ROWS + head * RUN, RUN)
            total = jnp.sum(l_ref[at, :], axis=1, keepdims=True)
            attended[half, 0, :, pl.ds(head * HEAD, HEAD)] = (acc_ref[at, :] / total).astype(
                jnp.bfloat16
            )
        ship(
            attended.at[half, 0],
            attended.at[half, 1],
            att_send.at[half],
            att_recv.at[half],
            peers[PAIR],
        )

    def rows(part):
        return pl.ds(part * PART, PART)

    left = pl.ds(0, HALF)
    right = pl.ds(HALF, HALF)

    def slab(event, part):
        return got.at[event, rows(part)]

    def send_part(part, event, source, target, peer):
        ship(source, target, part_send.at[part, event], part_recv.at[part, event], peers[peer])

    def await_part(part, event, target):
        arrive(target, part_send.at[part, event], part_recv.at[part, event])

    def project(half, slot):
        if slot == 0:
            arrive(attended.at[half, 1], att_send.at[half], att_recv.at[half])
        if half == LO:
            loads[2 + slot].wait()
            arrive(weights.at[slot, pl.ds(COLS, COLS)], w_send.at[slot], w_recv.at[slot])
        product = jnp.dot(
            attended[half, 0], weights[slot, pl.ds(0, COLS), :], preferred_element_type=jnp.float32
        ) + jnp.dot(
            attended[half, 1],
            weights[slot, pl.ds(COLS, COLS), :],
            preferred_element_type=jnp.float32,
        )
        step = FAR[slot]
        if step == 0:
            mine[pl.ds(half * RUN, RUN), :] = product
            return
        outgoing[slot, pl.ds(half * RUN, RUN), :] = product.astype(jnp.bfloat16)
        for part in range(half * PER_HALF, (half + 1) * PER_HALF):
            here = outgoing.at[slot, rows(part)]
            if part in SUM_DIRECT:
                (first, second), peer = {
                    2: ((UP_RELAY, DOWN_RELAY), Y_FAR),
                    1: ((UP_LAST, UP_DIRECT), Y_PLUS),
                    -1: ((DOWN_DIRECT, DOWN_LAST), Y_MINUS),
                }[step]
                send_part(part, first, here.at[:, left], slab(first, part), peer)
                send_part(part, second, here.at[:, right], slab(second, part), peer)
            elif step == 2:
                send_part(part, UP_RELAY, here.at[:, left], slab(UP_RELAY, part), Y_PLUS)
                send_part(part, DOWN_RELAY, here.at[:, right], slab(DOWN_RELAY, part), Y_MINUS)
            elif step == 1:
                send_part(part, UP_DIRECT, here.at[:, right], slab(UP_DIRECT, part), Y_PLUS)
            else:
                send_part(part, DOWN_DIRECT, here.at[:, left], slab(DOWN_DIRECT, part), Y_MINUS)

    def pass_on(part, way):
        arrival, onward, slot, half, peer = (
            (UP_RELAY, UP_LAST, 1, left, Y_PLUS),
            (DOWN_RELAY, DOWN_LAST, 2, right, Y_MINUS),
        )[way]
        at = rows(part)
        await_part(part, arrival, slab(arrival, part))
        total = outgoing[slot, at, half].astype(jnp.float32) + slab(arrival, part)[...].astype(
            jnp.float32
        )
        relayed[way, at, :] = total.astype(jnp.bfloat16)
        send_part(part, onward, relayed.at[way, at], slab(onward, part), peer)

    def finish(part):
        at = rows(part)
        half_of = part // PER_HALF
        if part == 0:
            loads[1].wait()
        squares = jnp.zeros((PART, HEAD), jnp.float32)
        peak = jnp.zeros((PART, HEAD), jnp.float32)
        inside = (part % PER_HALF) * PART
        one, two = pl.ds(inside, PART), pl.ds(RUN + inside, PART)
        turned = swapped[0:PART]
        for first, *events in (
            (0, DOWN_DIRECT, UP_LAST, UP_RELAY),
            (HALF, UP_DIRECT, DOWN_LAST, DOWN_RELAY),
        ):
            events = events if part in SUM_DIRECT else events[:2]
            for event in events:
                await_part(part, event, slab(event, part))
            for lane in range(0, HALF, HEAD):
                here = pl.ds(first + lane, HEAD)
                there = pl.ds(lane, HEAD)
                low = residual_ref[one, here].astype(jnp.float32)
                high = residual_ref[two, here].astype(jnp.float32)
                old = jnp.where(turned, high, low) if half_of == LO else jnp.where(turned, low, high)
                summed = mine[at, here] + old
                for event in events:
                    summed = summed + slab(event, part)[:, there].astype(jnp.float32)
                new_ref[at, here] = summed.astype(jnp.bfloat16)
                gained = summed * gain_ref[:, here]
                x_ref[at, columns(0, core, first + lane, HEAD)] = gained.astype(jnp.bfloat16)
                squares = squares + summed * summed
                peak = jnp.maximum(peak, jnp.abs(gained))
        lane = lax.broadcasted_iota(jnp.int32, (PART, HEAD), 1)
        both = jnp.where(
            lane == 0,
            jnp.sum(squares, axis=1, keepdims=True),
            jnp.max(peak, axis=1, keepdims=True),
        )
        if PART < HEAD:
            both = jnp.concatenate([both, jnp.zeros((HEAD - PART, HEAD), jnp.float32)], axis=0)
        stats[part, tp] = jnp.transpose(both)[0:8, :]
        for step in range(1, N_TP):
            ship(
                stats.at[part, tp],
                stats.at[part, tp],
                stat_send.at[part, step],
                stat_recv.at[part, step],
                (seq, lax.rem(tp + step, N_TP)),
            )

    def publish(part):
        at = rows(part)
        keep(new_ref.at[at], new_hbm.at[at], small_sem.at[2, part])
        if part == 0:
            keep(turn_ref, turn_hbm, early_sem.at[4])
        block = x_ref.at[at, columns(0, core)]
        send_part(part, X_UP, block, block, Y_PLUS)
        send_part(part, X_DOWN, block, block, Y_MINUS)
        if part in SHARE_DIRECT:
            for event, first in ((X_UP_FAR, 0), (X_DOWN_FAR, HALF)):
                half = x_ref.at[at, columns(0, core, first, HALF)]
                send_part(part, event, half, half, Y_FAR)
        send_part(part, X_PAIR, block, block, PAIR)

    def share(part, way):
        arrival, far, pair, step, first, peer = (
            (X_UP, X_UP_FAR, X_PAIR_UP, -1, 0, Y_PLUS),
            (X_DOWN, X_DOWN_FAR, X_PAIR_DOWN, 1, HALF, Y_MINUS),
        )[way]
        at = rows(part)
        block = x_ref.at[at, columns(step, core)]
        await_part(part, arrival, block)
        if part not in SHARE_DIRECT:
            half = x_ref.at[at, columns(step, core, first, HALF)]
            send_part(part, far, half, half, peer)
        send_part(part, pair, block, block, PAIR)

    def share_far(part, way):
        arrival, pair, first = (
            (X_UP_FAR, X_PAIR_UP_FAR, 0),
            (X_DOWN_FAR, X_PAIR_DOWN_FAR, HALF),
        )[way]
        half = x_ref.at[rows(part), columns(2, core, first, HALF)]
        await_part(part, arrival, half)
        send_part(part, pair, half, half, PAIR)

    def scales(part):
        for step in range(1, N_TP):
            source = lax.rem(tp + N_TP - step, N_TP)
            arrive(stats.at[part, source], stat_send.at[part, step], stat_recv.at[part, step])
        total = stats[part, 0, 0:1, :]
        high = stats[part, 0, 1:2, :]
        for source in range(1, N_TP):
            total = total + stats[part, source, 0:1, :]
            high = jnp.maximum(high, stats[part, source, 1:2, :])
        root = lax.rsqrt(total / D + 1e-05)
        scale = high * root + 1e-06
        scale_ref[part] = scale
        factor = jnp.transpose(jnp.broadcast_to(root / scale, (HEAD, HEAD)))
        factor_ref[rows(part), :] = factor[0:PART, :]
        keep(scale_ref.at[part], scale_hbm.at[part], small_sem.at[0, part])
        keep(factor_ref.at[rows(part)], factor_hbm.at[rows(part)], small_sem.at[1, part])

    def collect(part):
        at = rows(part)
        other = 1 - core
        for event, step, first, width in (
            (X_PAIR, 0, 0, COLS),
            (X_PAIR_UP, -1, 0, COLS),
            (X_PAIR_DOWN, 1, 0, COLS),
            (X_PAIR_UP_FAR, 2, 0, HALF),
            (X_PAIR_DOWN_FAR, 2, HALF, HALF),
        ):
            await_part(part, event, x_ref.at[at, columns(step, other, first, width)])
        keep(x_ref.at[at], x_hbm.at[at], store_sem.at[part])

    emit = {
        "relay": relay,
        "ids": pass_ids,
        "diagonal": diagonal,
        "lo_lo": lambda dz: unit(dz, LO, True),
        "hi_lo": lambda dz: unit(dz, HI, True),
        "hi_hi": lambda dz: unit(dz, HI, False),
        "attended": attend_half,
        "project": project,
        "pass_up": lambda part: pass_on(part, 0),
        "pass_down": lambda part: pass_on(part, 1),
        "finish": finish,
        "publish": publish,
        "share_up": lambda part: share(part, 0),
        "share_down": lambda part: share(part, 1),
        "far_up": lambda part: share_far(part, 0),
        "far_down": lambda part: share_far(part, 1),
        "scales": scales,
        "collect": collect,
    }
    for task, _ in ORDER:
        emit[task[0]](*task[1:])
    for copy in sent:
        copy.wait_send()
    for store in stores:
        store.wait()


def fused(positions, queries, keys, values, out_weight, residual, gain):
    hbm = pl.BlockSpec(memory_space=pltpu.HBM)
    bf16, f32 = jnp.bfloat16, jnp.float32
    dma = pltpu.SemaphoreType.DMA
    return pl.pallas_call(
        fused_kernel,
        out_shape=(
            jax.ShapeDtypeStruct((TOK, D), bf16),
            jax.ShapeDtypeStruct((TOK, COLS), bf16),
            jax.ShapeDtypeStruct((TOK, HEAD), f32),
            jax.ShapeDtypeStruct((PARTS, 1, HEAD), f32),
            jax.ShapeDtypeStruct((1, HEAD), f32),
        ),
        in_specs=[hbm] * 7,
        out_specs=[hbm] * 5,
        scratch_shapes=[
            pltpu.VMEM((TOK, D), bf16),
            pltpu.VMEM((TOK, COLS), bf16),
            pltpu.VMEM((TOK, HEAD), f32),
            pltpu.VMEM((PARTS, 1, HEAD), f32),
            pltpu.VMEM((1, HEAD), f32),
            pltpu.SMEM((TOK,), jnp.int32),
            pltpu.VMEM((TOK, COLS), bf16),
            pltpu.VMEM((TOK, HEAD), bf16),
            pltpu.VMEM((TOK, HEAD), bf16),
            pltpu.VMEM((TOK, COLS), bf16),
            pltpu.VMEM((1, COLS), f32),
            pltpu.VMEM((4, RUN, HEAD), bf16),
            pltpu.VMEM((1, 1, HEAD), f32),
            pltpu.VMEM((4, NX * NZ, RUN, HEAD), bf16),
            pltpu.VMEM((NX * NZ, 1, HEAD), f32),
            pltpu.VMEM((2 * ROWS, HEAD), bf16),
            pltpu.VMEM((2 * ROWS, HEAD), f32),
            pltpu.VMEM((2 * ROWS, HEAD), f32),
            pltpu.VMEM((2 * ROWS, HEAD), f32),
            pltpu.VMEM((4, 2 * COLS, COLS), bf16),
            pltpu.VMEM((2, 2, RUN, COLS), bf16),
            pltpu.VMEM((TOK, COLS), f32),
            pltpu.VMEM((3, TOK, COLS), bf16),
            pltpu.VMEM((2, TOK, HALF), bf16),
            pltpu.VMEM((6, TOK, HALF), bf16),
            pltpu.VMEM((PARTS, N_TP, 8, HEAD), f32),
            dma((PARTS,)),
            dma((3, PARTS)),
            dma((5,)),
            dma((6,)),
            dma((N_EVENTS,)),
            dma((N_EVENTS,)),
            dma((4,)),
            dma((4,)),
            dma((2,)),
            dma((2,)),
            dma((PARTS, N_ARRIVALS)),
            dma((PARTS, N_ARRIVALS)),
            dma((PARTS, N_TP)),
            dma((PARTS, N_TP)),
        ],
        compiler_params=pltpu.CompilerParams(
            collective_id=0, has_side_effects=True, vmem_limit_bytes=VMEM_LIMIT
        ),
        name="fused",
    )(positions, queries, keys, values, out_weight, residual, gain)


VMEM_LIMIT = 67043328
STRIP = 32


def final_kernel(
    x_hbm, new_hbm, factor_hbm, scale_hbm, turn_hbm, out_hbm, row_ref, kept_ref,
    x_ref, new_ref, factor_ref, scale_ref, turn_ref, out_ref, load_sem, x_sem, sem,
):
    loads = [
        pltpu.make_async_copy(source, target, load_sem.at[i])
        for i, (source, target) in enumerate(
            (
                (turn_hbm, turn_ref),
                (factor_hbm, factor_ref),
                (scale_hbm, scale_ref),
                (new_hbm, new_ref),
            )
        )
    ]
    strips = []
    for i, start in enumerate(range(0, RUN, STRIP)):
        for j in range(2):
            at = pl.ds(j * RUN + start, STRIP)
            strips.append(
                pltpu.make_async_copy(x_hbm.at[at], x_ref.at[at], x_sem.at[2 * i + j])
            )
    for load in loads[:2] + strips + loads[2:]:
        load.start()
    for load in loads[:2]:
        load.wait()
    turned = jnp.broadcast_to(turn_ref[...], (STRIP, HEAD)) > 0.5
    copies = []
    for start in range(0, RUN, STRIP):
        one, two = pl.ds(start, STRIP), pl.ds(RUN + start, STRIP)
        low, high = factor_ref[one, :], factor_ref[two, :]
        strips[len(copies)].wait()
        strips[len(copies) + 1].wait()

        def lanes(at, low, high, source, target, one=one, two=two):
            a = source[one, at].astype(jnp.float32) * low
            b = source[two, at].astype(jnp.float32) * high
            target[one, at] = jnp.where(turned, b, a).astype(jnp.bfloat16)
            target[two, at] = jnp.where(turned, a, b).astype(jnp.bfloat16)

        for lane in range(0, D, HEAD):
            lanes(pl.ds(lane, HEAD), low, high, x_ref, out_ref)
        for at in (one, two):
            copy = pltpu.make_async_copy(out_ref.at[at], out_hbm.at[at], sem.at[len(copies)])
            copy.start()
            copies.append(copy)
        if start == 0:
            for load in loads[2:]:
                load.wait()
        for lane in range(0, COLS, HEAD):
            lanes(pl.ds(lane, HEAD), 1.0, 1.0, new_ref, kept_ref)
    low = jnp.concatenate([scale_ref[i][:, :PART] for i in range(PER_HALF)], axis=1)
    high = jnp.concatenate([scale_ref[i][:, :PART] for i in range(PER_HALF, PARTS)], axis=1)
    flip = turn_ref[:, :RUN] > 0.5
    row_ref[...] = jnp.concatenate(
        [jnp.where(flip, high, low), jnp.where(flip, low, high)], axis=1
    )
    for copy in copies:
        copy.wait()


def finalize(*operands):
    vmem = pl.BlockSpec(memory_space=pltpu.VMEM)
    hbm = pl.BlockSpec(memory_space=pltpu.HBM)
    return pl.pallas_call(
        final_kernel,
        out_shape=(
            jax.ShapeDtypeStruct((TOK, D), jnp.bfloat16),
            jax.ShapeDtypeStruct((1, TOK), jnp.float32),
            jax.ShapeDtypeStruct((TOK, COLS), jnp.bfloat16),
        ),
        in_specs=[hbm] * 5,
        out_specs=[hbm, vmem, vmem],
        scratch_shapes=[
            pltpu.VMEM((TOK, D), jnp.bfloat16),
            pltpu.VMEM((TOK, COLS), jnp.bfloat16),
            pltpu.VMEM((TOK, HEAD), jnp.float32),
            pltpu.VMEM((PARTS, 1, HEAD), jnp.float32),
            pltpu.VMEM((1, HEAD), jnp.float32),
            pltpu.VMEM((TOK, D), jnp.bfloat16),
            pltpu.SemaphoreType.DMA((4,)),
            pltpu.SemaphoreType.DMA((2 * RUN // STRIP,)),
            pltpu.SemaphoreType.DMA((2 * RUN // STRIP,)),
        ],
        compiler_params=pltpu.CompilerParams(vmem_limit_bytes=VMEM_LIMIT),
        name="final",
    )(*operands)


def on_device(queries, key_vectors, value_vectors, positions, residual, norm_gain, out_weight):
    results = fused(
        positions, queries, key_vectors, value_vectors, out_weight, residual, norm_gain
    )
    quantized, row, new_residual = finalize(*results)
    return (quantized, row.reshape(TOK), new_residual)


def solution(mesh):
    in_specs = (
        P("seq", "tp"),
        P("seq", "tp"),
        P("seq", "tp"),
        P("seq"),
        P("seq", "tp"),
        P(None, "tp"),
        P("tp", None),
    )
    out_specs = (P("seq", None), P("seq"), P("seq", "tp"))
    return jax.shard_map(
        on_device, mesh=mesh, in_specs=in_specs, out_specs=out_specs, check_vma=False
    )
```

```python
import functools
import heapq
import math

import jax
import jax.numpy as jnp
from jax import lax
from jax.experimental import pallas as pl
from jax.experimental.pallas import tpu as pltpu
from jax.sharding import PartitionSpec as P

D = 6144
HEADS = 6
HEAD = 128
TOK = 192
RUN = TOK // 2
NX = 4
NY = 4
NZ = 8
N_TP = 8
ROWS = HEADS * RUN
GROUP = NX * RUN
CHUNK = 2 * RUN
COLS = HEADS * HEAD
HALF = COLS // 2
PER_HALF = 1
PARTS = 2 * PER_HALF
PART = TOK // PARTS
NEG = -1e30
SUM_DIRECT = ()
SHARE_DIRECT = ()
BEFORE_LO = [("pass_up", PARTS - 1), ("pass_down", PARTS - 1)]
EXP_SCALE = math.log2(math.e) / math.sqrt(HEAD)
MESH = pl.DeviceIdType.MESH

K_LO, V_LO, K_HI, V_HI, RUN_ID = range(5)
KINDS = (V_LO, K_LO, RUN_ID, V_HI, K_HI)
X_FIRST = {K_LO: True, V_LO: False, K_HI: True, V_HI: False, RUN_ID: True}
REACH = {
    K_LO: (2, 1, 4, 3),
    V_LO: (2, 1, 4, 3),
    K_HI: (1, 2, 3, 4),
    V_HI: (1, 2, 3, 4),
    RUN_ID: (2, 1, 4, 3),
}
LO, HI = 0, 1
DIRECT = (K_LO, K_HI, RUN_ID, V_LO, V_HI)
for _k in DIRECT:
    REACH[_k] = (2, 1) + REACH[_k][2:]
REACH[RUN_ID] = (2, 1, 0, 0)
FAR = (2, 1, -1, 0)
X_PLUS, X_MINUS, Z_PLUS, Z_MINUS, Y_PLUS, Y_MINUS, PAIR, X_FAR, Y_FAR = range(9)
(
    UP_RELAY, UP_DIRECT, UP_LAST, DOWN_RELAY, DOWN_DIRECT, DOWN_LAST,
    X_UP, X_DOWN, X_UP_FAR, X_DOWN_FAR,
    X_PAIR, X_PAIR_UP, X_PAIR_DOWN, X_PAIR_UP_FAR, X_PAIR_DOWN_FAR,
) = range(15)
N_ARRIVALS = 15


def children(kind, mx, mz):
    xp, xn, zp, zn = REACH[kind]
    along_x, along_z = [], []
    if kind in DIRECT and mx == 0:
        along_x = [(kind, 1, mz, X_PLUS), (kind, -1, mz, X_MINUS), (kind, 2, mz, X_FAR)]
    if kind in DIRECT:
        xp = xn = 0
    if 0 <= mx < xp:
        along_x.append((kind, mx + 1, mz, X_PLUS))
    if -xn < mx <= 0:
        along_x.append((kind, mx - 1, mz, X_MINUS))
    if 0 <= mz < zp:
        along_z.append((kind, mx, mz + 1, Z_PLUS))
    if -zn < mz <= 0:
        along_z.append((kind, mx, mz - 1, Z_MINUS))
    if X_FIRST[kind]:
        return along_z + along_x if mz == 0 else along_z
    return along_x + along_z if mx == 0 else along_x


def moves(kind):
    xp, xn, zp, zn = REACH[kind]
    return [
        (kind, mx, mz)
        for mx in range(-xn, xp + 1)
        for mz in range(-zn, zp + 1)
        if (mx, mz) != (0, 0)
    ]


def onward(mz):
    steps = []
    if 0 <= mz < 4:
        steps.append((mz + 1, Z_PLUS))
    if -3 < mz <= 0:
        steps.append((mz - 1, Z_MINUS))
    return steps


EVENT_ID = {
    key: i
    for i, key in enumerate(
        [key for kind in KINDS for key in moves(kind)]
        + [("ids", mz) for mz in range(-3, 5) if mz]
    )
}
N_EVENTS = len(EVENT_ID)
UNIT_US = 0.6
PROJECT_US = 0.5
HOP_US = 2.9
PAIR_US = 1.5
PIECE_US = 0.55
PART_US = 1.6 * PART / RUN


def plan():
    tasks = {}
    for kind in KINDS:
        took = 0.04 if kind == RUN_ID else PIECE_US
        for key in [(kind, 0, 0)] + moves(kind):
            sends = [(child[:3], child[3], took) for child in children(*key)]
            own = key[1:] == (0, 0)
            rank = (0 if kind in (K_LO, V_LO, RUN_ID) else 1) + (-2 if own and kind not in (K_HI, V_HI) else 0)
            tasks[("relay",) + key] = (rank, [] if own else [key], ([("relay", K_LO, 0, 2)]) if own and kind in (K_HI, V_HI) else [], 0.03, sends)
    start = [("relay", kind, 0, 0) for kind in KINDS[:3]]
    tasks[("diagonal",)] = (2, [], start, 0.8, [])

    for mz in range(-3, 5):
        needs = [("relay",) + key for key in moves(RUN_ID)] if mz == 0 else []
        tasks[("ids", mz)] = (
            0, [("ids", mz)] if mz else [], needs, 0.03,
            [(("ids", step), link, 0.05) for step, link in onward(mz)],
        )

    def group_keys(kinds, dz):
        return [k for kind in kinds for k in moves(kind) if (k[2] - dz) % NZ == 0]

    lo_kinds, hi_kinds = (K_LO, V_LO), (K_HI, V_HI)
    fins = {LO: [("diagonal",)], HI: [("diagonal",)]}
    for i, dz in enumerate((0, 1, -1, 2, -2, 3, -3, 4)):
        for name, kinds, half, base in (
            ("lo_lo", lo_kinds, LO, 20),
            ("hi_lo", lo_kinds, HI, 40),
            ("hi_hi", hi_kinds, HI, 41),
        ):
            keys = group_keys(kinds, dz)
            task = (name, dz)
            relays = [("relay",) + k for k in keys] + [("ids", dz)]
            tasks[task] = (base + 0.1 * i, [], relays + [("diagonal",)], UNIT_US, [])
            fins[half].append(task)
    for half in (LO, HI):
        late = 0.5 * half
        parts = range(half * PER_HALF, (half + 1) * PER_HALF)
        tasks[("attended", half)] = (10, [], fins[half], 0.4, [(("att", half), PAIR, 0.3)])
        for slot, step in enumerate(FAR):
            sends = []
            for part in parts:
                if part in SUM_DIRECT:
                    pairs, link = {
                        2: ((UP_RELAY, DOWN_RELAY), Y_FAR),
                        1: ((UP_LAST, UP_DIRECT), Y_PLUS),
                        -1: ((DOWN_DIRECT, DOWN_LAST), Y_MINUS),
                        0: ((), Y_PLUS),
                    }[step]
                    sends += [((part, event), link, PART_US) for event in pairs]
                elif step == 2:
                    sends += [((part, UP_RELAY), Y_PLUS, PART_US), ((part, DOWN_RELAY), Y_MINUS, PART_US)]
                elif step == 1:
                    sends += [((part, UP_DIRECT), Y_PLUS, PART_US)]
                elif step == -1:
                    sends += [((part, DOWN_DIRECT), Y_MINUS, PART_US)]
            needs = [("attended", half)] if slot == 0 else [("project", half, slot - 1)]
            tasks[("project", half, slot)] = (9 + late, [("att", half)], needs, PROJECT_US, sends)
        for part in parts:
            direct = part in SUM_DIRECT
            if not direct:
                tasks[("pass_up", part)] = (
                    4 + late, [(part, UP_RELAY)], [("project", half, 1)], 0.1,
                    [((part, UP_LAST), Y_PLUS, PART_US)],
                )
                tasks[("pass_down", part)] = (
                    4 + late, [(part, DOWN_RELAY)], [("project", half, 2)], 0.1,
                    [((part, DOWN_LAST), Y_MINUS, PART_US)],
                )
            tasks[("finish", part)] = (
                6 + late,
                [
                    (part, e)
                    for e in (UP_DIRECT, DOWN_DIRECT, UP_LAST, DOWN_LAST)
                    + ((UP_RELAY, DOWN_RELAY) if direct else ())
                ],
                [("project", half, 3)],
                0.4,
                [((part, "stats"), PAIR, 0.1)],
            )
            tasks[("publish", part)] = (
                6.1 + late,
                [],
                [("finish", part)] + (BEFORE_LO if half == LO else []),
                0.02,
                [
                    ((part, X_UP), Y_PLUS, 2 * PART_US),
                    ((part, X_DOWN), Y_MINUS, 2 * PART_US),
                    ((part, X_PAIR), PAIR, 0.15),
                ]
                + (
                    [((part, X_UP_FAR), Y_FAR, PART_US), ((part, X_DOWN_FAR), Y_FAR, PART_US)]
                    if part in SHARE_DIRECT
                    else []
                ),
            )
            tasks[("share_up", part)] = (
                5 + late, [(part, X_UP)], [], 0.03,
                [((part, X_PAIR_UP), PAIR, 0.15)]
                + ([] if part in SHARE_DIRECT else [((part, X_UP_FAR), Y_PLUS, PART_US)]),
            )
            tasks[("share_down", part)] = (
                5 + late, [(part, X_DOWN)], [], 0.03,
                [((part, X_PAIR_DOWN), PAIR, 0.15)]
                + ([] if part in SHARE_DIRECT else [((part, X_DOWN_FAR), Y_MINUS, PART_US)]),
            )
            tasks[("far_up", part)] = (
                5 + late, [(part, X_UP_FAR)], [], 0.03, [((part, X_PAIR_UP_FAR), PAIR, 0.1)]
            )
            tasks[("far_down", part)] = (
                5 + late, [(part, X_DOWN_FAR)], [], 0.03, [((part, X_PAIR_DOWN_FAR), PAIR, 0.1)]
            )
            tasks[("scales", part)] = (
                50,
                [(part, "stats")],
                [("publish", part)],
                0.3,
                [],
            )
            pairs = (X_PAIR, X_PAIR_UP, X_PAIR_DOWN, X_PAIR_UP_FAR, X_PAIR_DOWN_FAR)
            tasks[("collect", part)] = (60, [(part, e) for e in pairs], [], 0.02, [])

    free = [0.0] * 9
    when = {}
    order, done = [], set()
    left = dict(tasks)
    now = 0.0
    while left:
        best = None
        soonest = None
        for task, (rank, arrivals, needs, cost, sends) in left.items():
            if not all(n in done for n in needs) or not all(a in when for a in arrivals):
                continue
            ready = max([when[a] for a in arrivals], default=0.0)
            if ready <= now:
                if best is None or rank < best[0]:
                    best = (rank, task)
            elif soonest is None or ready < soonest:
                soonest = ready
        if best is None:
            now = soonest
            continue
        task = best[1]
        rank, arrivals, needs, cost, sends = left.pop(task)
        now += cost
        done.add(task)
        order.append((task, now))
        for arrival, link, took in sends:
            if link in (X_FAR, Y_FAR):
                ways = (X_PLUS, X_MINUS) if link == X_FAR else (Y_PLUS, Y_MINUS)
                for way in ways:
                    free[way] = max(free[way], now) + took
                when[arrival] = max(free[way] for way in ways) + HOP_US + 0.7
                continue
            free[link] = max(free[link], now) + took
            hop = 7.0 if arrival[-1] == "stats" else PAIR_US if link == PAIR else HOP_US
            when[arrival] = free[link] + hop
    return order, now


ORDER, PLANNED_US = plan()


def update(rows, queries, m_ref, l_ref, acc_ref, keys, values, bias, chunk):
    starts = range(rows[0], rows[1], chunk)
    all_scores, all_new, all_factors = [], [], []
    for start in starts:
        scores = lax.dot_general(
            queries[pl.ds(start, chunk), :],
            keys,
            (((1,), (1,)), ((), ())),
            preferred_element_type=jnp.float32,
        )
        scores = scores * EXP_SCALE
        all_scores.append(scores if bias is None else scores + bias)
    for start, scores in zip(starts, all_scores):
        at = pl.ds(start, chunk)
        old = m_ref[at, :]
        new = jnp.maximum(old, jnp.max(scores, axis=1, keepdims=True))
        m_ref[at, :] = new
        all_new.append(new)
        all_factors.append(jnp.exp2(old - new))
    for start, scores, new, factor in zip(starts, all_scores, all_new, all_factors):
        at = pl.ds(start, chunk)
        weights = [
            jnp.exp2(scores[:, i : i + HEAD] - new) for i in range(0, scores.shape[1], HEAD)
        ]
        l_ref[at, :] = l_ref[at, :] * factor + functools.reduce(jnp.add, weights)
        probs = jnp.concatenate([w.astype(jnp.bfloat16) for w in weights], axis=1)
        acc_ref[at, :] = acc_ref[at, :] * factor + jnp.dot(
            probs, values, preferred_element_type=jnp.float32
        )


def first_block(first, queries, m_ref, l_ref, acc_ref, keys, values):
    at = pl.ds(first, ROWS)
    scores = lax.dot_general(
        queries[at, :], keys, (((1,), (1,)), ((), ())), preferred_element_type=jnp.float32
    )
    scores = (scores * EXP_SCALE).reshape(HEADS, RUN, RUN)
    row = lax.broadcasted_iota(jnp.int32, (HEADS, RUN, RUN), 1)
    column = lax.broadcasted_iota(jnp.int32, (HEADS, RUN, RUN), 2)
    scores = jnp.where(column <= row, scores, NEG).reshape(ROWS, RUN)
    high = jnp.max(scores, axis=1, keepdims=True)
    weights = jnp.exp2(scores - high)
    m_ref[at, :] = jnp.broadcast_to(high, (ROWS, HEAD))
    total = jnp.sum(weights, axis=1, keepdims=True)
    lane = lax.broadcasted_iota(jnp.int32, (ROWS, HEAD), 1)
    l_ref[at, :] = jnp.where(lane == 0, total, 0.0)
    acc_ref[at, :] = jnp.dot(
        weights.astype(jnp.bfloat16), values, preferred_element_type=jnp.float32
    )


def lane_bias(ids, mine, low):
    one = [
        jnp.where(ids[j] < mine if low else ids[j] > mine, 0.0, NEG) for j in range(NX)
    ]
    lane = lax.broadcasted_iota(jnp.int32, (1, HEAD), 1)
    tiles = [
        jnp.where(lane < 96, one[0], one[1]),
        jnp.where(lane < 64, one[1], one[2]),
        jnp.where(lane < 32, one[2], one[3]),
    ]
    return jnp.concatenate(tiles, axis=1)


def fused_kernel(
    pos_hbm, q_hbm, k_hbm, v_hbm, w_ref, residual_hbm, gain_hbm,
    x_hbm, new_hbm, factor_hbm, scale_hbm, turn_hbm,
    x_ref, new_ref, factor_ref, scale_ref, turn_ref, pos_ref, q_ref, k_ref, v_ref, residual_ref, gain_ref, own, own_id, kv, ids, queries, m_ref, l_ref, acc_ref,
    weights, attended, mine, outgoing, relayed, got, stats,
    store_sem, small_sem, early_sem, load_sem, send, recv, w_send, w_recv, att_send, att_recv,
    part_send, part_recv, stat_send, stat_recv,
):
    seq = lax.axis_index("seq")
    tp = lax.axis_index("tp")
    x = lax.rem(seq, NX)
    z = seq // NX
    core = lax.rem(tp, 2)
    y = tp // 2
    peers = (
        (z * NX + lax.rem(x + 1, NX), tp),
        (z * NX + lax.rem(x + NX - 1, NX), tp),
        (lax.rem(z + 1, NZ) * NX + x, tp),
        (lax.rem(z + NZ - 1, NZ) * NX + x, tp),
        (seq, lax.rem(tp + 2, N_TP)),
        (seq, lax.rem(tp + 6, N_TP)),
        (seq, y * 2 + 1 - core),
        (z * NX + lax.rem(x + 2, NX), tp),
        (seq, lax.rem(tp + 4, N_TP)),
    )

    def columns(step, parity, first=0, width=COLS):
        block = lax.rem(y + step + NY, NY) * 2 + parity
        return pl.ds(pl.multiple_of(block * COLS + first, HEAD), width)

    sent = []
    stores = []

    def keep(source, target, sem):
        store = pltpu.make_async_copy(source, target, sem)
        store.start()
        stores.append(store)

    def remote(source, target, send_sem, recv_sem, peer):
        return pltpu.make_async_remote_copy(
            src_ref=source,
            dst_ref=target,
            send_sem=send_sem,
            recv_sem=recv_sem,
            device_id=peer,
            device_id_type=MESH,
        )

    def ship(*args):
        copy = remote(*args)
        copy.start()
        sent.append(copy)

    def arrive(target, send_sem, recv_sem):
        remote(target, target, send_sem, recv_sem, peers[PAIR]).wait_recv()

    loads = [
        pltpu.make_async_copy(q_hbm, q_ref, load_sem.at[0]),
        pltpu.make_async_copy(residual_hbm, residual_ref, load_sem.at[1]),
    ]
    for slot, step in enumerate(FAR):
        loads.append(
            pltpu.make_async_copy(
                w_ref.at[:, columns(step, core)],
                weights.at[slot, pl.ds(0, COLS)],
                load_sem.at[2 + slot],
            )
        )
    early = [
        pltpu.make_async_copy(k_hbm, k_ref, early_sem.at[0]),
        pltpu.make_async_copy(v_hbm, v_ref, early_sem.at[1]),
        pltpu.make_async_copy(pos_hbm, pos_ref, early_sem.at[2]),
        pltpu.make_async_copy(gain_hbm, gain_ref, early_sem.at[3]),
    ]
    for load in early + loads[:2]:
        load.start()

    barrier = pltpu.get_barrier_semaphore()
    greeted = list(peers[:4]) + [peers[X_FAR]] + [(seq, lax.rem(tp + step, N_TP)) for step in range(1, N_TP)]
    for peer in greeted:
        pl.semaphore_signal(barrier, inc=1, device_id=peer, device_id_type=MESH)
    for load in early:
        load.wait()

    first, last = pos_ref[0], pos_ref[RUN]
    low_run = jnp.minimum(first, last) // RUN
    mine_id = jnp.full((1, HEAD), low_run, jnp.int32).astype(jnp.float32)
    swapped = jnp.full((RUN, HEAD), jnp.where(first > last, 1, 0), jnp.int32) > 0

    def pick(ref, columns, half):
        one = ref[pl.ds(0, RUN), columns].astype(jnp.float32)
        two = ref[pl.ds(RUN, RUN), columns].astype(jnp.float32)
        return jnp.where(swapped, two, one) if half == LO else jnp.where(swapped, one, two)

    every = pl.ds(0, HEAD)
    for kind, ref, half in ((K_LO, k_ref, LO), (V_LO, v_ref, LO), (K_HI, k_ref, HI), (V_HI, v_ref, HI)):
        piece = pick(ref, every, half).astype(jnp.bfloat16)
        own[kind] = piece
        kv[kind, seq] = piece
    turn_ref[...] = swapped[0:1].astype(jnp.float32)
    own_id[0] = mine_id
    ids[seq] = mine_id

    pl.semaphore_wait(barrier, len(greeted))

    def source_of(mx, mz):
        return lax.rem(z + 2 * NZ - mz, NZ) * NX + lax.rem(x + 2 * NX - mx, NX)

    def place(kind, index):
        return ids.at[index] if kind == RUN_ID else kv.at[kind, index]

    def relay(kind, mx, mz):
        index = source_of(mx, mz)
        here = place(kind, index)
        source = here
        if (mx, mz) == (0, 0):
            source = own_id.at[0] if kind == RUN_ID else own.at[kind]
        else:
            event = EVENT_ID[(kind, mx, mz)]
            arrive(here, send.at[event], recv.at[event])
        for child in children(kind, mx, mz):
            event = EVENT_ID[child[:3]]
            ship(source, here, send.at[event], recv.at[event], peers[child[3]])

    def pass_ids(mz):
        here = ids.at[pl.ds(lax.rem(z + 2 * NZ - mz, NZ) * NX, NX)]
        if mz:
            event = EVENT_ID[("ids", mz)]
            arrive(here, send.at[event], recv.at[event])
        for step, link in onward(mz):
            event = EVENT_ID[("ids", step)]
            ship(here, here, send.at[event], recv.at[event], peers[link])

    def diagonal():
        for slot in range(4):
            loads[2 + slot].start()
        for slot, step in enumerate(FAR):
            ship(
                w_ref.at[:, columns(step, 1 - core)],
                weights.at[slot, pl.ds(COLS, COLS)],
                w_send.at[slot],
                w_recv.at[slot],
                peers[PAIR],
            )
        loads[0].wait()
        for head in range(HEADS):
            for half in (LO, HI):
                queries[pl.ds(half * ROWS + head * RUN, RUN), :] = pick(
                    q_ref, pl.ds(head * HEAD, HEAD), half
                ).astype(jnp.bfloat16)
        first_block(0, queries, m_ref, l_ref, acc_ref, own[K_LO], own[V_LO])
        first_block(ROWS, queries, m_ref, l_ref, acc_ref, own[K_HI], own[V_HI])

    def unit(dz, half, low_keys):
        at = pl.ds(lax.rem(z + 2 * NZ - dz, NZ) * NX, NX)
        keys = kv[K_LO if low_keys else K_HI, at].reshape(GROUP, HEAD)
        values = kv[V_LO if low_keys else V_HI, at].reshape(GROUP, HEAD)
        bias = None
        if low_keys == (half == LO):
            bias = lane_bias(ids[at], mine_id, low_keys)
        bounds = (half * ROWS, (half + 1) * ROWS)
        update(bounds, queries, m_ref, l_ref, acc_ref, keys, values, bias, CHUNK)

    def attend_half(half):
        for head in range(HEADS):
            at = pl.ds(half * ROWS + head * RUN, RUN)
            total = jnp.sum(l_ref[at, :], axis=1, keepdims=True)
            attended[half, 0, :, pl.ds(head * HEAD, HEAD)] = (acc_ref[at, :] / total).astype(
                jnp.bfloat16
            )
        ship(
            attended.at[half, 0],
            attended.at[half, 1],
            att_send.at[half],
            att_recv.at[half],
            peers[PAIR],
        )

    def rows(part):
        return pl.ds(part * PART, PART)

    left = pl.ds(0, HALF)
    right = pl.ds(HALF, HALF)

    def slab(event, part):
        return got.at[event, rows(part)]

    def send_part(part, event, source, target, peer):
        ship(source, target, part_send.at[part, event], part_recv.at[part, event], peers[peer])

    def await_part(part, event, target):
        arrive(target, part_send.at[part, event], part_recv.at[part, event])

    def project(half, slot):
        if slot == 0:
            arrive(attended.at[half, 1], att_send.at[half], att_recv.at[half])
        if half == LO:
            loads[2 + slot].wait()
            arrive(weights.at[slot, pl.ds(COLS, COLS)], w_send.at[slot], w_recv.at[slot])
        product = jnp.dot(
            attended[half, 0], weights[slot, pl.ds(0, COLS), :], preferred_element_type=jnp.float32
        ) + jnp.dot(
            attended[half, 1],
            weights[slot, pl.ds(COLS, COLS), :],
            preferred_element_type=jnp.float32,
        )
        step = FAR[slot]
        if step == 0:
            mine[pl.ds(half * RUN, RUN), :] = product
            return
        outgoing[slot, pl.ds(half * RUN, RUN), :] = product.astype(jnp.bfloat16)
        for part in range(half * PER_HALF, (half + 1) * PER_HALF):
            here = outgoing.at[slot, rows(part)]
            if part in SUM_DIRECT:
                (first, second), peer = {
                    2: ((UP_RELAY, DOWN_RELAY), Y_FAR),
                    1: ((UP_LAST, UP_DIRECT), Y_PLUS),
                    -1: ((DOWN_DIRECT, DOWN_LAST), Y_MINUS),
                }[step]
                send_part(part, first, here.at[:, left], slab(first, part), peer)
                send_part(part, second, here.at[:, right], slab(second, part), peer)
            elif step == 2:
                send_part(part, UP_RELAY, here.at[:, left], slab(UP_RELAY, part), Y_PLUS)
                send_part(part, DOWN_RELAY, here.at[:, right], slab(DOWN_RELAY, part), Y_MINUS)
            elif step == 1:
                send_part(part, UP_DIRECT, here.at[:, right], slab(UP_DIRECT, part), Y_PLUS)
            else:
                send_part(part, DOWN_DIRECT, here.at[:, left], slab(DOWN_DIRECT, part), Y_MINUS)

    def pass_on(part, way):
        arrival, onward, slot, half, peer = (
            (UP_RELAY, UP_LAST, 1, left, Y_PLUS),
            (DOWN_RELAY, DOWN_LAST, 2, right, Y_MINUS),
        )[way]
        at = rows(part)
        await_part(part, arrival, slab(arrival, part))
        total = outgoing[slot, at, half].astype(jnp.float32) + slab(arrival, part)[...].astype(
            jnp.float32
        )
        relayed[way, at, :] = total.astype(jnp.bfloat16)
        send_part(part, onward, relayed.at[way, at], slab(onward, part), peer)

    def finish(part):
        at = rows(part)
        half_of = part // PER_HALF
        if part == 0:
            loads[1].wait()
        squares = jnp.zeros((PART, HEAD), jnp.float32)
        peak = jnp.zeros((PART, HEAD), jnp.float32)
        inside = (part % PER_HALF) * PART
        one, two = pl.ds(inside, PART), pl.ds(RUN + inside, PART)
        turned = swapped[0:PART]
        for first, *events in (
            (0, DOWN_DIRECT, UP_LAST, UP_RELAY),
            (HALF, UP_DIRECT, DOWN_LAST, DOWN_RELAY),
        ):
            events = events if part in SUM_DIRECT else events[:2]
            for event in events:
                await_part(part, event, slab(event, part))
            for lane in range(0, HALF, HEAD):
                here = pl.ds(first + lane, HEAD)
                there = pl.ds(lane, HEAD)
                low = residual_ref[one, here].astype(jnp.float32)
                high = residual_ref[two, here].astype(jnp.float32)
                old = jnp.where(turned, high, low) if half_of == LO else jnp.where(turned, low, high)
                summed = mine[at, here] + old
                for event in events:
                    summed = summed + slab(event, part)[:, there].astype(jnp.float32)
                new_ref[at, here] = summed.astype(jnp.bfloat16)
                gained = summed * gain_ref[:, here]
                x_ref[at, columns(0, core, first + lane, HEAD)] = gained.astype(jnp.bfloat16)
                squares = squares + summed * summed
                peak = jnp.maximum(peak, jnp.abs(gained))
        lane = lax.broadcasted_iota(jnp.int32, (PART, HEAD), 1)
        both = jnp.where(
            lane == 0,
            jnp.sum(squares, axis=1, keepdims=True),
            jnp.max(peak, axis=1, keepdims=True),
        )
        if PART < HEAD:
            both = jnp.concatenate([both, jnp.zeros((HEAD - PART, HEAD), jnp.float32)], axis=0)
        stats[part, tp] = jnp.transpose(both)[0:8, :]
        for step in range(1, N_TP):
            ship(
                stats.at[part, tp],
                stats.at[part, tp],
                stat_send.at[part, step],
                stat_recv.at[part, step],
                (seq, lax.rem(tp + step, N_TP)),
            )

    def publish(part):
        at = rows(part)
        keep(new_ref.at[at], new_hbm.at[at], small_sem.at[2, part])
        if part == 0:
            keep(turn_ref, turn_hbm, early_sem.at[4])
        block = x_ref.at[at, columns(0, core)]
        send_part(part, X_UP, block, block, Y_PLUS)
        send_part(part, X_DOWN, block, block, Y_MINUS)
        if part in SHARE_DIRECT:
            for event, first in ((X_UP_FAR, 0), (X_DOWN_FAR, HALF)):
                half = x_ref.at[at, columns(0, core, first, HALF)]
                send_part(part, event, half, half, Y_FAR)
        send_part(part, X_PAIR, block, block, PAIR)

    def share(part, way):
        arrival, far, pair, step, first, peer = (
            (X_UP, X_UP_FAR, X_PAIR_UP, -1, 0, Y_PLUS),
            (X_DOWN, X_DOWN_FAR, X_PAIR_DOWN, 1, HALF, Y_MINUS),
        )[way]
        at = rows(part)
        block = x_ref.at[at, columns(step, core)]
        await_part(part, arrival, block)
        if part not in SHARE_DIRECT:
            half = x_ref.at[at, columns(step, core, first, HALF)]
            send_part(part, far, half, half, peer)
        send_part(part, pair, block, block, PAIR)

    def share_far(part, way):
        arrival, pair, first = (
            (X_UP_FAR, X_PAIR_UP_FAR, 0),
            (X_DOWN_FAR, X_PAIR_DOWN_FAR, HALF),
        )[way]
        half = x_ref.at[rows(part), columns(2, core, first, HALF)]
        await_part(part, arrival, half)
        send_part(part, pair, half, half, PAIR)

    def scales(part):
        for step in range(1, N_TP):
            source = lax.rem(tp + N_TP - step, N_TP)
            arrive(stats.at[part, source], stat_send.at[part, step], stat_recv.at[part, step])
        total = stats[part, 0, 0:1, :]
        high = stats[part, 0, 1:2, :]
        for source in range(1, N_TP):
            total = total + stats[part, source, 0:1, :]
            high = jnp.maximum(high, stats[part, source, 1:2, :])
        root = lax.rsqrt(total / D + 1e-05)
        scale = high * root + 1e-06
        scale_ref[part] = scale
        factor = jnp.transpose(jnp.broadcast_to(root / scale, (HEAD, HEAD)))
        factor_ref[rows(part), :] = factor[0:PART, :]
        keep(scale_ref.at[part], scale_hbm.at[part], small_sem.at[0, part])
        keep(factor_ref.at[rows(part)], factor_hbm.at[rows(part)], small_sem.at[1, part])

    def collect(part):
        at = rows(part)
        other = 1 - core
        for event, step, first, width in (
            (X_PAIR, 0, 0, COLS),
            (X_PAIR_UP, -1, 0, COLS),
            (X_PAIR_DOWN, 1, 0, COLS),
            (X_PAIR_UP_FAR, 2, 0, HALF),
            (X_PAIR_DOWN_FAR, 2, HALF, HALF),
        ):
            await_part(part, event, x_ref.at[at, columns(step, other, first, width)])
        keep(x_ref.at[at], x_hbm.at[at], store_sem.at[part])

    emit = {
        "relay": relay,
        "ids": pass_ids,
        "diagonal": diagonal,
        "lo_lo": lambda dz: unit(dz, LO, True),
        "hi_lo": lambda dz: unit(dz, HI, True),
        "hi_hi": lambda dz: unit(dz, HI, False),
        "attended": attend_half,
        "project": project,
        "pass_up": lambda part: pass_on(part, 0),
        "pass_down": lambda part: pass_on(part, 1),
        "finish": finish,
        "publish": publish,
        "share_up": lambda part: share(part, 0),
        "share_down": lambda part: share(part, 1),
        "far_up": lambda part: share_far(part, 0),
        "far_down": lambda part: share_far(part, 1),
        "scales": scales,
        "collect": collect,
    }
    for task, _ in ORDER:
        emit[task[0]](*task[1:])
    for copy in sent:
        copy.wait_send()
    for store in stores:
        store.wait()


def fused(positions, queries, keys, values, out_weight, residual, gain):
    hbm = pl.BlockSpec(memory_space=pltpu.HBM)
    bf16, f32 = jnp.bfloat16, jnp.float32
    dma = pltpu.SemaphoreType.DMA
    return pl.pallas_call(
        fused_kernel,
        out_shape=(
            jax.ShapeDtypeStruct((TOK, D), bf16),
            jax.ShapeDtypeStruct((TOK, COLS), bf16),
            jax.ShapeDtypeStruct((TOK, HEAD), f32),
            jax.ShapeDtypeStruct((PARTS, 1, HEAD), f32),
            jax.ShapeDtypeStruct((1, HEAD), f32),
        ),
        in_specs=[hbm] * 7,
        out_specs=[hbm] * 5,
        scratch_shapes=[
            pltpu.VMEM((TOK, D), bf16),
            pltpu.VMEM((TOK, COLS), bf16),
            pltpu.VMEM((TOK, HEAD), f32),
            pltpu.VMEM((PARTS, 1, HEAD), f32),
            pltpu.VMEM((1, HEAD), f32),
            pltpu.SMEM((TOK,), jnp.int32),
            pltpu.VMEM((TOK, COLS), bf16),
            pltpu.VMEM((TOK, HEAD), bf16),
            pltpu.VMEM((TOK, HEAD), bf16),
            pltpu.VMEM((TOK, COLS), bf16),
            pltpu.VMEM((1, COLS), f32),
            pltpu.VMEM((4, RUN, HEAD), bf16),
            pltpu.VMEM((1, 1, HEAD), f32),
            pltpu.VMEM((4, NX * NZ, RUN, HEAD), bf16),
            pltpu.VMEM((NX * NZ, 1, HEAD), f32),
            pltpu.VMEM((2 * ROWS, HEAD), bf16),
            pltpu.VMEM((2 * ROWS, HEAD), f32),
            pltpu.VMEM((2 * ROWS, HEAD), f32),
            pltpu.VMEM((2 * ROWS, HEAD), f32),
            pltpu.VMEM((4, 2 * COLS, COLS), bf16),
            pltpu.VMEM((2, 2, RUN, COLS), bf16),
            pltpu.VMEM((TOK, COLS), f32),
            pltpu.VMEM((3, TOK, COLS), bf16),
            pltpu.VMEM((2, TOK, HALF), bf16),
            pltpu.VMEM((6, TOK, HALF), bf16),
            pltpu.VMEM((PARTS, N_TP, 8, HEAD), f32),
            dma((PARTS,)),
            dma((3, PARTS)),
            dma((5,)),
            dma((6,)),
            dma((N_EVENTS,)),
            dma((N_EVENTS,)),
            dma((4,)),
            dma((4,)),
            dma((2,)),
            dma((2,)),
            dma((PARTS, N_ARRIVALS)),
            dma((PARTS, N_ARRIVALS)),
            dma((PARTS, N_TP)),
            dma((PARTS, N_TP)),
        ],
        compiler_params=pltpu.CompilerParams(
            collective_id=0, has_side_effects=True, vmem_limit_bytes=VMEM_LIMIT
        ),
        name="fused",
    )(positions, queries, keys, values, out_weight, residual, gain)


VMEM_LIMIT = 67043328
STRIP = 32


def final_kernel(
    x_hbm, new_hbm, factor_hbm, scale_hbm, turn_hbm, out_hbm, row_ref, kept_ref,
    x_ref, new_ref, factor_ref, scale_ref, turn_ref, out_ref, load_sem, x_sem, sem,
):
    loads = [
        pltpu.make_async_copy(source, target, load_sem.at[i])
        for i, (source, target) in enumerate(
            (
                (turn_hbm, turn_ref),
                (factor_hbm, factor_ref),
                (scale_hbm, scale_ref),
                (new_hbm, new_ref),
            )
        )
    ]
    strips = []
    for i, start in enumerate(range(0, RUN, STRIP)):
        for j in range(2):
            at = pl.ds(j * RUN + start, STRIP)
            strips.append(
                pltpu.make_async_copy(x_hbm.at[at], x_ref.at[at], x_sem.at[2 * i + j])
            )
    for load in loads[:2] + strips + loads[2:]:
        load.start()
    for load in loads[:2]:
        load.wait()
    turned = jnp.broadcast_to(turn_ref[...], (STRIP, HEAD)) > 0.5
    copies = []
    for start in range(0, RUN, STRIP):
        one, two = pl.ds(start, STRIP), pl.ds(RUN + start, STRIP)
        low, high = factor_ref[one, :], factor_ref[two, :]
        strips[len(copies)].wait()
        strips[len(copies) + 1].wait()

        def lanes(at, low, high, source, target, one=one, two=two):
            a = source[one, at].astype(jnp.float32) * low
            b = source[two, at].astype(jnp.float32) * high
            target[one, at] = jnp.where(turned, b, a).astype(jnp.bfloat16)
            target[two, at] = jnp.where(turned, a, b).astype(jnp.bfloat16)

        for lane in range(0, D, HEAD):
            lanes(pl.ds(lane, HEAD), low, high, x_ref, out_ref)
        for at in (one, two):
            copy = pltpu.make_async_copy(out_ref.at[at], out_hbm.at[at], sem.at[len(copies)])
            copy.start()
            copies.append(copy)
        if start == 0:
            for load in loads[2:]:
                load.wait()
        for lane in range(0, COLS, HEAD):
            lanes(pl.ds(lane, HEAD), 1.0, 1.0, new_ref, kept_ref)
    low = jnp.concatenate([scale_ref[i][:, :PART] for i in range(PER_HALF)], axis=1)
    high = jnp.concatenate([scale_ref[i][:, :PART] for i in range(PER_HALF, PARTS)], axis=1)
    flip = turn_ref[:, :RUN] > 0.5
    row_ref[...] = jnp.concatenate(
        [jnp.where(flip, high, low), jnp.where(flip, low, high)], axis=1
    )
    for copy in copies:
        copy.wait()


def finalize(*operands):
    vmem = pl.BlockSpec(memory_space=pltpu.VMEM)
    hbm = pl.BlockSpec(memory_space=pltpu.HBM)
    return pl.pallas_call(
        final_kernel,
        out_shape=(
            jax.ShapeDtypeStruct((TOK, D), jnp.bfloat16),
            jax.ShapeDtypeStruct((1, TOK), jnp.float32),
            jax.ShapeDtypeStruct((TOK, COLS), jnp.bfloat16),
        ),
        in_specs=[hbm] * 5,
        out_specs=[hbm, vmem, vmem],
        scratch_shapes=[
            pltpu.VMEM((TOK, D), jnp.bfloat16),
            pltpu.VMEM((TOK, COLS), jnp.bfloat16),
            pltpu.VMEM((TOK, HEAD), jnp.float32),
            pltpu.VMEM((PARTS, 1, HEAD), jnp.float32),
            pltpu.VMEM((1, HEAD), jnp.float32),
            pltpu.VMEM((TOK, D), jnp.bfloat16),
            pltpu.SemaphoreType.DMA((4,)),
            pltpu.SemaphoreType.DMA((2 * RUN // STRIP,)),
            pltpu.SemaphoreType.DMA((2 * RUN // STRIP,)),
        ],
        compiler_params=pltpu.CompilerParams(vmem_limit_bytes=VMEM_LIMIT),
        name="final",
    )(*operands)


def on_device(queries, key_vectors, value_vectors, positions, residual, norm_gain, out_weight):
    results = fused(
        positions, queries, key_vectors, value_vectors, out_weight, residual, norm_gain
    )
    quantized, row, new_residual = finalize(*results)
    return (quantized, row.reshape(TOK), new_residual)


def solution(mesh):
    in_specs = (
        P("seq", "tp"),
        P("seq", "tp"),
        P("seq", "tp"),
        P("seq"),
        P("seq", "tp"),
        P(None, "tp"),
        P("tp", None),
    )
    out_specs = (P("seq", None), P("seq"), P("seq", "tp"))
    return jax.shard_map(
        on_device, mesh=mesh, in_specs=in_specs, out_specs=out_specs, check_vma=False
    )
```
